32 devices in a mesh: dp: 8 (over z, y), tensor: 4 (over x, core).
Axes of the slice: x: 2, y: 2, z: 4, core: 2. Of those that a mesh axis runs over, the one named last changes fastest.
Arguments:
- tokens: bfloat16 [16384, 768], P(('dp', 'tensor')), may hold values from -6 to 6
- cotangent: bfloat16 [16384, 768], P(('dp', 'tensor')), may hold values from -6 to 6
- seq_lengths: int32 [8], P('dp'), may hold values from 1 to 2048, 8192 in all
- norm1_gain: float32 [768], replicated, may hold values from 0.5 to 1.5
- norm1_bias: float32 [768], replicated, may hold values from -1.75 to 1.75
- norm2_gain: float32 [768], replicated, may hold values from 0.5 to 1.5
- norm2_bias: float32 [768], replicated, may hold values from -1.75 to 1.75
- w_qkv: bfloat16 [768, 3, 768], P('dp', None, 'tensor'), may hold values from -3 to 3
- b_qkv: float32 [3, 768], P(None, 'tensor'), may hold values from -1.75 to 1.75
- w_attn_out: bfloat16 [768, 768], P('tensor', 'dp'), may hold values from -0.875 to 0.875
- w_in: bfloat16 [768, 3072], P('dp', 'tensor'), may hold values from -0.21875 to 0.21875
- b_in: float32 [3072], P('tensor'), may hold values from -3 to 3
- w_down: bfloat16 [3072, 768], P('tensor', 'dp'), may hold values from -0.109375 to 0.109375
- b_out: float32 [768], replicated, may hold values from -3 to 3
- b_down: float32 [768], replicated, may hold values from -3 to 3
Outputs:
- output: float32 [16384, 768], P(('dp', 'tensor'))
- grad_tokens: float32 [16384, 768], P(('dp', 'tensor'))
- grad_w_qkv: float32 [768, 3, 768], P('dp', None, 'tensor')
- grad_b_qkv: float32 [3, 768], P(None, 'tensor')
- grad_w_attn_out: float32 [768, 768], P('tensor', 'dp')
- grad_w_in: float32 [768, 3072], P('dp', 'tensor')
- grad_b_in: float32 [3072], P('tensor')
- grad_w_down: float32 [3072, 768], P('tensor', 'dp')
- grad_small: float32 [5, 768], replicated
The draws below stay inside these ranges and needn't reach their ends.
Inputs may be any that keep to these rules, and one draw needn't show every extreme that they name: `seq_lengths`: the longest sequence has exactly 2048.
All inputs are finite; a program needn't handle non-finite values. No bound on the sum of `seq_lengths` on one device may be relied on, other than what follows from the above.
Results may differ from the reference program's by a relative error of at most 0.0062.
Values may be sent and summed in bfloat16 or wider, within the bound.
A program may use at most 128 MiB of HBM per device.

```python
import math
import jax
import jax.numpy as jnp
import numpy as np
from jax import lax

D = 768
H = 12
HD = 64
ROT = 16
FF = 3072
LMAX = 2048
SEQS = 8
TOKENS = 16384


def draw_w_qkv(key, part):
    base = jax.random.truncated_normal(key, -4.0, 4.0, (D, 3, D), jnp.float32) * D ** (-0.5)
    return base.astype(jnp.bfloat16)


def level_of(rng, dims, cuts, least, high):
    level = 1.0
    for dim, parts in cuts:
        draws = jax.random.uniform(jax.random.fold_in(jax.random.fold_in(rng, 6), dim), (parts,), jnp.float32, least / len(cuts), high / len(cuts))
        level = level * jnp.repeat(jnp.exp(draws), dims[dim] // parts).reshape((-1,) + (1,) * (len(dims) - 1 - dim))
    return level


def length_profile(amount, total, most, skew):
    weights = [(1 << 20) // math.isqrt(grade ** skew) + 1 for grade in range(2, amount + 1)]
    surplus, counts = total - most - (amount - 1), [1] * (amount - 1)
    while surplus > 0:
        movable = [i for i in range(amount - 1) if counts[i] < most]
        pool, budget = sum([weights[i] for i in movable]), surplus
        for i in movable:
            extra = min(most - counts[i], max(1, budget * weights[i] // pool), surplus)
            counts[i] = counts[i] + extra
            surplus = surplus - extra
    return np.array([most] + counts)


def ragged_sizes(rng, count, total, reach, skew):
    if count == 2:
        one = jax.random.randint(rng, (), max(1, total - reach), min(reach, total - 1) + 1)
        return jnp.stack([one, total - one])
    tallies = jnp.asarray(length_profile(count, total, reach, skew), jnp.int32)
    twos = (count - 1) // 2
    source_of, sink = tallies[1:1 + 2 * twos:2], tallies[2:2 + 2 * twos:2]
    room = jnp.minimum(source_of - 1, reach - sink)
    moved = jax.random.randint(jax.random.fold_in(rng, 1), (twos,), 0, 1 << 20) % (room + 1)
    tallies = tallies.at[1:1 + 2 * twos:2].set(source_of - moved).at[2:2 + 2 * twos:2].set(sink + moved)
    return tallies[jax.random.permutation(jax.random.fold_in(rng, 2), count)]


def noise(own_key, extent, scale, most, cuts=(), held_as=jnp.bfloat16):
    entries = scale * jax.random.normal(own_key, extent, jnp.float32)
    if cuts:
        entries = entries * level_of(own_key, extent, cuts, -0.22, 0.18)
    return jnp.clip(entries, -most, most).astype(held_as)


def setup_inputs(seed: int = 0) -> dict:
    splits = jax.random.split(jax.random.key(seed), 16)
    return {
        "tokens": noise(splits[0], (TOKENS, D), 1.0, 6.0, ((0, 32),)),
        "cotangent": noise(splits[1], (TOKENS, D), 1.0, 6.0, ((0, 32),)),
        "seq_lengths": ragged_sizes(splits[2], SEQS, SEQS * LMAX // 2, LMAX, 2).astype(jnp.int32),
        "norm1_gain": jnp.clip(1.0 + 0.1 * jax.random.normal(splits[3], (D,), jnp.float32), 0.5, 1.5),
        "norm1_bias": noise(splits[4], (D,), 0.3, 1.75, (), jnp.float32),
        "norm2_gain": jnp.clip(1.0 + 0.1 * jax.random.normal(splits[5], (D,), jnp.float32), 0.5, 1.5),
        "norm2_bias": noise(splits[6], (D,), 0.3, 1.75, (), jnp.float32),
        "w_qkv": draw_w_qkv(jax.random.fold_in(splits[15], 71), 0),
        "b_qkv": noise(splits[8], (3, D), 0.3, 1.75, ((1, 4),), jnp.float32),
        "w_attn_out": noise(splits[9], (D, D), (D // 16) ** -0.5, 0.875, ((0, 4), (1, 8))),
        "w_in": noise(splits[10], (D, FF), D ** -0.5, 0.21875, ((0, 8), (1, 4))),
        "b_in": noise(splits[11], (FF,), 0.5, 3.0, ((0, 4),), jnp.float32),
        "w_down": noise(splits[12], (FF, D), FF ** -0.5, 0.109375, ((0, 4), (1, 8))),
        "b_out": noise(splits[13], (D,), 0.5, 3.0, (), jnp.float32),
        "b_down": noise(splits[14], (D,), 0.5, 3.0, (), jnp.float32),
    }


eps_norm = 1e-05
neg_large = -1e+30
inv_root_two = 1.0 / math.sqrt(2.0)
inv_root_tau = 1.0 / math.sqrt(2.0 * math.pi)

def layer_norm(values):
    centre = lax.optimization_barrier(jnp.mean(values, axis=-1, keepdims=True))
    shifted = values - centre
    variance = lax.optimization_barrier(jnp.mean(shifted * shifted, axis=-1, keepdims=True))
    inv_std = lax.rsqrt(variance + eps_norm)
    return (shifted * inv_std, inv_std)

def rotary_tables(positions):
    head_dims = jnp.arange(HD)
    half_rot = ROT // 2
    freq_index = (head_dims % half_rot).astype(jnp.float32)
    inverse = jnp.exp(freq_index * (-2.0 * math.log(10000.0) / ROT))
    angles = positions.astype(jnp.float32)[:, None] * inverse[None, :]
    inside = (head_dims < ROT)[None, :]
    return (jnp.where(inside, jnp.cos(angles), 1.0), jnp.where(inside, jnp.sin(angles), 0.0))

def rotate(values, cosine, sine_part):
    half_rot = ROT // 2
    turned = jnp.concatenate([-values[..., half_rot:ROT], values[..., :half_rot], jnp.zeros_like(values[..., ROT:])], axis=-1)
    return values * cosine[:, None, :] + turned * sine_part[:, None, :]

def gelu_with_slope(inputs):
    normal_cdf = 0.5 * (1.0 + jax.scipy.special.erf(inputs * inv_root_two))
    density = jnp.exp(-0.5 * inputs * inputs) * inv_root_tau
    return (inputs * normal_cdf, normal_cdf + inputs * density)

def reference(tokens, cotangent, seq_lengths, norm1_gain, norm1_bias, norm2_gain, norm2_bias, w_qkv, b_qkv, w_attn_out, w_in, b_in, w_down, b_out, b_down):
    scale = HD ** (-0.5)
    qkv_flat = w_qkv.reshape(D, 3 * D)
    positions = jnp.arange(LMAX)
    cosine, sine_part = rotary_tables(positions)
    f32 = jnp.float32
    low = jnp.bfloat16

    def one_sequence(totals, inputs):
        x_rows, cot_rows, length = inputs
        x_float = x_rows.astype(f32)
        normed, inv_std = layer_norm(x_float)
        first_in = (normed * norm1_gain + norm1_bias).astype(low)
        second_in = (normed * norm2_gain + norm2_bias).astype(low)
        projected = jnp.dot(first_in, qkv_flat, preferred_element_type=f32).reshape(LMAX, 3, H, HD) + b_qkv.reshape(1, 3, H, HD)
        queries = rotate(projected[:, 0], cosine, sine_part).astype(low)
        key_rows = rotate(projected[:, 1], cosine, sine_part).astype(low)
        value_rows = projected[:, 2].astype(low)
        allowed = (positions[None, :] <= positions[:, None]) & (positions[None, :] < length)
        scores = jnp.einsum('qhd,khd->hqk', queries.astype(f32), key_rows.astype(f32)) * scale
        scores = jnp.where(allowed[None], scores, neg_large)
        top = lax.optimization_barrier(jnp.max(scores, axis=-1, keepdims=True))
        log_total = top + jnp.log(lax.optimization_barrier(jnp.sum(jnp.exp(scores - top), axis=-1, keepdims=True)))
        probs = jnp.exp(scores - log_total)
        probs_low = probs.astype(low)
        context = jnp.einsum('hqk,khd->qhd', probs_low.astype(f32), value_rows.astype(f32)).astype(low)
        context_flat = context.reshape(LMAX, D)
        hidden_pre = jnp.dot(second_in, w_in, preferred_element_type=f32) + b_in
        activated, slope = gelu_with_slope(hidden_pre)
        act_low = activated.astype(low)
        branches = jnp.dot(context_flat, w_attn_out, preferred_element_type=f32) + jnp.dot(act_low, w_down, preferred_element_type=f32)
        row_mask = (positions < length).astype(f32)[:, None]
        output = x_float + row_mask * (branches + b_out + b_down)
        grad_rows = row_mask * cot_rows.astype(f32)
        grad_low = grad_rows.astype(low)
        dense_grad = lax.optimization_barrier(jnp.sum(grad_rows, axis=0))
        grad_attn_out = jnp.dot(context_flat.T, grad_low, preferred_element_type=f32)
        grad_down = jnp.dot(act_low.T, grad_low, preferred_element_type=f32)
        grad_context = jnp.dot(grad_low, w_attn_out.T, preferred_element_type=f32).astype(low).reshape(LMAX, H, HD)
        grad_hidden = jnp.dot(grad_low, w_down.T, preferred_element_type=f32) * slope
        grad_hidden_low = grad_hidden.astype(low)
        grad_in_bias = lax.optimization_barrier(jnp.sum(grad_hidden, axis=0))
        grad_in = jnp.dot(second_in.T, grad_hidden_low, preferred_element_type=f32)
        grad_probs = jnp.einsum('qhd,khd->hqk', grad_context.astype(f32), value_rows.astype(f32))
        delta = lax.optimization_barrier(jnp.sum(grad_context.astype(f32) * context.astype(f32), axis=-1)).T
        grad_scores = (probs * (grad_probs - delta[:, :, None]) * scale).astype(low)
        grad_query = jnp.einsum('hqk,khd->qhd', grad_scores.astype(f32), key_rows.astype(f32))
        grad_key = jnp.einsum('hqk,qhd->khd', grad_scores.astype(f32), queries.astype(f32))
        grad_value = jnp.einsum('hqk,qhd->khd', probs_low.astype(f32), grad_context.astype(f32))
        grad_projected = jnp.stack([rotate(grad_query, cosine, -sine_part), rotate(grad_key, cosine, -sine_part), grad_value], axis=1)
        grad_qkv_bias = lax.optimization_barrier(jnp.sum(grad_projected, axis=0)).reshape(3, D)
        grad_proj_low = grad_projected.astype(low).reshape(LMAX, 3 * D)
        grad_qkv = jnp.dot(first_in.T, grad_proj_low, preferred_element_type=f32).reshape(D, 3, D)
        grad_first = jnp.dot(grad_proj_low, qkv_flat.T, preferred_element_type=f32)
        grad_second = jnp.dot(grad_hidden_low, w_in.T, preferred_element_type=f32)
        small_terms = jnp.stack([lax.optimization_barrier(jnp.sum(grad_first * normed, axis=0)), lax.optimization_barrier(jnp.sum(grad_first, axis=0)), lax.optimization_barrier(jnp.sum(grad_second * normed, axis=0)), lax.optimization_barrier(jnp.sum(grad_second, axis=0)), dense_grad])
        grad_normed = grad_first * norm1_gain + grad_second * norm2_gain
        grad_x = cot_rows.astype(f32) + inv_std * (grad_normed - lax.optimization_barrier(jnp.mean(grad_normed, axis=-1, keepdims=True)) - normed * lax.optimization_barrier(jnp.mean(grad_normed * normed, axis=-1, keepdims=True)))
        updates = (grad_qkv, grad_qkv_bias, grad_attn_out, grad_in, grad_in_bias, grad_down, small_terms)
        totals = tuple((total + update for total, update in zip(totals, updates)))
        return (totals, (output, grad_x))
    start_totals = (jnp.zeros((D, 3, D), f32), jnp.zeros((3, D), f32), jnp.zeros((D, D), f32), jnp.zeros((D, FF), f32), jnp.zeros((FF,), f32), jnp.zeros((FF, D), f32), jnp.zeros((5, D), f32))
    sequences = (tokens.reshape(SEQS, LMAX, D), cotangent.reshape(SEQS, LMAX, D), seq_lengths)
    totals, results = lax.scan(one_sequence, start_totals, sequences)
    outputs, grad_tokens = results
    return (outputs.reshape(TOKENS, D), grad_tokens.reshape(TOKENS, D), totals[0], totals[1], totals[2], totals[3], totals[4], totals[5], totals[6])
```

```python
import functools
import math

import jax
import jax.numpy as jnp
import numpy as np
from jax import lax
from jax.experimental import pallas as pl
from jax.experimental.pallas import tpu as pltpu
from jax.sharding import PartitionSpec as P

HD = 64
ROT = 16
LMAX = 2048
LANES = 128
EPS = 1e-05
BLOCK = 256
FAST = 64
VMEM = 66 * 1024 * 1024

f32 = jnp.float32
low = jnp.bfloat16

NN = (((1,), (0,)), ((), ()))
NT = (((1,), (1,)), ((), ()))
TN = (((0,), (0,)), ((), ()))


def dot(a, b, dims):
    return lax.dot_general(a, b, dims, preferred_element_type=f32)


def round_up(n, m):
    return (n + m - 1) // m * m


def rotary_base():
    d = np.arange(LANES) % HD
    half = ROT // 2
    inverse = np.where(d < ROT, np.exp((d % half) * (-2.0 * math.log(10000.0) / ROT)), 0.0)
    slow = np.arange(0, LMAX, FAST)[:, None] * inverse
    fast = np.arange(FAST)[:, None] * inverse
    return np.concatenate([np.cos(slow), np.sin(slow), np.cos(fast), np.sin(fast)]).astype(
        np.float32
    )


def rotary_rows(table_ref, block):
    slow_rows = LMAX // FAST
    fast_cos = table_ref[2 * slow_rows : 2 * slow_rows + FAST, :]
    fast_sin = table_ref[2 * slow_rows + FAST :, :]
    cosines, sines = [], []
    for part in range(BLOCK // FAST):
        row = block * (BLOCK // FAST) + part
        slow_cos = table_ref[pl.ds(row, 1), :]
        slow_sin = table_ref[pl.ds(row + slow_rows, 1), :]
        cosines.append(slow_cos * fast_cos - slow_sin * fast_sin)
        sines.append(slow_sin * fast_cos + slow_cos * fast_sin)
    cosine, sine = jnp.concatenate(cosines), jnp.concatenate(sines)
    d = lax.broadcasted_iota(jnp.int32, cosine.shape, 1) % HD
    return (
        cosine,
        jnp.where(d < ROT // 2, -sine, 0.0),
        jnp.where((d >= ROT // 2) & (d < ROT), sine, 0.0),
    )


def rotate(values, tables, sign):
    cosine, from_right, from_left = tables
    half = ROT // 2
    turned = []
    for first in range(0, values.shape[1], LANES):
        t = values[:, first : first + LANES]
        side = (
            pltpu.roll(t, LANES - half, axis=1) * from_right
            + pltpu.roll(t, half, axis=1) * from_left
        )
        turned.append(t * cosine + side if sign > 0 else t * cosine - side)
    return jnp.concatenate(turned, axis=1)


def three_terms(value):
    first = value.astype(low).astype(f32)
    second = (value - first).astype(low).astype(f32)
    return first, second, value - first - second


def front_kernel(width, x_ref, norm_ref, wq_ref, bq_ref, table_ref, first_ref, second_ref, qkv_ref):
    padded = qkv_ref.shape[1] // 3
    x = x_ref[...].astype(f32)
    shifted = x - jnp.mean(x, axis=1, keepdims=True)
    inv_std = lax.rsqrt(jnp.mean(shifted * shifted, axis=1, keepdims=True) + EPS)
    normed = shifted * inv_std
    first = (normed * norm_ref[0:1, :] + norm_ref[1:2, :]).astype(low)
    first_ref[...] = first
    second_ref[...] = (normed * norm_ref[2:3, :] + norm_ref[3:4, :]).astype(low)
    projected = dot(first, wq_ref[...], NN) + bq_ref[...]
    tables = rotary_rows(table_ref, pl.program_id(0))
    lane = lax.broadcasted_iota(jnp.int32, (BLOCK, padded), 1)
    extra = (lane >= width) & (lane < width + 3)
    qkv_ref[:, :padded] = rotate(projected[:, :padded], tables, 1).astype(low)
    keys = rotate(projected[:, padded : 2 * padded], tables, 1)
    qkv_ref[:, padded : 2 * padded] = jnp.where(extra, 1.0, keys).astype(low)
    qkv_ref[:, 2 * padded :] = jnp.where(extra, 1.0, projected[:, 2 * padded :]).astype(low)


def front(width, x, norms, wq, bq, table):
    rows, d = x.shape
    full = lambda a: pl.BlockSpec(a.shape, lambda r: (0,) * a.ndim)
    block = lambda w: pl.BlockSpec((BLOCK, w), lambda r: (r, 0))
    return pl.pallas_call(
        functools.partial(front_kernel, width),
        name="front",
        grid=(rows // BLOCK,),
        in_specs=[block(d), full(norms), full(wq), full(bq), full(table)],
        out_specs=[block(d), block(d), block(wq.shape[1])],
        out_shape=[
            jax.ShapeDtypeStruct((rows, d), low),
            jax.ShapeDtypeStruct((rows, d), low),
            jax.ShapeDtypeStruct((rows, wq.shape[1]), low),
        ],
        compiler_params=pltpu.CompilerParams(vmem_limit_bytes=VMEM),
    )(x, norms, wq, bq, table)


def attend_kernel(width, qkv_ref, context_ref, qx_ref, vm_ref, scores_ref):
    heads = width // HD
    rows = qkv_ref.shape[0]
    padded = qkv_ref.shape[1] // 3
    blocks = rows // BLOCK
    scale = HD ** (-0.5)
    step = pl.program_id(0)
    lane = lax.broadcasted_iota(jnp.int32, (BLOCK, padded), 1)
    of_head = [(lane >= h * HD) & (lane < (h + 1) * HD) for h in range(heads)]

    @pl.when(step == 0)
    def _():
        @pl.loop(0, blocks)
        def _(j):
            v = qkv_ref[pl.ds(pl.multiple_of(j * BLOCK, BLOCK), BLOCK), 2 * padded :].astype(f32)
            for h in range(heads):
                vm_ref[j, h * BLOCK : (h + 1) * BLOCK, :] = jnp.where(
                    of_head[h], v, jnp.where(lane == width + h, 1.0, 0.0)
                ).astype(low)

    q = qkv_ref[pl.ds(pl.multiple_of(step * BLOCK, BLOCK), BLOCK), :padded].astype(f32)
    query = jnp.concatenate([jnp.where(of_head[h], q, 0.0).astype(low) for h in range(heads)])

    def keys(j):
        return qkv_ref[pl.ds(pl.multiple_of(j * BLOCK, BLOCK), BLOCK), padded : 2 * padded]

    def widest(s):
        return functools.reduce(
            jnp.maximum, [s[:, c : c + LANES] for c in range(0, BLOCK, LANES)]
        )

    own = dot(query, keys(step), NT)
    row = lax.broadcasted_iota(jnp.int32, own.shape, 0) % BLOCK
    col = lax.broadcasted_iota(jnp.int32, own.shape, 1)
    own = jnp.where(col <= row, own, -1e30)

    def first_pass(j, top):
        s = dot(query, keys(j), NT)
        scores_ref[j] = s
        return jnp.maximum(top, widest(s))

    top = lax.fori_loop(0, step, first_pass, widest(own))
    top = jnp.max(top, axis=1, keepdims=True)

    def weigh(s, j):
        p = jnp.exp((s - top) * scale).astype(low)
        return functools.reduce(
            jnp.add,
            [
                dot(
                    p[h * BLOCK : (h + 1) * BLOCK],
                    vm_ref[j, h * BLOCK : (h + 1) * BLOCK, :],
                    NN,
                )
                for h in range(heads)
            ],
        )

    def second_pass(j, total):
        return total + weigh(scores_ref[j], j)

    mixed = lax.fori_loop(0, step, second_pass, weigh(own, step))
    inverse = jnp.zeros((BLOCK, padded), f32)
    for h in range(heads):
        total = mixed[:, width + h : width + h + 1]
        inverse = jnp.where(of_head[h], 1.0 / total, inverse)
        log_total = top[h * BLOCK : (h + 1) * BLOCK] + jnp.log(total) / scale
        extended = query[h * BLOCK : (h + 1) * BLOCK].astype(f32)
        for k, term in enumerate(three_terms(-log_total)):
            extended = jnp.where(lane == width + k, term, extended)
        qx_ref[0, h * BLOCK : (h + 1) * BLOCK, :] = extended.astype(low)
    context_ref[...] = (mixed * inverse).astype(low)


def attend(width, qkv):
    rows = qkv.shape[0]
    padded = qkv.shape[1] // 3
    heads = width // HD
    blocks = rows // BLOCK
    return pl.pallas_call(
        functools.partial(attend_kernel, width),
        name="attend",
        grid=(blocks,),
        in_specs=[pl.BlockSpec(qkv.shape, lambda r: (0, 0))],
        out_specs=[
            pl.BlockSpec((BLOCK, padded), lambda r: (r, 0)),
            pl.BlockSpec((1, heads * BLOCK, padded), lambda r: (r, 0, 0)),
        ],
        out_shape=[
            jax.ShapeDtypeStruct((rows, padded), low),
            jax.ShapeDtypeStruct((blocks, heads * BLOCK, padded), low),
        ],
        scratch_shapes=[
            pltpu.VMEM((blocks, heads * BLOCK, padded), low),
            pltpu.VMEM((blocks, heads * BLOCK, BLOCK), f32),
        ],
        compiler_params=pltpu.CompilerParams(vmem_limit_bytes=VMEM),
    )(qkv)


def feed_kernel(
    width, length_ref, second_ref, context_ref, cot_ref, wi_ref, wd_ref, bias_ref, norm_ref,
    branch_ref, dox_ref, back_ref, gwi_ref, gwd_ref, gbias_ref, gsmall_ref, gwi_sum, gwd_sum,
):
    heads = width // HD
    padded = context_ref.shape[1]
    hidden = wi_ref.shape[1]
    step = pl.program_id(0)

    @pl.when(step == 0)
    def _():
        gwi_sum[...] = jnp.zeros_like(gwi_sum)
        gwd_sum[...] = jnp.zeros_like(gwd_sum)
        gbias_ref[...] = jnp.zeros_like(gbias_ref)
        gsmall_ref[...] = jnp.zeros_like(gsmall_ref)

    second = second_ref[...]
    context = context_ref[...]
    row = lax.broadcasted_iota(jnp.int32, cot_ref.shape, 0) + step * BLOCK
    grad = jnp.where(row < length_ref[0], cot_ref[...].astype(f32), 0.0).astype(low)

    u = dot(second, wi_ref[...], NN) + bias_ref[...]
    cdf = 0.5 * (1.0 + lax.erf(u * (1.0 / math.sqrt(2.0))))
    act = (u * cdf).astype(low)
    slope = cdf + u * (jnp.exp(-0.5 * u * u) * (1.0 / math.sqrt(2.0 * math.pi)))
    both = jnp.concatenate([act, context], axis=1)
    branch_ref[...] = dot(both, wd_ref[...], NT).astype(low)

    back = dot(grad, wd_ref[...], NN)
    grad_hidden = back[:, :hidden] * slope
    gbias_ref[...] += jnp.sum(grad_hidden, axis=0, keepdims=True)
    hidden_low = grad_hidden.astype(low)
    gwi_sum[...] += dot(second, hidden_low, TN)
    gwd_sum[...] += dot(grad, both, TN)

    grad_context = back[:, hidden:].astype(low).astype(f32)
    lane = lax.broadcasted_iota(jnp.int32, grad_context.shape, 1)
    product = grad_context * context.astype(f32)
    for h in range(heads):
        inside = (lane >= h * HD) & (lane < (h + 1) * HD)
        extended = jnp.where(inside, grad_context, 0.0)
        delta = jnp.sum(jnp.where(inside, product, 0.0), axis=1, keepdims=True)
        for k, term in enumerate(three_terms(-delta)):
            extended = jnp.where(lane == width + k, term, extended)
        dox_ref[0, h * BLOCK : (h + 1) * BLOCK, :] = extended.astype(low)

    part = dot(hidden_low, wi_ref[...], NT)
    gsmall_ref[0:1, :] += jnp.sum(part * second.astype(f32), axis=0, keepdims=True)
    gsmall_ref[1:2, :] += jnp.sum(part, axis=0, keepdims=True)
    back_ref[...] = (part * norm_ref[2:3, :]).astype(low)

    @pl.when(step == pl.num_programs(0) - 1)
    def _():
        gwi_ref[...] = gwi_sum[...].astype(low)
        gwd_ref[...] = gwd_sum[...].astype(low)


def feed(width, length, second, context, cot, wi, wd, bias, norms):
    rows, d = second.shape
    padded = context.shape[1]
    heads = width // HD
    blocks = rows // BLOCK
    full = lambda a: pl.BlockSpec(a.shape, lambda r: (0,) * a.ndim)
    block = lambda w: pl.BlockSpec((BLOCK, w), lambda r: (r, 0))
    outs = [
        jax.ShapeDtypeStruct((rows, d), low),
        jax.ShapeDtypeStruct((blocks, heads * BLOCK, padded), low),
        jax.ShapeDtypeStruct((rows, d), low),
        jax.ShapeDtypeStruct(wi.shape, low),
        jax.ShapeDtypeStruct(wd.shape, low),
        jax.ShapeDtypeStruct(bias.shape, f32),
        jax.ShapeDtypeStruct((8, d), f32),
    ]
    return pl.pallas_call(
        functools.partial(feed_kernel, width),
        name="feed",
        grid=(blocks,),
        in_specs=[
            pl.BlockSpec(memory_space=pltpu.SMEM),
            block(d), block(padded), block(d), full(wi), full(wd), full(bias), full(norms),
        ],
        out_specs=[
            block(d),
            pl.BlockSpec((1, heads * BLOCK, padded), lambda r: (r, 0, 0)),
            block(d), full(outs[3]), full(outs[4]), full(outs[5]), full(outs[6]),
        ],
        out_shape=outs,
        scratch_shapes=[pltpu.VMEM(wi.shape, f32), pltpu.VMEM(wd.shape, f32)],
        compiler_params=pltpu.CompilerParams(vmem_limit_bytes=VMEM),
    )(length, second, context, cot, wi, wd, bias, norms)


def back_kernel(
    width, qkv_ref, qx_ref, dox_ref, first_ref, part_ref, wq_ref, norm_ref, table_ref,
    gn_ref, gwq_ref, gbias_ref, gsmall_ref, keyt_ref, dqt_ref, gwq_sum,
):
    heads = width // HD
    rows = qkv_ref.shape[0]
    padded = qkv_ref.shape[1] // 3
    blocks = rows // BLOCK
    scale = HD ** (-0.5)
    step = pl.program_id(0)

    @pl.when(step == 0)
    def _():
        dqt_ref[...] = jnp.zeros_like(dqt_ref)
        gwq_sum[...] = jnp.zeros_like(gwq_sum)
        gbias_ref[...] = jnp.zeros_like(gbias_ref)
        gsmall_ref[...] = jnp.zeros_like(gsmall_ref)

    here = pl.ds(pl.multiple_of(step * BLOCK, BLOCK), BLOCK)
    keys = qkv_ref[here, padded : 2 * padded]
    values = qkv_ref[here, 2 * padded :]
    keyt_ref[...] = keys.astype(f32).T[:width].astype(low)

    def pair(i, own):
        query, dout = qx_ref[i], dox_ref[i]
        p = jnp.exp(dot(keys, query, NT) * scale)
        if own:
            key_at = lax.broadcasted_iota(jnp.int32, p.shape, 0)
            query_at = lax.broadcasted_iota(jnp.int32, p.shape, 1) % BLOCK
            p = jnp.where(key_at <= query_at, p, 0.0)
        ds = (p * dot(values, dout, NT)).astype(low)
        grad_value = dot(p.astype(low), dout, NN)
        grad_key = dot(ds, query, NN)
        for h in range(heads):
            dqt_ref[i, h * HD : (h + 1) * HD, :] += dot(
                keyt_ref[h * HD : (h + 1) * HD, :], ds[:, h * BLOCK : (h + 1) * BLOCK], NN
            )
        return grad_key, grad_value

    def later(i, carry):
        grad_key, grad_value = pair(i, False)
        return carry[0] + grad_key, carry[1] + grad_value

    grad_key, grad_value = lax.fori_loop(step + 1, blocks, later, pair(step, True))

    tables = rotary_rows(table_ref, step)
    inside = lax.broadcasted_iota(jnp.int32, (BLOCK, padded), 1) < width
    grad_query = jnp.concatenate(
        [dqt_ref[step].T, jnp.zeros((BLOCK, padded - width), f32)], axis=1
    )
    projected = jnp.concatenate(
        [
            rotate(grad_query * scale, tables, -1),
            rotate(jnp.where(inside, grad_key * scale, 0.0), tables, -1),
            jnp.where(inside, grad_value, 0.0),
        ],
        axis=1,
    )
    gbias_ref[...] += jnp.sum(projected, axis=0, keepdims=True)
    proj_low = projected.astype(low)
    first = first_ref[...]
    gwq_sum[...] += dot(first, proj_low, TN)
    part = dot(proj_low, wq_ref[...], NT)
    gsmall_ref[0:1, :] += jnp.sum(part * first.astype(f32), axis=0, keepdims=True)
    gsmall_ref[1:2, :] += jnp.sum(part, axis=0, keepdims=True)
    gn_ref[...] = (part * norm_ref[0:1, :] + part_ref[...].astype(f32)).astype(low)

    @pl.when(step == blocks - 1)
    def _():
        gwq_ref[...] = gwq_sum[...].astype(low)


def back(width, qkv, qx, dox, first, part, wq, norms, table):
    rows, d = first.shape
    padded = qkv.shape[1] // 3
    blocks = rows // BLOCK
    full = lambda a: pl.BlockSpec(a.shape, lambda r: (0,) * a.ndim)
    block = lambda w: pl.BlockSpec((BLOCK, w), lambda r: (r, 0))
    outs = [
        jax.ShapeDtypeStruct((rows, d), low),
        jax.ShapeDtypeStruct(wq.shape, low),
        jax.ShapeDtypeStruct((1, wq.shape[1]), f32),
        jax.ShapeDtypeStruct((8, d), f32),
    ]
    return pl.pallas_call(
        functools.partial(back_kernel, width),
        name="back",
        grid=(blocks,),
        in_specs=[
            full(qkv), full(qx), full(dox), block(d), block(d), full(wq), full(norms), full(table),
        ],
        out_specs=[block(d)] + [full(o) for o in outs[1:]],
        out_shape=outs,
        scratch_shapes=[
            pltpu.VMEM((width, BLOCK), low),
            pltpu.VMEM((blocks, width, BLOCK), f32),
            pltpu.VMEM(wq.shape, f32),
        ],
        compiler_params=pltpu.CompilerParams(vmem_limit_bytes=VMEM),
    )(qkv, qx, dox, first, part, wq, norms, table)


def layer_norm(values):
    shifted = values - jnp.mean(values, axis=-1, keepdims=True)
    inv_std = lax.rsqrt(jnp.mean(shifted * shifted, axis=-1, keepdims=True) + EPS)
    return shifted * inv_std, inv_std


def per_device(
    tokens, cotangent, seq_lengths, norm1_gain, norm1_bias, norm2_gain, norm2_bias,
    w_qkv, b_qkv, w_attn_out, w_in, b_in, w_down, b_out, b_down,
):
    local_rows, d = tokens.shape
    width = w_qkv.shape[2]
    padded = round_up(width + 3, LANES)
    extra = padded - width
    assert local_rows * lax.axis_size("tensor") == LMAX and seq_lengths.shape[0] == 1
    hidden = w_in.shape[1]

    gather = lambda a, axis: lax.all_gather(a, axis, axis=0, tiled=True)
    wq = jnp.pad(w_qkv, ((0, 0), (0, 0), (0, extra))).reshape(-1, 3 * padded)
    bq = jnp.pad(b_qkv, ((0, 0), (0, extra))).reshape(1, 3 * padded)
    wd = jnp.concatenate([w_down.T, jnp.pad(w_attn_out.T, ((0, 0), (0, extra)))], axis=1)
    norms = jnp.stack([norm1_gain, norm1_bias, norm2_gain, norm2_bias])
    table = jnp.asarray(rotary_base())

    x_full = gather(tokens, "tensor")
    wq_full = gather(wq, "dp")
    cot_full = gather(cotangent, "tensor")
    wi_full, wd_full = gather(w_in, "dp"), gather(wd, "dp")

    first, second, qkv = front(width, x_full, norms, wq_full, bq, table)
    context, qx = attend(width, qkv)
    branch, dox, part, gwi, gwd, gb_in, small2 = feed(
        width, seq_lengths, second, context, cot_full, wi_full, wd_full, b_in.reshape(1, -1), norms
    )
    scatter = lambda a, axis: lax.psum_scatter(a, axis, scatter_dimension=0, tiled=True).astype(f32)
    branches = scatter(branch, "tensor")
    gn, gwq, gb_qkv, small1 = back(width, qkv, qx, dox, first, part, wq_full, norms, table)
    grad_normed = scatter(gn, "tensor")
    gwi, gwd, gwq = scatter(gwi, "dp"), scatter(gwd, "dp"), scatter(gwq, "dp")

    row = lax.axis_index("tensor") * local_rows + jnp.arange(local_rows)
    row_mask = (row < seq_lengths[0]).astype(f32)[:, None]
    x = tokens.astype(f32)
    cot = cotangent.astype(f32)
    output = x + row_mask * (branches + b_out + b_down)
    normed, inv_std = layer_norm(x)
    grad_x = cot + inv_std * (
        grad_normed
        - jnp.mean(grad_normed, axis=-1, keepdims=True)
        - normed * jnp.mean(grad_normed * normed, axis=-1, keepdims=True)
    )
    gb_qkv = gb_qkv.reshape(3, padded)[:, :width]
    small = jnp.concatenate(
        [small1[:2], small2[:2], jnp.sum(row_mask * cot, axis=0, keepdims=True)]
    )
    gb_qkv, gb_in, small = lax.psum((gb_qkv, gb_in, small), "dp")
    small = lax.psum(small, "tensor")
    small = jnp.stack(
        [
            (small[0] - norm1_bias * small[1]) / norm1_gain,
            small[1],
            (small[2] - norm2_bias * small[3]) / norm2_gain,
            small[3],
            small[4],
        ]
    )
    return (
        output,
        grad_x,
        gwq.reshape(-1, 3, padded)[:, :, :width],
        gb_qkv,
        gwd[:, hidden : hidden + width].T,
        gwi,
        gb_in.reshape(-1),
        gwd[:, :hidden].T,
        small,
    )


def solution(mesh):
    rows = P(("dp", "tensor"), None)
    placed = (
        rows, rows, P("dp"), P(), P(), P(), P(), P("dp", None, "tensor"), P(None, "tensor"),
        P("tensor", "dp"), P("dp", "tensor"), P("tensor"), P("tensor", "dp"), P(), P(),
    )
    return jax.shard_map(
        per_device,
        mesh=mesh,
        in_specs=placed,
        out_specs=(
            rows, rows, P("dp", None, "tensor"), P(None, "tensor"), P("tensor", "dp"),
            P("dp", "tensor"), P("tensor"), P("tensor", "dp"), P(),
        ),
        check_vma=False,
    )
```

```python
import functools
import math

import jax
import jax.numpy as jnp
import numpy as np
from jax import lax
from jax.experimental import pallas as pl
from jax.experimental.pallas import tpu as pltpu
from jax.sharding import PartitionSpec as P

HD = 64
ROT = 16
LMAX = 2048
LANES = 128
EPS = 1e-05
BLOCK = 256
FAST = 64
VMEM = 66 * 1024 * 1024

f32 = jnp.float32
low = jnp.bfloat16

NN = (((1,), (0,)), ((), ()))
NT = (((1,), (1,)), ((), ()))
TN = (((0,), (0,)), ((), ()))


def dot(a, b, dims):
    return lax.dot_general(a, b, dims, preferred_element_type=f32)


def round_up(n, m):
    return (n + m - 1) // m * m


def rotary_base():
    d = np.arange(LANES) % HD
    half = ROT // 2
    inverse = np.where(d < ROT, np.exp((d % half) * (-2.0 * math.log(10000.0) / ROT)), 0.0)
    slow = np.arange(0, LMAX, FAST)[:, None] * inverse
    fast = np.arange(FAST)[:, None] * inverse
    return np.concatenate([np.cos(slow), np.sin(slow), np.cos(fast), np.sin(fast)]).astype(
        np.float32
    )


def rotary_rows(table_ref, block):
    slow_rows = LMAX // FAST
    fast_cos = table_ref[2 * slow_rows : 2 * slow_rows + FAST, :]
    fast_sin = table_ref[2 * slow_rows + FAST :, :]
    cosines, sines = [], []
    for part in range(BLOCK // FAST):
        row = block * (BLOCK // FAST) + part
        slow_cos = table_ref[pl.ds(row, 1), :]
        slow_sin = table_ref[pl.ds(row + slow_rows, 1), :]
        cosines.append(slow_cos * fast_cos - slow_sin * fast_sin)
        sines.append(slow_sin * fast_cos + slow_cos * fast_sin)
    cosine, sine = jnp.concatenate(cosines), jnp.concatenate(sines)
    d = lax.broadcasted_iota(jnp.int32, cosine.shape, 1) % HD
    return (
        cosine,
        jnp.where(d < ROT // 2, -sine, 0.0),
        jnp.where((d >= ROT // 2) & (d < ROT), sine, 0.0),
    )


def rotate(values, tables, sign):
    cosine, from_right, from_left = tables
    half = ROT // 2
    turned = []
    for first in range(0, values.shape[1], LANES):
        t = values[:, first : first + LANES]
        side = (
            pltpu.roll(t, LANES - half, axis=1) * from_right
            + pltpu.roll(t, half, axis=1) * from_left
        )
        turned.append(t * cosine + side if sign > 0 else t * cosine - side)
    return jnp.concatenate(turned, axis=1)


def three_terms(value):
    first = value.astype(low).astype(f32)
    second = (value - first).astype(low).astype(f32)
    return first, second, value - first - second


def front_kernel(width, x_ref, norm_ref, wq_ref, bq_ref, table_ref, first_ref, second_ref, qkv_ref):
    padded = qkv_ref.shape[1] // 3
    x = x_ref[...].astype(f32)
    shifted = x - jnp.mean(x, axis=1, keepdims=True)
    inv_std = lax.rsqrt(jnp.mean(shifted * shifted, axis=1, keepdims=True) + EPS)
    normed = shifted * inv_std
    first = (normed * norm_ref[0:1, :] + norm_ref[1:2, :]).astype(low)
    first_ref[...] = first
    second_ref[...] = (normed * norm_ref[2:3, :] + norm_ref[3:4, :]).astype(low)
    projected = dot(first, wq_ref[...], NN) + bq_ref[...]
    tables = rotary_rows(table_ref, pl.program_id(0))
    lane = lax.broadcasted_iota(jnp.int32, (BLOCK, padded), 1)
    extra = (lane >= width) & (lane < width + 3)
    qkv_ref[:, :padded] = rotate(projected[:, :padded], tables, 1).astype(low)
    keys = rotate(projected[:, padded : 2 * padded], tables, 1)
    qkv_ref[:, padded : 2 * padded] = jnp.where(extra, 1.0, keys).astype(low)
    qkv_ref[:, 2 * padded :] = jnp.where(extra, 1.0, projected[:, 2 * padded :]).astype(low)


def front(width, x, norms, wq, bq, table):
    rows, d = x.shape
    full = lambda a: pl.BlockSpec(a.shape, lambda r: (0,) * a.ndim)
    block = lambda w: pl.BlockSpec((BLOCK, w), lambda r: (r, 0))
    return pl.pallas_call(
        functools.partial(front_kernel, width),
        name="front",
        grid=(rows // BLOCK,),
        in_specs=[block(d), full(norms), full(wq), full(bq), full(table)],
        out_specs=[block(d), block(d), block(wq.shape[1])],
        out_shape=[
            jax.ShapeDtypeStruct((rows, d), low),
            jax.ShapeDtypeStruct((rows, d), low),
            jax.ShapeDtypeStruct((rows, wq.shape[1]), low),
        ],
        compiler_params=pltpu.CompilerParams(vmem_limit_bytes=VMEM),
    )(x, norms, wq, bq, table)


def attend_kernel(width, qkv_ref, context_ref, qx_ref, vm_ref, scores_ref):
    heads = width // HD
    rows = qkv_ref.shape[0]
    padded = qkv_ref.shape[1] // 3
    blocks = rows // BLOCK
    scale = HD ** (-0.5)
    step = pl.program_id(0)
    lane = lax.broadcasted_iota(jnp.int32, (BLOCK, padded), 1)
    of_head = [(lane >= h * HD) & (lane < (h + 1) * HD) for h in range(heads)]

    @pl.when(step == 0)
    def _():
        @pl.loop(0, blocks)
        def _(j):
            v = qkv_ref[pl.ds(pl.multiple_of(j * BLOCK, BLOCK), BLOCK), 2 * padded :].astype(f32)
            for h in range(heads):
                vm_ref[j, h * BLOCK : (h + 1) * BLOCK, :] = jnp.where(
                    of_head[h], v, jnp.where(lane == width + h, 1.0, 0.0)
                ).astype(low)

    q = qkv_ref[pl.ds(pl.multiple_of(step * BLOCK, BLOCK), BLOCK), :padded].astype(f32)
    query = jnp.concatenate([jnp.where(of_head[h], q, 0.0).astype(low) for h in range(heads)])

    def keys(j):
        return qkv_ref[pl.ds(pl.multiple_of(j * BLOCK, BLOCK), BLOCK), padded : 2 * padded]

    def widest(s):
        return functools.reduce(
            jnp.maximum, [s[:, c : c + LANES] for c in range(0, BLOCK, LANES)]
        )

    own = dot(query, keys(step), NT)
    row = lax.broadcasted_iota(jnp.int32, own.shape, 0) % BLOCK
    col = lax.broadcasted_iota(jnp.int32, own.shape, 1)
    own = jnp.where(col <= row, own, -1e30)

    def first_pass(j, top):
        s = dot(query, keys(j), NT)
        scores_ref[j] = s
        return jnp.maximum(top, widest(s))

    top = lax.fori_loop(0, step, first_pass, widest(own))
    top = jnp.max(top, axis=1, keepdims=True)

    def weigh(s, j):
        p = jnp.exp((s - top) * scale).astype(low)
        return functools.reduce(
            jnp.add,
            [
                dot(
                    p[h * BLOCK : (h + 1) * BLOCK],
                    vm_ref[j, h * BLOCK : (h + 1) * BLOCK, :],
                    NN,
                )
                for h in range(heads)
            ],
        )

    def second_pass(j, total):
        return total + weigh(scores_ref[j], j)

    mixed = lax.fori_loop(0, step, second_pass, weigh(own, step))
    inverse = jnp.zeros((BLOCK, padded), f32)
    for h in range(heads):
        total = mixed[:, width + h : width + h + 1]
        inverse = jnp.where(of_head[h], 1.0 / total, inverse)
        log_total = top[h * BLOCK : (h + 1) * BLOCK] + jnp.log(total) / scale
        extended = query[h * BLOCK : (h + 1) * BLOCK].astype(f32)
        for k, term in enumerate(three_terms(-log_total)):
            extended = jnp.where(lane == width + k, term, extended)
        qx_ref[0, h * BLOCK : (h + 1) * BLOCK, :] = extended.astype(low)
    context_ref[...] = (mixed * inverse).astype(low)


def attend(width, qkv):
    rows = qkv.shape[0]
    padded = qkv.shape[1] // 3
    heads = width // HD
    blocks = rows // BLOCK
    return pl.pallas_call(
        functools.partial(attend_kernel, width),
        name="attend",
        grid=(blocks,),
        in_specs=[pl.BlockSpec(qkv.shape, lambda r: (0, 0))],
        out_specs=[
            pl.BlockSpec((BLOCK, padded), lambda r: (r, 0)),
            pl.BlockSpec((1, heads * BLOCK, padded), lambda r: (r, 0, 0)),
        ],
        out_shape=[
            jax.ShapeDtypeStruct((rows, padded), low),
            jax.ShapeDtypeStruct((blocks, heads * BLOCK, padded), low),
        ],
        scratch_shapes=[
            pltpu.VMEM((blocks, heads * BLOCK, padded), low),
            pltpu.VMEM((blocks, heads * BLOCK, BLOCK), f32),
        ],
        compiler_params=pltpu.CompilerParams(vmem_limit_bytes=VMEM),
    )(qkv)


def feed_kernel(
    width, length_ref, second_ref, context_ref, cot_ref, wi_ref, wd_ref, bias_ref, norm_ref,
    branch_ref, dox_ref, back_ref, gw_ref, gbias_ref, gsmall_ref, gwi_sum, gwd_sum,
):
    heads = width // HD
    padded = context_ref.shape[1]
    hidden = wi_ref.shape[1]
    step = pl.program_id(0)

    @pl.when(step == 0)
    def _():
        gwi_sum[...] = jnp.zeros_like(gwi_sum)
        gwd_sum[...] = jnp.zeros_like(gwd_sum)
        gbias_ref[...] = jnp.zeros_like(gbias_ref)
        gsmall_ref[...] = jnp.zeros_like(gsmall_ref)

    second = second_ref[...]
    context = context_ref[...]
    row = lax.broadcasted_iota(jnp.int32, cot_ref.shape, 0) + step * BLOCK
    grad = jnp.where(row < length_ref[0], cot_ref[...].astype(f32), 0.0).astype(low)

    u = dot(second, wi_ref[...], NN) + bias_ref[...]
    cdf = 0.5 * (1.0 + lax.erf(u * (1.0 / math.sqrt(2.0))))
    act = (u * cdf).astype(low)
    slope = cdf + u * (jnp.exp(-0.5 * u * u) * (1.0 / math.sqrt(2.0 * math.pi)))
    both = jnp.concatenate([act, context], axis=1)
    branch_ref[...] = dot(both, wd_ref[...], NT).astype(low)

    back = dot(grad, wd_ref[...], NN)
    grad_hidden = back[:, :hidden] * slope
    gbias_ref[...] += jnp.sum(grad_hidden, axis=0, keepdims=True)
    hidden_low = grad_hidden.astype(low)
    gwi_sum[...] += dot(second, hidden_low, TN)
    gwd_sum[...] += dot(grad, both, TN)

    grad_context = back[:, hidden:].astype(low).astype(f32)
    lane = lax.broadcasted_iota(jnp.int32, grad_context.shape, 1)
    product = grad_context * context.astype(f32)
    for h in range(heads):
        inside = (lane >= h * HD) & (lane < (h + 1) * HD)
        extended = jnp.where(inside, grad_context, 0.0)
        delta = jnp.sum(jnp.where(inside, product, 0.0), axis=1, keepdims=True)
        for k, term in enumerate(three_terms(-delta)):
            extended = jnp.where(lane == width + k, term, extended)
        dox_ref[0, h * BLOCK : (h + 1) * BLOCK, :] = extended.astype(low)

    part = dot(hidden_low, wi_ref[...], NT)
    gsmall_ref[0:1, :] += jnp.sum(part * second.astype(f32), axis=0, keepdims=True)
    gsmall_ref[1:2, :] += jnp.sum(part, axis=0, keepdims=True)
    back_ref[...] = (part * norm_ref[2:3, :]).astype(low)

    @pl.when(step == pl.num_programs(0) - 1)
    def _():
        side = gw_ref.shape[1]
        for block in range(gw_ref.shape[0]):
            rows_of = slice(block * side, (block + 1) * side)
            gw_ref[block, :, :hidden] = gwi_sum[rows_of, :].astype(low)
            gw_ref[block, :, hidden:] = gwd_sum[rows_of, :].astype(low)


def feed(width, length, second, context, cot, wi, wd, bias, norms):
    rows, d = second.shape
    padded = context.shape[1]
    heads = width // HD
    blocks = rows // BLOCK
    n = lax.axis_size("dp")
    full = lambda a: pl.BlockSpec(a.shape, lambda r: (0,) * len(a.shape))
    block = lambda w: pl.BlockSpec((BLOCK, w), lambda r: (r, 0))
    outs = [
        jax.ShapeDtypeStruct((rows, d), low),
        jax.ShapeDtypeStruct((blocks, heads * BLOCK, padded), low),
        jax.ShapeDtypeStruct((rows, d), low),
        jax.ShapeDtypeStruct((n, d // n, wi.shape[1] + wd.shape[1]), low),
        jax.ShapeDtypeStruct(bias.shape, f32),
        jax.ShapeDtypeStruct((8, d), f32),
    ]
    return pl.pallas_call(
        functools.partial(feed_kernel, width),
        name="feed",
        grid=(blocks,),
        in_specs=[
            pl.BlockSpec(memory_space=pltpu.SMEM),
            block(d), block(padded), block(d), full(wi), full(wd), full(bias), full(norms),
        ],
        out_specs=[
            block(d),
            pl.BlockSpec((1, heads * BLOCK, padded), lambda r: (r, 0, 0)),
            block(d), full(outs[3]), full(outs[4]), full(outs[5]),
        ],
        out_shape=outs,
        scratch_shapes=[pltpu.VMEM(wi.shape, f32), pltpu.VMEM(wd.shape, f32)],
        compiler_params=pltpu.CompilerParams(vmem_limit_bytes=VMEM),
    )(length, second, context, cot, wi, wd, bias, norms)


MESH = pl.DeviceIdType.MESH


class Place:
    def __init__(self):
        self.dp, self.t = lax.axis_index("dp"), lax.axis_index("tensor")
        self.n, self.ways = lax.axis_size("dp"), lax.axis_size("tensor")
        self.majors = self.n // 2
        self.a, self.b = self.dp // 2, self.dp % 2
        self.chip, self.core = self.t // 2, self.t % 2
        self.near = (self.dp, self.t + 1 - 2 * self.core)
        self.across = (self.dp, (self.t + 2) % 4)
        self.beside = (self.dp + 1 - 2 * self.b, self.t)

    def major(self, k):
        return ((self.a + k) % self.majors, (self.a + k) % self.majors * 2 + self.b)

    def greet(self, everyone):
        barrier = pltpu.get_barrier_semaphore()
        others = [self.near, self.across]
        if everyone:
            others += [(self.dp, 3 - self.t)]
            others += [((self.dp + k) % self.n, self.t) for k in range(1, self.n)]
        else:
            others += [self.beside]
            others += [(self.major(k)[1], self.t) for k in range(1, self.majors)]
        for other in others:
            pl.semaphore_signal(barrier, inc=1, device_id=other, device_id_type=MESH)
        pl.semaphore_wait(barrier, len(others))


def send(src, dst, sems, k, to):
    return pltpu.make_async_remote_copy(
        src_ref=src,
        dst_ref=dst,
        send_sem=sems.at[0, k],
        recv_sem=sems.at[1, k],
        device_id=to,
        device_id_type=MESH,
    )


def plus(*terms):
    return functools.reduce(jnp.add, [t.astype(f32) for t in terms])


class Scatter:
    def __init__(self, place, mine, got, mid, last, sems):
        self.p, self.mine, self.got, self.mid, self.last = place, mine, got, mid, last
        self.pairs, self.lines = sems

    def first(self, k):
        p = self.p
        a = p.major(k)[0]
        return send(
            self.mine.at[a * 2 + 1 - p.b], self.got.at[k % p.majors], self.pairs, k % p.majors, p.beside
        )

    def second(self, k):
        return send(
            self.mid.at[k - 1], self.last.at[k - 1], self.lines, k - 1, (self.p.major(k)[1], self.p.t)
        )

    def start(self):
        for k in range(1, self.p.majors + 1):
            self.first(k).start()

    def add(self, k):
        self.first(k).wait_recv()
        self.mid[k - 1] = plus(
            self.mine[self.p.major(k)[1]], self.got[k % self.p.majors]
        ).astype(self.mid.dtype)

    def forward(self, k):
        self.second(k).start()

    def finish(self):
        p = self.p
        for k in range(1, p.majors + 1):
            self.first(k).wait_send()
        self.first(p.majors).wait_recv()
        for k in range(1, p.majors):
            self.second(k).wait()
        return plus(
            self.mine[p.dp], self.got[0], *[self.last[k] for k in range(p.majors - 1)]
        )


class Exchange:
    def __init__(self, slots, sems, me, count, device):
        self.slots, self.sems, self.me, self.count, self.device = slots, sems, me, count, device

    def copy(self, k, source):
        return pltpu.make_async_remote_copy(
            src_ref=self.slots.at[source],
            dst_ref=self.slots.at[source],
            send_sem=self.sems.at[0, k],
            recv_sem=self.sems.at[1, source],
            device_id=self.device((self.me + k) % self.count),
            device_id_type=MESH,
        )

    def start(self):
        for k in range(1, self.count):
            self.copy(k, self.me).start()

    def total(self):
        for k in range(1, self.count):
            self.copy(k, (self.me + k) % self.count).wait_recv()
        return functools.reduce(jnp.add, [self.slots[k] for k in range(self.count)])

    def finish(self):
        for k in range(1, self.count):
            self.copy(k, self.me).wait_send()


def scatter_scratch(majors, rows, columns):
    return [
        pltpu.VMEM((majors, rows, columns), low),
        pltpu.VMEM((majors - 1, rows, columns), low),
        pltpu.VMEM((majors - 1, rows, columns), low),
        pltpu.SemaphoreType.DMA((2, majors)),
        pltpu.SemaphoreType.DMA((2, majors - 1)),
    ]


def back_kernel(
    width, hidden, length_ref, qkv_ref, qx_ref, dox_ref, first_ref, part_ref, wq_ref, norm_ref,
    table_ref, branch_ref, gw_ref, gbin_ref, gpart_ref, tokens_ref, cot_ref,
    out_ref, gx_ref, gq_ref, gbq_ref, go_ref, gi_ref, gb_ref, gd_ref, small_ref,
    keyt_ref, dqt_ref, dk_ref, dv_ref, gwq_sum, gbias_sum, gsmall_sum,
    gn_ref, gn_near, gn_mid, gn_own, gn_far, gn_sem1, gn_sem2,
    br_near, br_mid, br_far, br_sem1, br_sem2,
    w_got, w_mid, w_last, w_sem1, w_sem2,
    gq_low, q_got, q_mid, q_last, q_sem1, q_sem2,
    line_ref, cross_ref, line_sem, cross_sem,
):
    heads = width // HD
    rows = qkv_ref.shape[0]
    padded = qkv_ref.shape[1] // 3
    blocks = rows // BLOCK
    local = tokens_ref.shape[0]
    per = local // BLOCK
    d = tokens_ref.shape[1]
    scale = HD ** (-0.5)
    step = pl.program_id(0)
    last = blocks - 1
    here = Place()
    weights = Scatter(here, gw_ref, w_got, w_mid, w_last, (w_sem1, w_sem2))
    final = Scatter(here, gq_low, q_got, q_mid, q_last, (q_sem1, q_sem2))

    def near_branch(chip):
        owner = chip * 2 + 1 - here.core
        return send(
            branch_ref.at[pl.ds(pl.multiple_of(owner * local, local), local)], br_near.at[chip],
            br_sem1, chip, here.near,
        )

    def far_branch():
        return send(br_mid, br_far, br_sem2, 0, here.across)

    def branch_rows(chip):
        owner = chip * 2 + here.core
        return branch_ref[pl.ds(pl.multiple_of(owner * local, local), local), :]

    def block_of(number):
        return number // 2 + number % 2 * (blocks - 1 - number // 2 * 2)

    def near_block(r):
        slot = r // per // 2 * per + r % per
        return send(gn_ref.at[r], gn_near.at[slot], gn_sem1, slot, here.near)

    def far_block(r):
        return send(gn_mid.at[r % per], gn_far.at[r % per], gn_sem2, r % per, here.across)

    def collect(r):
        owner = r // per

        @pl.when(owner % 2 == here.core)
        def _():
            near_block(r).wait_recv()
            total = plus(gn_ref[r], gn_near[owner // 2 * per + r % per])

            @pl.when(owner // 2 == here.chip)
            def _():
                gn_own[r % per] = total

            @pl.when(owner // 2 != here.chip)
            def _():
                gn_mid[r % per] = total.astype(low)

    def pass_on(r):
        owner = r // per

        @pl.when((owner % 2 == here.core) & (owner // 2 != here.chip))
        def _():
            far_block(r).start()

    @pl.when(step == 0)
    def _():
        here.greet(True)
        weights.start()
        for chip in range(2):
            near_branch(chip).start()
        dqt_ref[...] = jnp.zeros_like(dqt_ref)
        dk_ref[...] = jnp.zeros_like(dk_ref)
        dv_ref[...] = jnp.zeros_like(dv_ref)
        gwq_sum[...] = jnp.zeros_like(gwq_sum)
        gbias_sum[...] = jnp.zeros_like(gbias_sum)
        gsmall_sum[...] = jnp.zeros_like(gsmall_sum)

        @pl.loop(0, blocks)
        def _(j):
            k = qkv_ref[pl.ds(pl.multiple_of(j * BLOCK, BLOCK), BLOCK), padded : 2 * padded]
            keyt_ref[j] = k.astype(f32).T[:width].astype(low)

    @pl.when(step == 1)
    def _():
        for chip in range(2):
            near_branch(chip).wait_recv()
        br_mid[...] = plus(branch_rows(1 - here.chip), br_near[1 - here.chip]).astype(low)

    for k in range(1, here.majors):

        @pl.when(step == min(k, last - 2))
        def _():
            weights.add(k)

    @pl.when(step > 0)
    def _():
        collect(block_of(step - 1))

    def pair(i, j, own):
        at = pl.ds(pl.multiple_of(j * BLOCK, BLOCK), BLOCK)
        keys, values = qkv_ref[at, padded : 2 * padded], qkv_ref[at, 2 * padded :]
        query, dout = qx_ref[i], dox_ref[i]
        p = jnp.exp(dot(keys, query, NT) * scale)
        if own:
            key_at = lax.broadcasted_iota(jnp.int32, p.shape, 0)
            query_at = lax.broadcasted_iota(jnp.int32, p.shape, 1) % BLOCK
            p = jnp.where(key_at <= query_at, p, 0.0)
        ds = (p * dot(values, dout, NT)).astype(low)
        dv_ref[j] += dot(p.astype(low), dout, NN)
        dk_ref[j] += dot(ds, query, NN)
        for h in range(heads):
            dqt_ref[i, h * HD : (h + 1) * HD, :] += dot(
                keyt_ref[j, h * HD : (h + 1) * HD, :], ds[:, h * BLOCK : (h + 1) * BLOCK], NN
            )

    turn = step // 2
    odd = step % 2
    now = block_of(step)

    @pl.loop(0, last - step)
    def _(number):
        other = turn + 1 + number
        pair(other + odd * (last - turn - other), turn + odd * (other - turn), False)

    @pl.when(step == 1)
    def _():
        far_branch().start()

    for k in range(1, here.majors):

        @pl.when(step == min(k, last - 2))
        def _():
            weights.forward(k)

    @pl.when(step > 0)
    def _():
        pass_on(block_of(step - 1))

    pair(now, now, True)

    tables = rotary_rows(table_ref, now)
    inside = lax.broadcasted_iota(jnp.int32, (BLOCK, padded), 1) < width
    grad_query = jnp.concatenate([dqt_ref[now].T, jnp.zeros((BLOCK, padded - width), f32)], axis=1)
    projected = jnp.concatenate(
        [
            rotate(grad_query * scale, tables, -1),
            rotate(jnp.where(inside, dk_ref[now] * scale, 0.0), tables, -1),
            jnp.where(inside, dv_ref[now], 0.0),
        ],
        axis=1,
    )
    gbias_sum[...] += jnp.sum(projected, axis=0, keepdims=True)
    proj_low = projected.astype(low)
    at = pl.ds(pl.multiple_of(now * BLOCK, BLOCK), BLOCK)
    first = first_ref[at, :]
    gwq_sum[...] += dot(first, proj_low, TN)
    part = dot(proj_low, wq_ref[...], NT)
    gsmall_sum[0:1, :] += jnp.sum(part * first.astype(f32), axis=0, keepdims=True)
    gsmall_sum[1:2, :] += jnp.sum(part, axis=0, keepdims=True)
    gn_ref[now] = (part * norm_ref[0:1, :] + part_ref[at, :].astype(f32)).astype(low)

    @pl.when(now // per % 2 != here.core)
    def _():
        near_block(now).start()

    row = lax.broadcasted_iota(jnp.int32, (local, d), 0) + here.t * local
    kept = row < length_ref[0]

    @pl.when(step == last - 1)
    def _():
        far_branch().wait()
        for chip in range(2):
            near_branch(chip).wait_send()
        total = plus(branch_rows(here.chip), br_near[here.chip], br_far[...])
        total = total + (norm_ref[4:5, :] + norm_ref[5:6, :])
        out_ref[...] = tokens_ref[...].astype(f32) + jnp.where(kept, total, 0.0)

    @pl.when(step == last)
    def _():
        side = gwq_sum.shape[0] // here.n
        for block in range(here.n):
            rows_of = slice(block * side, (block + 1) * side)
            gq_low[block] = jnp.concatenate(
                [gwq_sum[rows_of, k * padded : k * padded + width] for k in range(3)], axis=1
            ).astype(low)
        cot = cot_ref[...].astype(f32)
        dense = jnp.sum(jnp.where(kept, cot, 0.0), axis=0, keepdims=True)
        line_ref[here.dp] = jnp.concatenate(
            [gbias_sum[...], gbin_ref[...], gsmall_sum[0:2, :], gpart_ref[0:2, :], dense, dense]
        )
        final.start()

        line = Exchange(line_ref, line_sem, here.dp, here.n, lambda to: (to, here.t))
        cross = Exchange(cross_ref, cross_sem, here.t, here.ways, lambda to: (here.dp, to))
        line.start()
        collect(now)
        x = tokens_ref[...].astype(f32)
        shifted = x - jnp.mean(x, axis=1, keepdims=True)
        inv_std = lax.rsqrt(jnp.mean(shifted * shifted, axis=1, keepdims=True) + EPS)
        normed = shifted * inv_std
        pass_on(now)

        total = weights.finish()
        gi_ref[...] = total[:, :hidden]
        gd_ref[...] = total[:, hidden : 2 * hidden].T
        go_ref[...] = total[:, 2 * hidden : 2 * hidden + width].T

        for k in range(1, here.majors):
            final.add(k)
            final.forward(k)
        summed = line.total()
        gbq_ref[...] = summed[0:1, :]
        gb_ref[...] = summed[1:2, :]
        cross_ref[here.t] = summed
        for k in range(per):
            far_block(k).wait()
        for slot in range(2 * per):
            near_block(slot // per * 2 * per + (1 - here.core) * per + slot % per).wait_send()
        grad_normed = jnp.concatenate([gn_own[k] + gn_far[k].astype(f32) for k in range(per)])
        cross.start()
        gx_ref[...] = cot + inv_std * (
            grad_normed
            - jnp.mean(grad_normed, axis=1, keepdims=True)
            - normed * jnp.mean(grad_normed * normed, axis=1, keepdims=True)
        )
        summed = cross.total()
        for k in range(2):
            product, plain = summed[2 + 2 * k : 3 + 2 * k, :], summed[3 + 2 * k : 4 + 2 * k, :]
            gain, bias = norm_ref[2 * k : 2 * k + 1, :], norm_ref[2 * k + 1 : 2 * k + 2, :]
            small_ref[2 * k : 2 * k + 1, :] = (product - bias * plain) / gain
            small_ref[2 * k + 1 : 2 * k + 2, :] = plain
        small_ref[4:5, :] = summed[6:7, :]
        line.finish()
        cross.finish()
        gq_ref[...] = final.finish()


def back(width, length, qkv, qx, dox, first, part, wq, norms, table, branch, gw, gb_in, gpart, tokens, cot):
    rows, d = first.shape
    padded = qkv.shape[1] // 3
    blocks = rows // BLOCK
    local = tokens.shape[0]
    per = local // BLOCK
    n, side, columns = gw.shape
    hidden = gb_in.shape[1]
    majors = n // 2
    ways = lax.axis_size("tensor")
    assert ways == 4 and 3 * padded == d == hidden and side * n == d
    full = lambda a: pl.BlockSpec(
        a.shape, lambda r: (0,) * len(a.shape), pipeline_mode=pl.Buffered(1)
    )
    outs = [
        jax.ShapeDtypeStruct((local, d), f32),
        jax.ShapeDtypeStruct((local, d), f32),
        jax.ShapeDtypeStruct((side, 3 * width), f32),
        jax.ShapeDtypeStruct((1, 3 * padded), f32),
        jax.ShapeDtypeStruct((width, side), f32),
        jax.ShapeDtypeStruct((side, hidden), f32),
        jax.ShapeDtypeStruct((1, hidden), f32),
        jax.ShapeDtypeStruct((hidden, side), f32),
        jax.ShapeDtypeStruct((5, d), f32),
    ]
    args = (qkv, qx, dox, first, part, wq, norms, table, branch, gw, gb_in, gpart, tokens, cot)
    return pl.pallas_call(
        functools.partial(back_kernel, width, hidden),
        name="back",
        grid=(blocks,),
        in_specs=[pl.BlockSpec(memory_space=pltpu.SMEM)] + [full(a) for a in args],
        out_specs=[pl.BlockSpec(memory_space=pltpu.VMEM)] * len(outs),
        out_shape=outs,
        scratch_shapes=[
            pltpu.VMEM((blocks, width, BLOCK), low),
            pltpu.VMEM((blocks, width, BLOCK), f32),
            pltpu.VMEM((blocks, BLOCK, padded), f32),
            pltpu.VMEM((blocks, BLOCK, padded), f32),
            pltpu.VMEM(wq.shape, f32),
            pltpu.VMEM((1, 3 * padded), f32),
            pltpu.VMEM((8, d), f32),
            pltpu.VMEM((blocks, BLOCK, d), low),
            pltpu.VMEM((2 * per, BLOCK, d), low),
            pltpu.VMEM((per, BLOCK, d), low),
            pltpu.VMEM((per, BLOCK, d), f32),
            pltpu.VMEM((per, BLOCK, d), low),
            pltpu.SemaphoreType.DMA((2, 2 * per)),
            pltpu.SemaphoreType.DMA((2, per)),
            pltpu.VMEM((2, local, d), low),
            pltpu.VMEM((local, d), low),
            pltpu.VMEM((local, d), low),
            pltpu.SemaphoreType.DMA((2, 2)),
            pltpu.SemaphoreType.DMA((2, 1)),
        ]
        + scatter_scratch(majors, side, columns)
        + [pltpu.VMEM((n, side, 3 * width), low)]
        + scatter_scratch(majors, side, 3 * width)
        + [
            pltpu.VMEM((n, 8, d), f32),
            pltpu.VMEM((ways, 8, d), f32),
            pltpu.SemaphoreType.DMA((2, n)),
            pltpu.SemaphoreType.DMA((2, ways)),
        ],
        compiler_params=pltpu.CompilerParams(
            vmem_limit_bytes=VMEM, collective_id=2, has_side_effects=True
        ),
    )(length, *args)


def per_device(
    tokens, cotangent, seq_lengths, norm1_gain, norm1_bias, norm2_gain, norm2_bias,
    w_qkv, b_qkv, w_attn_out, w_in, b_in, w_down, b_out, b_down,
):
    local_rows, d = tokens.shape
    width = w_qkv.shape[2]
    padded = round_up(width + 3, LANES)
    extra = padded - width
    assert local_rows * lax.axis_size("tensor") == LMAX and seq_lengths.shape[0] == 1
    hidden = w_in.shape[1]

    gather = lambda a, axis: lax.all_gather(a, axis, axis=0, tiled=True)
    wq = jnp.pad(w_qkv, ((0, 0), (0, 0), (0, extra))).reshape(-1, 3 * padded)
    bq = jnp.pad(b_qkv, ((0, 0), (0, extra))).reshape(1, 3 * padded)
    wd = jnp.concatenate([w_down.T, jnp.pad(w_attn_out.T, ((0, 0), (0, extra)))], axis=1)
    norms = jnp.stack([norm1_gain, norm1_bias, norm2_gain, norm2_bias, b_out, b_down])
    table = jnp.asarray(rotary_base())

    x_full = gather(tokens, "tensor")
    wq_full = gather(wq, "dp")
    cot_full = gather(cotangent, "tensor")
    wi_full, wd_full = gather(w_in, "dp"), gather(wd, "dp")

    first, second, qkv = front(width, x_full, norms, wq_full, bq, table)
    context, qx = attend(width, qkv)
    branch, dox, part, gw, gb_in, gpart = feed(
        width, seq_lengths, second, context, cot_full, wi_full, wd_full, b_in.reshape(1, -1), norms
    )
    output, grad_x, gq, gb_qkv, g_out, g_in, gb_in, g_down, small = back(
        width, seq_lengths, qkv, qx, dox, first, part, wq_full, norms, table, branch, gw, gb_in, gpart,
        tokens, cotangent,
    )
    return (
        output,
        grad_x,
        gq.reshape(-1, 3, width),
        gb_qkv.reshape(3, padded)[:, :width],
        g_out,
        g_in,
        gb_in.reshape(-1),
        g_down,
        small,
    )


def solution(mesh):
    rows = P(("dp", "tensor"), None)
    placed = (
        rows, rows, P("dp"), P(), P(), P(), P(), P("dp", None, "tensor"), P(None, "tensor"),
        P("tensor", "dp"), P("dp", "tensor"), P("tensor"), P("tensor", "dp"), P(), P(),
    )
    return jax.shard_map(
        per_device,
        mesh=mesh,
        in_specs=placed,
        out_specs=(
            rows, rows, P("dp", None, "tensor"), P(None, "tensor"), P("tensor", "dp"),
            P("dp", "tensor"), P("tensor"), P("tensor", "dp"), P(),
        ),
        check_vma=False,
    )
```

```python
import functools
import math

import jax
import jax.numpy as jnp
import numpy as np
from jax import lax
from jax.experimental import pallas as pl
from jax.experimental.pallas import tpu as pltpu
from jax.sharding import PartitionSpec as P

HD = 64
ROT = 16
LMAX = 2048
LANES = 128
EPS = 1e-05
BLOCK = 256
FAST = 64
VMEM = 66 * 1024 * 1024

f32 = jnp.float32
low = jnp.bfloat16

NN = (((1,), (0,)), ((), ()))
NT = (((1,), (1,)), ((), ()))
TN = (((0,), (0,)), ((), ()))


def dot(a, b, dims):
    return lax.dot_general(a, b, dims, preferred_element_type=f32)


def round_up(n, m):
    return (n + m - 1) // m * m


def rotary_base():
    d = np.arange(LANES) % HD
    half = ROT // 2
    inverse = np.where(d < ROT, np.exp((d % half) * (-2.0 * math.log(10000.0) / ROT)), 0.0)
    slow = np.arange(0, LMAX, FAST)[:, None] * inverse
    fast = np.arange(FAST)[:, None] * inverse
    return np.concatenate([np.cos(slow), np.sin(slow), np.cos(fast), np.sin(fast)]).astype(
        np.float32
    )


def rotary_rows(table_ref, block):
    slow_rows = LMAX // FAST
    fast_cos = table_ref[2 * slow_rows : 2 * slow_rows + FAST, :]
    fast_sin = table_ref[2 * slow_rows + FAST :, :]
    cosines, sines = [], []
    for part in range(BLOCK // FAST):
        row = block * (BLOCK // FAST) + part
        slow_cos = table_ref[pl.ds(row, 1), :]
        slow_sin = table_ref[pl.ds(row + slow_rows, 1), :]
        cosines.append(slow_cos * fast_cos - slow_sin * fast_sin)
        sines.append(slow_sin * fast_cos + slow_cos * fast_sin)
    cosine, sine = jnp.concatenate(cosines), jnp.concatenate(sines)
    d = lax.broadcasted_iota(jnp.int32, cosine.shape, 1) % HD
    return (
        cosine,
        jnp.where(d < ROT // 2, -sine, 0.0),
        jnp.where((d >= ROT // 2) & (d < ROT), sine, 0.0),
    )


def rotate(values, tables, sign):
    cosine, from_right, from_left = tables
    half = ROT // 2
    turned = []
    for first in range(0, values.shape[1], LANES):
        t = values[:, first : first + LANES]
        side = (
            pltpu.roll(t, LANES - half, axis=1) * from_right
            + pltpu.roll(t, half, axis=1) * from_left
        )
        turned.append(t * cosine + side if sign > 0 else t * cosine - side)
    return jnp.concatenate(turned, axis=1)


def three_terms(value):
    first = value.astype(low).astype(f32)
    second = (value - first).astype(low).astype(f32)
    return first, second, value - first - second


MESH = pl.DeviceIdType.MESH


class Place:
    def __init__(self):
        self.dp, self.t = lax.axis_index("dp"), lax.axis_index("tensor")
        self.n, self.ways = lax.axis_size("dp"), lax.axis_size("tensor")
        self.majors = self.n // 2
        self.a, self.b = self.dp // 2, self.dp % 2
        self.chip, self.core = self.t // 2, self.t % 2
        self.near = (self.dp, self.t + 1 - 2 * self.core)
        self.across = (self.dp, (self.t + 2) % 4)
        self.beside = (self.dp + 1 - 2 * self.b, self.t)

    def major(self, k):
        return ((self.a + k) % self.majors, (self.a + k) % self.majors * 2 + self.b)

    def greet(self, everyone):
        barrier = pltpu.get_barrier_semaphore()
        others = [self.near, self.across]
        if everyone:
            others += [(self.dp, 3 - self.t)]
            others += [((self.dp + k) % self.n, self.t) for k in range(1, self.n)]
        else:
            others += [self.beside]
            others += [(self.major(k)[1], self.t) for k in range(1, self.majors)]
        for other in others:
            pl.semaphore_signal(barrier, inc=1, device_id=other, device_id_type=MESH)
        pl.semaphore_wait(barrier, len(others))


def send(src, dst, sems, k, to):
    return pltpu.make_async_remote_copy(
        src_ref=src,
        dst_ref=dst,
        send_sem=sems.at[0, k],
        recv_sem=sems.at[1, k],
        device_id=to,
        device_id_type=MESH,
    )


def plus(*terms):
    return functools.reduce(jnp.add, [t.astype(f32) for t in terms])


class Scatter:
    def __init__(self, place, mine, got, mid, last, sems):
        self.p, self.mine, self.got, self.mid, self.last = place, mine, got, mid, last
        self.pairs, self.lines = sems

    def first(self, k):
        p = self.p
        a = p.major(k)[0]
        return send(
            self.mine.at[a * 2 + 1 - p.b], self.got.at[k % p.majors], self.pairs, k % p.majors, p.beside
        )

    def second(self, k):
        return send(
            self.mid.at[k - 1], self.last.at[k - 1], self.lines, k - 1, (self.p.major(k)[1], self.p.t)
        )

    def start(self):
        for k in range(1, self.p.majors + 1):
            self.first(k).start()

    def add(self, k):
        self.first(k).wait_recv()
        self.mid[k - 1] = plus(
            self.mine[self.p.major(k)[1]], self.got[k % self.p.majors]
        ).astype(self.mid.dtype)

    def forward(self, k):
        self.second(k).start()

    def finish(self):
        p = self.p
        for k in range(1, p.majors + 1):
            self.first(k).wait_send()
        self.first(p.majors).wait_recv()
        for k in range(1, p.majors):
            self.second(k).wait()
        return plus(
            self.mine[p.dp], self.got[0], *[self.last[k] for k in range(p.majors - 1)]
        )


class Gather:
    def __init__(self, place, mine, whole, sems):
        self.p, self.mine, self.whole, self.lines, self.pairs = place, mine, whole, *sems

    def line(self, k):
        p = self.p
        return send(self.mine, self.whole.at[p.dp], self.lines, k - 1, (p.major(k)[1], p.t))

    def pair(self, k):
        p = self.p
        if k == 0:
            return send(self.mine, self.whole.at[p.dp], self.pairs, 0, p.beside)
        block = self.whole.at[p.major(p.majors - k)[1]]
        return send(block, block, self.pairs, k, p.beside)

    def start(self):
        self.pair(0).start()
        for k in range(1, self.p.majors):
            self.line(k).start()

    def forward(self, k):
        self.line(k).wait_recv()
        self.pair(k).start()

    def arrived(self):
        for k in range(self.p.majors):
            self.pair(k).wait_recv()

    def finish(self):
        for k in range(self.p.majors):
            self.pair(k).wait_send()
        for k in range(1, self.p.majors):
            self.line(k).wait_send()


def gather_scratch(majors):
    return [pltpu.SemaphoreType.DMA((2, majors - 1)), pltpu.SemaphoreType.DMA((2, majors))]


class Rows:
    def __init__(self, place, mine, whole, chunks, sems):
        self.p, self.mine, self.whole, self.chunks, self.sems = place, mine, whole, chunks, sems
        self.size = mine.shape[0] // chunks

    def copy(self, kind, c):
        p = self.p
        at = pl.ds(c * self.size, self.size)
        if kind == 2:
            block = self.whole.at[p.across[1], at]
            return send(block, block, self.sems, 2 * self.chunks + c, p.near)
        to = p.near if kind == 0 else p.across
        return send(self.mine.at[at], self.whole.at[p.t, at], self.sems, kind * self.chunks + c, to)

    def start(self):
        for c in range(self.chunks):
            for kind in range(2):
                self.copy(kind, c).start()

    def arrived(self, kind, c):
        self.copy(kind, c).wait_recv()

    def forward(self, c):
        self.copy(1, c).wait_recv()
        self.copy(2, c).start()

    def finish(self):
        for c in range(self.chunks):
            for kind in range(3):
                self.copy(kind, c).wait_send()


def rows_scratch(chunks):
    return pltpu.SemaphoreType.DMA((2, 3 * chunks))


class Exchange:
    def __init__(self, slots, sems, me, count, device):
        self.slots, self.sems, self.me, self.count, self.device = slots, sems, me, count, device

    def copy(self, k, source):
        return pltpu.make_async_remote_copy(
            src_ref=self.slots.at[source],
            dst_ref=self.slots.at[source],
            send_sem=self.sems.at[0, k],
            recv_sem=self.sems.at[1, source],
            device_id=self.device((self.me + k) % self.count),
            device_id_type=MESH,
        )

    def start(self):
        for k in range(1, self.count):
            self.copy(k, self.me).start()

    def total(self):
        for k in range(1, self.count):
            self.copy(k, (self.me + k) % self.count).wait_recv()
        return functools.reduce(jnp.add, [self.slots[k] for k in range(self.count)])

    def finish(self):
        for k in range(1, self.count):
            self.copy(k, self.me).wait_send()


def scatter_scratch(majors, rows, columns):
    return [
        pltpu.VMEM((majors, rows, columns), low),
        pltpu.VMEM((majors - 1, rows, columns), low),
        pltpu.VMEM((majors - 1, rows, columns), low),
        pltpu.SemaphoreType.DMA((2, majors)),
        pltpu.SemaphoreType.DMA((2, majors - 1)),
    ]


def flat(blocks_ref):
    n, side, columns = blocks_ref.shape
    if side % 16 == 0:
        return blocks_ref[...].reshape(n * side, columns)
    return jnp.concatenate([blocks_ref[k].astype(f32) for k in range(n)]).astype(low)


def front_kernel(
    width, x_ref, wq_ref, norm_ref, bq_ref, table_ref, first_out, second_out, qkv_out, wq_out,
    x_all, wq_all, first_ref, second_ref, qkv_ref, x_sems, wq_lines, wq_pairs, own_sems, out_sems,
):
    padded = qkv_ref.shape[2] // 3
    per = x_ref.shape[0] // BLOCK
    here = Place()
    here.greet(False)
    rows = Rows(here, x_ref, x_all, per, x_sems)
    weights = Gather(here, wq_ref, wq_all, (wq_lines, wq_pairs))
    rows.start()
    weights.start()
    own = [
        pltpu.make_async_copy(x_ref, x_all.at[here.t], own_sems.at[0]),
        pltpu.make_async_copy(wq_ref, wq_all.at[here.dp], own_sems.at[1]),
    ]
    for copy in own:
        copy.start()

    def shard(kind):
        return (here.chip + kind // 2) % 2 * 2 + (here.core + kind % 2) % 2

    def out(ref, target, r, k):
        at = pl.ds(pl.multiple_of(r * BLOCK, BLOCK), BLOCK)
        return pltpu.make_async_copy(ref.at[r], target.at[at], out_sems.at[k, r])

    def norm(kind, c):
        x = x_all[shard(kind), pl.ds(pl.multiple_of(c * BLOCK, BLOCK), BLOCK), :].astype(f32)
        shifted = x - jnp.mean(x, axis=1, keepdims=True)
        inv_std = lax.rsqrt(jnp.mean(shifted * shifted, axis=1, keepdims=True) + EPS)
        normed = shifted * inv_std
        r = shard(kind) * per + c
        first_ref[r] = (normed * norm_ref[0:1, :] + norm_ref[1:2, :]).astype(low)
        second_ref[r] = (normed * norm_ref[2:3, :] + norm_ref[3:4, :]).astype(low)

    def project(kind, c):
        r = shard(kind) * per + c
        projected = dot(first_ref[r], flat(wq_all), NN) + bq_ref[...]
        tables = rotary_rows(table_ref, r)
        lane = lax.broadcasted_iota(jnp.int32, (BLOCK, padded), 1)
        extra = (lane >= width) & (lane < width + 3)
        qkv_ref[r, :, :padded] = rotate(projected[:, :padded], tables, 1).astype(low)
        keys = rotate(projected[:, padded : 2 * padded], tables, 1)
        qkv_ref[r, :, padded : 2 * padded] = jnp.where(extra, 1.0, keys).astype(low)
        values = projected[:, 2 * padded :]
        qkv_ref[r, :, 2 * padded :] = jnp.where(extra, 1.0, values).astype(low)
        out(first_ref, first_out, r, 0).start()
        out(second_ref, second_out, r, 1).start()
        out(qkv_ref, qkv_out, r, 2).start()

    own[0].wait()

    @pl.loop(0, per)
    def _(c):
        norm(0, c)

    for c in range(per):
        rows.arrived(0, c)

    @pl.loop(0, per)
    def _(c):
        norm(1, c)

    for c in range(per - 1):
        rows.forward(c)
        norm(2, c)
    for k in range(1, here.majors):
        weights.forward(k)
    for c in range(per - 1):
        rows.arrived(2, c)
        norm(3, c)
    own[1].wait()
    weights.arrived()

    @pl.loop(0, per)
    def _(c):
        project(0, c)

    rows.forward(per - 1)

    @pl.loop(0, per + 2 * (per - 1))
    def _(number):
        later = number // per
        project(1 + later + number % per * later, number % per * (1 - later))

    norm(2, per - 1)
    project(2, per - 1)
    rows.arrived(2, per - 1)
    norm(3, per - 1)
    project(3, per - 1)
    copy = pltpu.make_async_copy(wq_all, wq_out, own_sems.at[2])
    copy.start()
    copy.wait()

    @pl.loop(0, 4 * per)
    def _(r):
        out(first_ref, first_out, r, 0).wait()
        out(second_ref, second_out, r, 1).wait()
        out(qkv_ref, qkv_out, r, 2).wait()

    rows.finish()
    weights.finish()


def front(width, x, wq, norms, bq, table):
    local, d = x.shape
    side, columns = wq.shape
    n = lax.axis_size("dp")
    ways = lax.axis_size("tensor")
    rows = local * ways
    blocks = rows // BLOCK
    assert ways == 4 and local // BLOCK == 2
    vmem = pl.BlockSpec(memory_space=pltpu.VMEM)
    hbm = pl.BlockSpec(memory_space=pl.ANY)
    return pl.pallas_call(
        functools.partial(front_kernel, width),
        name="front",
        in_specs=[vmem] * 5,
        out_specs=[hbm] * 4,
        out_shape=[
            jax.ShapeDtypeStruct((rows, d), low),
            jax.ShapeDtypeStruct((rows, d), low),
            jax.ShapeDtypeStruct((rows, columns), low),
            jax.ShapeDtypeStruct((n, side, columns), low),
        ],
        scratch_shapes=[
            pltpu.VMEM((ways, local, d), low),
            pltpu.VMEM((n, side, columns), low),
            pltpu.VMEM((blocks, BLOCK, d), low),
            pltpu.VMEM((blocks, BLOCK, d), low),
            pltpu.VMEM((blocks, BLOCK, columns), low),
            rows_scratch(local // BLOCK),
        ]
        + gather_scratch(n // 2)
        + [pltpu.SemaphoreType.DMA((3,)), pltpu.SemaphoreType.DMA((3, blocks))],
        compiler_params=pltpu.CompilerParams(
            vmem_limit_bytes=VMEM, collective_id=0, has_side_effects=True
        ),
    )(x, wq, norms, bq, table)


def attend_kernel(
    width, qkv_ref, wi_ref, wd_ref, cot_ref, context_ref, qx_ref, wi_out, wd_out, cot_out,
    vm_ref, scores_ref, cot_sems, wi_lines, wi_pairs, wd_lines, wd_pairs, own_sems,
):
    heads = width // HD
    rows = qkv_ref.shape[0]
    padded = qkv_ref.shape[1] // 3
    blocks = rows // BLOCK
    scale = HD ** (-0.5)
    step = pl.program_id(0)
    lane = lax.broadcasted_iota(jnp.int32, (BLOCK, padded), 1)
    of_head = [(lane >= h * HD) & (lane < (h + 1) * HD) for h in range(heads)]
    here = Place()
    cots = Rows(here, cot_ref, cot_out, 2, cot_sems)
    inner = Gather(here, wi_ref, wi_out, (wi_lines, wi_pairs))
    down = Gather(here, wd_ref, wd_out, (wd_lines, wd_pairs))
    copies = [
        pltpu.make_async_copy(wi_ref, wi_out.at[here.dp], own_sems.at[0]),
        pltpu.make_async_copy(wd_ref, wd_out.at[here.dp], own_sems.at[1]),
        pltpu.make_async_copy(cot_ref, cot_out.at[here.t], own_sems.at[2]),
    ]

    @pl.when(step == 0)
    def _():
        here.greet(False)
        inner.start()
        down.start()
        cots.start()
        for copy in copies:
            copy.start()

        @pl.loop(0, blocks)
        def _(j):
            v = qkv_ref[pl.ds(pl.multiple_of(j * BLOCK, BLOCK), BLOCK), 2 * padded :].astype(f32)
            for h in range(heads):
                vm_ref[j, h * BLOCK : (h + 1) * BLOCK, :] = jnp.where(
                    of_head[h], v, jnp.where(lane == width + h, 1.0, 0.0)
                ).astype(low)

    for k in range(1, here.majors):

        @pl.when(step == blocks - 3)
        def _():
            inner.forward(k)

    @pl.when(step == blocks - 2)
    def _():
        cots.forward(0)

    for k in range(1, here.majors - 1):

        @pl.when(step == blocks - 1)
        def _():
            down.forward(k)

    q = qkv_ref[pl.ds(pl.multiple_of(step * BLOCK, BLOCK), BLOCK), :padded].astype(f32)
    query = jnp.concatenate([jnp.where(of_head[h], q, 0.0).astype(low) for h in range(heads)])

    def keys(j):
        return qkv_ref[pl.ds(pl.multiple_of(j * BLOCK, BLOCK), BLOCK), padded : 2 * padded]

    def widest(s):
        return functools.reduce(
            jnp.maximum, [s[:, c : c + LANES] for c in range(0, BLOCK, LANES)]
        )

    own = dot(query, keys(step), NT)
    row = lax.broadcasted_iota(jnp.int32, own.shape, 0) % BLOCK
    col = lax.broadcasted_iota(jnp.int32, own.shape, 1)
    own = jnp.where(col <= row, own, -1e30)

    def first_pass(j, top):
        s = dot(query, keys(j), NT)
        scores_ref[j] = s
        return jnp.maximum(top, widest(s))

    top = lax.fori_loop(0, step, first_pass, widest(own))
    top = jnp.max(top, axis=1, keepdims=True)

    def weigh(s, j):
        p = jnp.exp((s - top) * scale).astype(low)
        return functools.reduce(
            jnp.add,
            [
                dot(
                    p[h * BLOCK : (h + 1) * BLOCK],
                    vm_ref[j, h * BLOCK : (h + 1) * BLOCK, :],
                    NN,
                )
                for h in range(heads)
            ],
        )

    def second_pass(j, total):
        return total + weigh(scores_ref[j], j)

    mixed = lax.fori_loop(0, step, second_pass, weigh(own, step))
    inverse = jnp.zeros((BLOCK, padded), f32)
    for h in range(heads):
        total = mixed[:, width + h : width + h + 1]
        inverse = jnp.where(of_head[h], 1.0 / total, inverse)
        log_total = top[h * BLOCK : (h + 1) * BLOCK] + jnp.log(total) / scale
        extended = query[h * BLOCK : (h + 1) * BLOCK].astype(f32)
        for k, term in enumerate(three_terms(-log_total)):
            extended = jnp.where(lane == width + k, term, extended)
        qx_ref[0, h * BLOCK : (h + 1) * BLOCK, :] = extended.astype(low)
    context_ref[...] = (mixed * inverse).astype(low)

    @pl.when(step == blocks - 1)
    def _():
        down.forward(here.majors - 1)
        cots.forward(1)
        for copy in copies:
            copy.wait()
        inner.arrived()
        for c in range(2):
            cots.arrived(0, c)
            cots.arrived(2, c)
        down.arrived()
        inner.finish()
        cots.finish()
        down.finish()


def attend(width, qkv, wi, wd, cot):
    rows = qkv.shape[0]
    padded = qkv.shape[1] // 3
    heads = width // HD
    blocks = rows // BLOCK
    n = lax.axis_size("dp")
    ways = lax.axis_size("tensor")
    once = lambda a: pl.BlockSpec(
        a.shape, lambda r: (0,) * len(a.shape), pipeline_mode=pl.Buffered(1)
    )
    hbm = pl.BlockSpec(memory_space=pl.ANY)
    return pl.pallas_call(
        functools.partial(attend_kernel, width),
        name="attend",
        grid=(blocks,),
        in_specs=[once(qkv), once(wi), once(wd), once(cot)],
        out_specs=[
            pl.BlockSpec((BLOCK, padded), lambda r: (r, 0)),
            pl.BlockSpec((1, heads * BLOCK, padded), lambda r: (r, 0, 0)),
            hbm,
            hbm,
            hbm,
        ],
        out_shape=[
            jax.ShapeDtypeStruct((rows, padded), low),
            jax.ShapeDtypeStruct((blocks, heads * BLOCK, padded), low),
            jax.ShapeDtypeStruct((n,) + wi.shape, low),
            jax.ShapeDtypeStruct((n,) + wd.shape, low),
            jax.ShapeDtypeStruct((ways,) + cot.shape, low),
        ],
        scratch_shapes=[
            pltpu.VMEM((blocks, heads * BLOCK, padded), low),
            pltpu.VMEM((blocks, heads * BLOCK, BLOCK), f32),
            rows_scratch(2),
        ]
        + gather_scratch(n // 2)
        + gather_scratch(n // 2)
        + [pltpu.SemaphoreType.DMA((3,))],
        compiler_params=pltpu.CompilerParams(
            vmem_limit_bytes=VMEM, collective_id=1, has_side_effects=True
        ),
    )(qkv, wi, wd, cot)


def feed_kernel(
    width, length_ref, second_ref, context_ref, cot_ref, wi_ref, wd_ref, bias_ref, norm_ref,
    branch_ref, dox_ref, back_ref, gw_ref, gbias_ref, gsmall_ref, gwi_sum, gwd_sum,
):
    heads = width // HD
    padded = context_ref.shape[1]
    hidden = wi_ref.shape[1]
    step = pl.program_id(0)

    @pl.when(step == 0)
    def _():
        gwi_sum[...] = jnp.zeros_like(gwi_sum)
        gwd_sum[...] = jnp.zeros_like(gwd_sum)
        gbias_ref[...] = jnp.zeros_like(gbias_ref)
        gsmall_ref[...] = jnp.zeros_like(gsmall_ref)

    second = second_ref[...]
    context = context_ref[...]
    row = lax.broadcasted_iota(jnp.int32, cot_ref.shape, 0) + step * BLOCK
    grad = jnp.where(row < length_ref[0], cot_ref[...].astype(f32), 0.0).astype(low)

    u = dot(second, wi_ref[...], NN) + bias_ref[...]
    cdf = 0.5 * (1.0 + lax.erf(u * (1.0 / math.sqrt(2.0))))
    act = (u * cdf).astype(low)
    slope = cdf + u * (jnp.exp(-0.5 * u * u) * (1.0 / math.sqrt(2.0 * math.pi)))
    both = jnp.concatenate([act, context], axis=1)
    branch_ref[...] = dot(both, wd_ref[...], NT).astype(low)

    back = dot(grad, wd_ref[...], NN)
    grad_hidden = back[:, :hidden] * slope
    gbias_ref[...] += jnp.sum(grad_hidden, axis=0, keepdims=True)
    hidden_low = grad_hidden.astype(low)
    gwi_sum[...] += dot(second, hidden_low, TN)
    gwd_sum[...] += dot(grad, both, TN)

    grad_context = back[:, hidden:].astype(low).astype(f32)
    lane = lax.broadcasted_iota(jnp.int32, grad_context.shape, 1)
    product = grad_context * context.astype(f32)
    for h in range(heads):
        inside = (lane >= h * HD) & (lane < (h + 1) * HD)
        extended = jnp.where(inside, grad_context, 0.0)
        delta = jnp.sum(jnp.where(inside, product, 0.0), axis=1, keepdims=True)
        for k, term in enumerate(three_terms(-delta)):
            extended = jnp.where(lane == width + k, term, extended)
        dox_ref[0, h * BLOCK : (h + 1) * BLOCK, :] = extended.astype(low)

    part = dot(hidden_low, wi_ref[...], NT)
    gsmall_ref[0:1, :] += jnp.sum(part * second.astype(f32), axis=0, keepdims=True)
    gsmall_ref[1:2, :] += jnp.sum(part, axis=0, keepdims=True)
    back_ref[...] = (part * norm_ref[2:3, :]).astype(low)

    @pl.when(step == pl.num_programs(0) - 1)
    def _():
        side = gw_ref.shape[1]
        for block in range(gw_ref.shape[0]):
            rows_of = slice(block * side, (block + 1) * side)
            gw_ref[block, :, :hidden] = gwi_sum[rows_of, :].astype(low)
            gw_ref[block, :, hidden:] = gwd_sum[rows_of, :].astype(low)


def feed(width, length, second, context, cot, wi, wd, bias, norms):
    rows, d = second.shape
    padded = context.shape[1]
    heads = width // HD
    blocks = rows // BLOCK
    n = lax.axis_size("dp")
    full = lambda a: pl.BlockSpec(a.shape, lambda r: (0,) * len(a.shape))
    block = lambda w: pl.BlockSpec((BLOCK, w), lambda r: (r, 0))
    outs = [
        jax.ShapeDtypeStruct((rows, d), low),
        jax.ShapeDtypeStruct((blocks, heads * BLOCK, padded), low),
        jax.ShapeDtypeStruct((rows, d), low),
        jax.ShapeDtypeStruct((n, d // n, wi.shape[1] + wd.shape[1]), low),
        jax.ShapeDtypeStruct(bias.shape, f32),
        jax.ShapeDtypeStruct((8, d), f32),
    ]
    return pl.pallas_call(
        functools.partial(feed_kernel, width),
        name="feed",
        grid=(blocks,),
        in_specs=[
            pl.BlockSpec(memory_space=pltpu.SMEM),
            block(d), block(padded), block(d), full(wi), full(wd), full(bias), full(norms),
        ],
        out_specs=[
            block(d),
            pl.BlockSpec((1, heads * BLOCK, padded), lambda r: (r, 0, 0)),
            block(d), full(outs[3]), full(outs[4]), full(outs[5]),
        ],
        out_shape=outs,
        scratch_shapes=[pltpu.VMEM(wi.shape, f32), pltpu.VMEM(wd.shape, f32)],
        compiler_params=pltpu.CompilerParams(vmem_limit_bytes=VMEM),
    )(length, second, context, cot, wi, wd, bias, norms)


def back_kernel(
    width, hidden, length_ref, qkv_ref, qx_ref, dox_ref, first_ref, part_ref, wq_ref, norm_ref,
    table_ref, branch_ref, gw_ref, gbin_ref, gpart_ref, tokens_ref, cot_ref,
    out_ref, gx_ref, gq_ref, gbq_ref, go_ref, gi_ref, gb_ref, gd_ref, small_ref,
    keyt_ref, dqt_ref, dk_ref, dv_ref, gwq_sum, gbias_sum, gsmall_sum,
    gn_ref, gn_near, gn_mid, gn_own, gn_far, gn_sem1, gn_sem2,
    br_near, br_mid, br_far, br_sem1, br_sem2,
    w_got, w_mid, w_last, w_sem1, w_sem2,
    gq_low, q_got, q_mid, q_last, q_sem1, q_sem2,
    line_ref, cross_ref, line_sem, cross_sem,
):
    heads = width // HD
    rows = qkv_ref.shape[0]
    padded = qkv_ref.shape[1] // 3
    blocks = rows // BLOCK
    local = tokens_ref.shape[0]
    per = local // BLOCK
    d = tokens_ref.shape[1]
    scale = HD ** (-0.5)
    step = pl.program_id(0)
    last = blocks - 1
    here = Place()
    weights = Scatter(here, gw_ref, w_got, w_mid, w_last, (w_sem1, w_sem2))
    final = Scatter(here, gq_low, q_got, q_mid, q_last, (q_sem1, q_sem2))

    def near_branch(chip):
        owner = chip * 2 + 1 - here.core
        return send(
            branch_ref.at[pl.ds(pl.multiple_of(owner * local, local), local)], br_near.at[chip],
            br_sem1, chip, here.near,
        )

    def far_branch():
        return send(br_mid, br_far, br_sem2, 0, here.across)

    def branch_rows(chip):
        owner = chip * 2 + here.core
        return branch_ref[pl.ds(pl.multiple_of(owner * local, local), local), :]

    def block_of(number):
        return number // 2 + number % 2 * (blocks - 1 - number // 2 * 2)

    def near_block(r):
        slot = r // per // 2 * per + r % per
        return send(gn_ref.at[r], gn_near.at[slot], gn_sem1, slot, here.near)

    def far_block(r):
        return send(gn_mid.at[r % per], gn_far.at[r % per], gn_sem2, r % per, here.across)

    def collect(r):
        owner = r // per

        @pl.when(owner % 2 == here.core)
        def _():
            near_block(r).wait_recv()
            total = plus(gn_ref[r], gn_near[owner // 2 * per + r % per])

            @pl.when(owner // 2 == here.chip)
            def _():
                gn_own[r % per] = total

            @pl.when(owner // 2 != here.chip)
            def _():
                gn_mid[r % per] = total.astype(low)

    def pass_on(r):
        owner = r // per

        @pl.when((owner % 2 == here.core) & (owner // 2 != here.chip))
        def _():
            far_block(r).start()

    @pl.when(step == 0)
    def _():
        here.greet(True)
        weights.start()
        for chip in range(2):
            near_branch(chip).start()
        dqt_ref[...] = jnp.zeros_like(dqt_ref)
        dk_ref[...] = jnp.zeros_like(dk_ref)
        dv_ref[...] = jnp.zeros_like(dv_ref)
        gwq_sum[...] = jnp.zeros_like(gwq_sum)
        gbias_sum[...] = jnp.zeros_like(gbias_sum)
        gsmall_sum[...] = jnp.zeros_like(gsmall_sum)

        @pl.loop(0, blocks)
        def _(j):
            k = qkv_ref[pl.ds(pl.multiple_of(j * BLOCK, BLOCK), BLOCK), padded : 2 * padded]
            keyt_ref[j] = k.astype(f32).T[:width].astype(low)

    @pl.when(step == 1)
    def _():
        for chip in range(2):
            near_branch(chip).wait_recv()
        br_mid[...] = plus(branch_rows(1 - here.chip), br_near[1 - here.chip]).astype(low)

    for k in range(1, here.majors):

        @pl.when(step == min(k, last - 2))
        def _():
            weights.add(k)

    @pl.when(step > 0)
    def _():
        collect(block_of(step - 1))

    def pair(i, j, own):
        at = pl.ds(pl.multiple_of(j * BLOCK, BLOCK), BLOCK)
        keys, values = qkv_ref[at, padded : 2 * padded], qkv_ref[at, 2 * padded :]
        query, dout = qx_ref[i], dox_ref[i]
        p = jnp.exp(dot(keys, query, NT) * scale)
        if own:
            key_at = lax.broadcasted_iota(jnp.int32, p.shape, 0)
            query_at = lax.broadcasted_iota(jnp.int32, p.shape, 1) % BLOCK
            p = jnp.where(key_at <= query_at, p, 0.0)
        ds = (p * dot(values, dout, NT)).astype(low)
        dv_ref[j] += dot(p.astype(low), dout, NN)
        dk_ref[j] += dot(ds, query, NN)
        for h in range(heads):
            dqt_ref[i, h * HD : (h + 1) * HD, :] += dot(
                keyt_ref[j, h * HD : (h + 1) * HD, :], ds[:, h * BLOCK : (h + 1) * BLOCK], NN
            )

    turn = step // 2
    odd = step % 2
    now = block_of(step)

    @pl.loop(0, last - step)
    def _(number):
        other = turn + 1 + number
        pair(other + odd * (last - turn - other), turn + odd * (other - turn), False)

    @pl.when(step == 1)
    def _():
        far_branch().start()

    for k in range(1, here.majors):

        @pl.when(step == min(k, last - 2))
        def _():
            weights.forward(k)

    @pl.when(step > 0)
    def _():
        pass_on(block_of(step - 1))

    pair(now, now, True)

    tables = rotary_rows(table_ref, now)
    inside = lax.broadcasted_iota(jnp.int32, (BLOCK, padded), 1) < width
    grad_query = jnp.concatenate([dqt_ref[now].T, jnp.zeros((BLOCK, padded - width), f32)], axis=1)
    projected = jnp.concatenate(
        [
            rotate(grad_query * scale, tables, -1),
            rotate(jnp.where(inside, dk_ref[now] * scale, 0.0), tables, -1),
            jnp.where(inside, dv_ref[now], 0.0),
        ],
        axis=1,
    )
    gbias_sum[...] += jnp.sum(projected, axis=0, keepdims=True)
    proj_low = projected.astype(low)
    at = pl.ds(pl.multiple_of(now * BLOCK, BLOCK), BLOCK)
    first = first_ref[at, :]
    gwq_sum[...] += dot(first, proj_low, TN)
    part = dot(proj_low, wq_ref[...], NT)
    gsmall_sum[0:1, :] += jnp.sum(part * first.astype(f32), axis=0, keepdims=True)
    gsmall_sum[1:2, :] += jnp.sum(part, axis=0, keepdims=True)
    gn_ref[now] = (part * norm_ref[0:1, :] + part_ref[at, :].astype(f32)).astype(low)

    @pl.when(now // per % 2 != here.core)
    def _():
        near_block(now).start()

    row = lax.broadcasted_iota(jnp.int32, (local, d), 0) + here.t * local
    kept = row < length_ref[0]

    @pl.when(step == last - 1)
    def _():
        far_branch().wait()
        for chip in range(2):
            near_branch(chip).wait_send()
        total = plus(branch_rows(here.chip), br_near[here.chip], br_far[...])
        total = total + (norm_ref[4:5, :] + norm_ref[5:6, :])
        out_ref[...] = tokens_ref[...].astype(f32) + jnp.where(kept, total, 0.0)

    @pl.when(step == last)
    def _():
        side = gwq_sum.shape[0] // here.n
        for block in range(here.n):
            rows_of = slice(block * side, (block + 1) * side)
            gq_low[block] = jnp.concatenate(
                [gwq_sum[rows_of, k * padded : k * padded + width] for k in range(3)], axis=1
            ).astype(low)
        cot = cot_ref[...].astype(f32)
        dense = jnp.sum(jnp.where(kept, cot, 0.0), axis=0, keepdims=True)
        line_ref[here.dp] = jnp.concatenate(
            [gbias_sum[...], gbin_ref[...], gsmall_sum[0:2, :], gpart_ref[0:2, :], dense, dense]
        )
        final.start()

        line = Exchange(line_ref, line_sem, here.dp, here.n, lambda to: (to, here.t))
        cross = Exchange(cross_ref, cross_sem, here.t, here.ways, lambda to: (here.dp, to))
        line.start()
        collect(now)
        x = tokens_ref[...].astype(f32)
        shifted = x - jnp.mean(x, axis=1, keepdims=True)
        inv_std = lax.rsqrt(jnp.mean(shifted * shifted, axis=1, keepdims=True) + EPS)
        normed = shifted * inv_std
        pass_on(now)

        total = weights.finish()
        gi_ref[...] = total[:, :hidden]
        gd_ref[...] = total[:, hidden : 2 * hidden].T
        go_ref[...] = total[:, 2 * hidden : 2 * hidden + width].T

        for k in range(1, here.majors):
            final.add(k)
            final.forward(k)
        summed = line.total()
        gbq_ref[...] = summed[0:1, :]
        gb_ref[...] = summed[1:2, :]
        cross_ref[here.t] = summed
        for k in range(per):
            far_block(k).wait()
        for slot in range(2 * per):
            near_block(slot // per * 2 * per + (1 - here.core) * per + slot % per).wait_send()
        grad_normed = jnp.concatenate([gn_own[k] + gn_far[k].astype(f32) for k in range(per)])
        cross.start()
        gx_ref[...] = cot + inv_std * (
            grad_normed
            - jnp.mean(grad_normed, axis=1, keepdims=True)
            - normed * jnp.mean(grad_normed * normed, axis=1, keepdims=True)
        )
        summed = cross.total()
        for k in range(2):
            product, plain = summed[2 + 2 * k : 3 + 2 * k, :], summed[3 + 2 * k : 4 + 2 * k, :]
            gain, bias = norm_ref[2 * k : 2 * k + 1, :], norm_ref[2 * k + 1 : 2 * k + 2, :]
            small_ref[2 * k : 2 * k + 1, :] = (product - bias * plain) / gain
            small_ref[2 * k + 1 : 2 * k + 2, :] = plain
        small_ref[4:5, :] = summed[6:7, :]
        line.finish()
        cross.finish()
        gq_ref[...] = final.finish()


def back(width, length, qkv, qx, dox, first, part, wq, norms, table, branch, gw, gb_in, gpart, tokens, cot):
    rows, d = first.shape
    padded = qkv.shape[1] // 3
    blocks = rows // BLOCK
    local = tokens.shape[0]
    per = local // BLOCK
    n, side, columns = gw.shape
    hidden = gb_in.shape[1]
    majors = n // 2
    ways = lax.axis_size("tensor")
    assert ways == 4 and 3 * padded == d == hidden and side * n == d
    full = lambda a: pl.BlockSpec(
        a.shape, lambda r: (0,) * len(a.shape), pipeline_mode=pl.Buffered(1)
    )
    outs = [
        jax.ShapeDtypeStruct((local, d), f32),
        jax.ShapeDtypeStruct((local, d), f32),
        jax.ShapeDtypeStruct((side, 3 * width), f32),
        jax.ShapeDtypeStruct((1, 3 * padded), f32),
        jax.ShapeDtypeStruct((width, side), f32),
        jax.ShapeDtypeStruct((side, hidden), f32),
        jax.ShapeDtypeStruct((1, hidden), f32),
        jax.ShapeDtypeStruct((hidden, side), f32),
        jax.ShapeDtypeStruct((5, d), f32),
    ]
    args = (qkv, qx, dox, first, part, wq, norms, table, branch, gw, gb_in, gpart, tokens, cot)
    return pl.pallas_call(
        functools.partial(back_kernel, width, hidden),
        name="back",
        grid=(blocks,),
        in_specs=[pl.BlockSpec(memory_space=pltpu.SMEM)] + [full(a) for a in args],
        out_specs=[pl.BlockSpec(memory_space=pltpu.VMEM)] * len(outs),
        out_shape=outs,
        scratch_shapes=[
            pltpu.VMEM((blocks, width, BLOCK), low),
            pltpu.VMEM((blocks, width, BLOCK), f32),
            pltpu.VMEM((blocks, BLOCK, padded), f32),
            pltpu.VMEM((blocks, BLOCK, padded), f32),
            pltpu.VMEM(wq.shape, f32),
            pltpu.VMEM((1, 3 * padded), f32),
            pltpu.VMEM((8, d), f32),
            pltpu.VMEM((blocks, BLOCK, d), low),
            pltpu.VMEM((2 * per, BLOCK, d), low),
            pltpu.VMEM((per, BLOCK, d), low),
            pltpu.VMEM((per, BLOCK, d), f32),
            pltpu.VMEM((per, BLOCK, d), low),
            pltpu.SemaphoreType.DMA((2, 2 * per)),
            pltpu.SemaphoreType.DMA((2, per)),
            pltpu.VMEM((2, local, d), low),
            pltpu.VMEM((local, d), low),
            pltpu.VMEM((local, d), low),
            pltpu.SemaphoreType.DMA((2, 2)),
            pltpu.SemaphoreType.DMA((2, 1)),
        ]
        + scatter_scratch(majors, side, columns)
        + [pltpu.VMEM((n, side, 3 * width), low)]
        + scatter_scratch(majors, side, 3 * width)
        + [
            pltpu.VMEM((n, 8, d), f32),
            pltpu.VMEM((ways, 8, d), f32),
            pltpu.SemaphoreType.DMA((2, n)),
            pltpu.SemaphoreType.DMA((2, ways)),
        ],
        compiler_params=pltpu.CompilerParams(
            vmem_limit_bytes=VMEM, collective_id=2, has_side_effects=True
        ),
    )(length, *args)


def per_device(
    tokens, cotangent, seq_lengths, norm1_gain, norm1_bias, norm2_gain, norm2_bias,
    w_qkv, b_qkv, w_attn_out, w_in, b_in, w_down, b_out, b_down,
):
    local_rows, d = tokens.shape
    width = w_qkv.shape[2]
    padded = round_up(width + 3, LANES)
    extra = padded - width
    assert local_rows * lax.axis_size("tensor") == LMAX and seq_lengths.shape[0] == 1
    hidden = w_in.shape[1]

    wq = jnp.pad(w_qkv, ((0, 0), (0, 0), (0, extra))).reshape(-1, 3 * padded)
    bq = jnp.pad(b_qkv, ((0, 0), (0, extra))).reshape(1, 3 * padded)
    wd = jnp.concatenate([w_down.T, jnp.pad(w_attn_out.T, ((0, 0), (0, extra)))], axis=1)
    norms = jnp.stack([norm1_gain, norm1_bias, norm2_gain, norm2_bias, b_out, b_down])
    table = jnp.asarray(rotary_base())

    first, second, qkv, wq_full = front(width, tokens, wq, norms, bq, table)
    context, qx, wi_full, wd_full, cot_full = attend(width, qkv, w_in, wd, cotangent)
    merge = lambda a: a.reshape(-1, a.shape[-1])
    wq_full, wi_full, wd_full = merge(wq_full), merge(wi_full), merge(wd_full)
    branch, dox, part, gw, gb_in, gpart = feed(
        width, seq_lengths, second, context, merge(cot_full), wi_full, wd_full,
        b_in.reshape(1, -1), norms,
    )
    output, grad_x, gq, gb_qkv, g_out, g_in, gb_in, g_down, small = back(
        width, seq_lengths, qkv, qx, dox, first, part, wq_full, norms, table, branch, gw, gb_in, gpart,
        tokens, cotangent,
    )
    return (
        output,
        grad_x,
        gq.reshape(-1, 3, width),
        gb_qkv.reshape(3, padded)[:, :width],
        g_out,
        g_in,
        gb_in.reshape(-1),
        g_down,
        small,
    )


def solution(mesh):
    rows = P(("dp", "tensor"), None)
    placed = (
        rows, rows, P("dp"), P(), P(), P(), P(), P("dp", None, "tensor"), P(None, "tensor"),
        P("tensor", "dp"), P("dp", "tensor"), P("tensor"), P("tensor", "dp"), P(), P(),
    )
    return jax.shard_map(
        per_device,
        mesh=mesh,
        in_specs=placed,
        out_specs=(
            rows, rows, P("dp", None, "tensor"), P(None, "tensor"), P("tensor", "dp"),
            P("dp", "tensor"), P("tensor"), P("tensor", "dp"), P(),
        ),
        check_vma=False,
    )
```

```python
import functools
import math

import jax
import jax.numpy as jnp
import numpy as np
from jax import lax
from jax.experimental import pallas as pl
from jax.experimental.pallas import tpu as pltpu
from jax.sharding import PartitionSpec as P

HD = 64
ROT = 16
LMAX = 2048
LANES = 128
EPS = 1e-05
BLOCK = 256
FAST = 64
VMEM = 66 * 1024 * 1024

f32 = jnp.float32
low = jnp.bfloat16

NN = (((1,), (0,)), ((), ()))
NT = (((1,), (1,)), ((), ()))
TN = (((0,), (0,)), ((), ()))


def dot(a, b, dims):
    return lax.dot_general(a, b, dims, preferred_element_type=f32)


def round_up(n, m):
    return (n + m - 1) // m * m


def rotary_base():
    d = np.arange(LANES) % HD
    half = ROT // 2
    inverse = np.where(d < ROT, np.exp((d % half) * (-2.0 * math.log(10000.0) / ROT)), 0.0)
    slow = np.arange(0, LMAX, FAST)[:, None] * inverse
    fast = np.arange(FAST)[:, None] * inverse
    return np.concatenate([np.cos(slow), np.sin(slow), np.cos(fast), np.sin(fast)]).astype(
        np.float32
    )


def rotary_rows(table_ref, block):
    slow_rows = LMAX // FAST
    fast_cos = table_ref[2 * slow_rows : 2 * slow_rows + FAST, :]
    fast_sin = table_ref[2 * slow_rows + FAST :, :]
    cosines, sines = [], []
    for part in range(BLOCK // FAST):
        row = block * (BLOCK // FAST) + part
        slow_cos = table_ref[pl.ds(row, 1), :]
        slow_sin = table_ref[pl.ds(row + slow_rows, 1), :]
        cosines.append(slow_cos * fast_cos - slow_sin * fast_sin)
        sines.append(slow_sin * fast_cos + slow_cos * fast_sin)
    cosine, sine = jnp.concatenate(cosines), jnp.concatenate(sines)
    d = lax.broadcasted_iota(jnp.int32, cosine.shape, 1) % HD
    return (
        cosine,
        jnp.where(d < ROT // 2, -sine, 0.0),
        jnp.where((d >= ROT // 2) & (d < ROT), sine, 0.0),
    )


def rotate(values, tables, sign):
    cosine, from_right, from_left = tables
    half = ROT // 2
    turned = []
    for first in range(0, values.shape[1], LANES):
        t = values[:, first : first + LANES]
        side = (
            pltpu.roll(t, LANES - half, axis=1) * from_right
            + pltpu.roll(t, half, axis=1) * from_left
        )
        turned.append(t * cosine + side if sign > 0 else t * cosine - side)
    return jnp.concatenate(turned, axis=1)


def three_terms(value):
    first = value.astype(low).astype(f32)
    second = (value - first).astype(low).astype(f32)
    return first, second, value - first - second


MESH = pl.DeviceIdType.MESH


class Place:
    def __init__(self):
        self.dp, self.t = lax.axis_index("dp"), lax.axis_index("tensor")
        self.n, self.ways = lax.axis_size("dp"), lax.axis_size("tensor")
        self.majors = self.n // 2
        self.a, self.b = self.dp // 2, self.dp % 2
        self.chip, self.core = self.t // 2, self.t % 2
        self.upper = self.a * 2 // self.majors
        self.near = (self.dp, self.t + 1 - 2 * self.core)
        self.across = (self.dp, (self.t + 2) % 4)
        self.beside = (self.dp + 1 - 2 * self.b, self.t)

    def major(self, k):
        return ((self.a + k) % self.majors, (self.a + k) % self.majors * 2 + self.b)

    def shard(self, kind):
        return (self.chip + kind // 2) % 2 * 2 + (self.core + kind % 2) % 2

    def greet(self):
        barrier = pltpu.get_barrier_semaphore()
        others = [self.near, self.across, (self.dp, 3 - self.t)]
        others += [((self.dp + k) % self.n, self.t) for k in range(1, self.n)]
        for other in others:
            pl.semaphore_signal(barrier, inc=1, device_id=other, device_id_type=MESH)
        pl.semaphore_wait(barrier, len(others))


def send(src, dst, sems, k, to):
    return pltpu.make_async_remote_copy(
        src_ref=src,
        dst_ref=dst,
        send_sem=sems.at[0, k],
        recv_sem=sems.at[1, k],
        device_id=to,
        device_id_type=MESH,
    )


def plus(*terms):
    return functools.reduce(jnp.add, [t.astype(f32) for t in terms])


class Scatter:
    def __init__(self, place, mine, got, last, sems):
        self.p, self.mine, self.got, self.last, self.pairs, self.lines = place, mine, got, last, *sems

    def first(self, k):
        p = self.p
        mine = self.mine.at[p.major(k)[0] * 2 + 1 - p.b]
        return send(mine, self.got.at[k % p.majors], self.pairs, k % p.majors, p.beside)

    def second(self, k):
        to = (self.p.major(k)[1], self.p.t)
        return send(self.got.at[k], self.last.at[k - 1], self.lines, k - 1, to)

    def start(self):
        for k in range(1, self.p.majors + 1):
            self.first(k).start()

    def add(self, k):
        self.first(k).wait_recv()
        self.got[k] = plus(self.mine[self.p.major(k)[1]], self.got[k]).astype(self.got.dtype)

    def forward(self, k):
        self.second(k).start()

    def finish(self):
        p = self.p
        for k in range(1, p.majors + 1):
            self.first(k).wait_send()
        self.first(p.majors).wait_recv()
        for k in range(1, p.majors):
            self.second(k).wait()
        return plus(self.mine[p.dp], self.got[0], *[self.last[k] for k in range(p.majors - 1)])


class Gather:
    def __init__(self, place, mine, whole, sems):
        self.p, self.mine, self.whole, self.lines, self.pairs = place, mine, whole, *sems

    def line(self, k):
        p = self.p
        return send(self.mine, self.whole.at[p.dp], self.lines, k - 1, (p.major(k)[1], p.t))

    def pair(self, k):
        block = self.whole.at[self.p.major(self.p.majors - k)[1]]
        return send(block, block, self.pairs, k, self.p.beside)

    def own_pair(self):
        return send(self.mine, self.whole.at[self.p.dp], self.pairs, 0, self.p.beside)

    def start(self):
        p = self.p
        for k in range(1, p.majors):
            self.line(k + p.upper * (p.majors - 2 * k)).start()

    def forward(self, number):
        p = self.p
        k = p.majors - number + p.upper * (2 * number - p.majors)
        self.line(k).wait_recv()
        self.pair(k).start()

    def arrived(self):
        self.own_pair().wait_recv()
        for k in range(1, self.p.majors):
            self.pair(k).wait_recv()

    def finish(self):
        self.own_pair().wait_send()
        for k in range(1, self.p.majors):
            self.pair(k).wait_send()
            self.line(k).wait_send()


def gather_scratch(majors):
    return [pltpu.SemaphoreType.DMA((2, majors - 1)), pltpu.SemaphoreType.DMA((2, majors))]


class Rows:
    def __init__(self, place, mine, whole, sems):
        self.p, self.mine, self.whole, self.sems = place, mine, whole, sems
        self.per = mine.shape[0] // BLOCK

    def copy(self, kind, c):
        p = self.p
        if kind == 2:
            block = self.whole.at[p.across[1] * self.per + c]
            return send(block, block, self.sems, 2 * self.per + c, p.near)
        to = p.near if kind == 0 else p.across
        mine = self.mine.at[pl.ds(c * BLOCK, BLOCK)]
        return send(mine, self.whole.at[p.t * self.per + c], self.sems, kind * self.per + c, to)

    def start(self):
        for c in range(self.per):
            for kind in range(2):
                self.copy(kind, c).start()

    def arrived(self, kind, c):
        self.copy(kind, c).wait_recv()

    def forward(self, c):
        self.copy(1, c).wait_recv()
        self.copy(2, c).start()

    def released(self):
        for c in range(self.per):
            self.copy(2, c).wait_send()

    def finish(self):
        for c in range(self.per):
            for kind in range(2):
                self.copy(kind, c).wait_send()


class Exchange:
    def __init__(self, slots, sems, me, count, device):
        self.slots, self.sems, self.me, self.count, self.device = slots, sems, me, count, device

    def copy(self, k, source):
        return pltpu.make_async_remote_copy(
            src_ref=self.slots.at[source],
            dst_ref=self.slots.at[source],
            send_sem=self.sems.at[0, k],
            recv_sem=self.sems.at[1, source],
            device_id=self.device((self.me + k) % self.count),
            device_id_type=MESH,
        )

    def start(self):
        for k in range(1, self.count):
            self.copy(k, self.me).start()

    def total(self):
        for k in range(1, self.count):
            self.copy(k, (self.me + k) % self.count).wait_recv()
        return functools.reduce(jnp.add, [self.slots[k] for k in range(self.count)])

    def finish(self):
        for k in range(1, self.count):
            self.copy(k, self.me).wait_send()


def scatter_scratch(majors, rows, columns):
    return [
        pltpu.VMEM((majors, rows, columns), low),
        pltpu.VMEM((majors - 1, rows, columns), low),
        pltpu.SemaphoreType.DMA((2, majors)),
        pltpu.SemaphoreType.DMA((2, majors - 1)),
    ]


def flat(blocks_ref):
    n, side, columns = blocks_ref.shape
    if side % 16 == 0:
        return blocks_ref[...].reshape(n * side, columns)
    return jnp.concatenate([blocks_ref[k].astype(f32) for k in range(n)]).astype(low)


def norm_rows(x):
    shifted = x - jnp.mean(x, axis=1, keepdims=True)
    inv_std = lax.rsqrt(jnp.mean(shifted * shifted, axis=1, keepdims=True) + EPS)
    return shifted * inv_std, inv_std


def layer_kernel(
    length_ref, tokens_ref, cot_ref, g1_ref, b1_ref, g2_ref, b2_ref, wq_ref, bq_ref, wo_ref, wi_ref,
    bi_ref, wd_ref, bo_ref, bd_ref, table_ref,
    out_out, gx_out, gq_ref, gbq_ref, go_ref, gi_ref, gb_ref, gd_ref, small_ref,
    norm_ref, bias_ref, wq_mine, wd_mine, wq_all, wi_all, wd_all,
    x_all, first_ref, second_ref, cot_all, qkv_ref, qx_ref, vm_ref, context_ref, pool_ref,
    keyt_ref, gwi_sum, gwd_sum, gb_sum, gs_sum, gw_ref, own_sems, out_sems, x_sems, cot_sems,
    wq_lines, wq_pairs, wi_lines, wi_pairs, wd_lines, wd_pairs,
    gn_near, gn_own, gn_far, gn_sem1, gn_sem2,
    br_near, br_far, br_sem1, br_sem2,
    w_got, w_last, w_sem1, w_sem2,
    gq_low, q_got, q_last, q_sem1, q_sem2,
    line_ref, cross_ref, line_sem, cross_sem,
):
    here = Place()
    blocks, _, d = x_all.shape
    local = tokens_ref.shape[0]
    per = local // BLOCK
    width = wq_ref.shape[2]
    heads = width // HD
    padded = qkv_ref.shape[2] // 3
    hidden = wi_ref.shape[1]
    side = wi_ref.shape[0]
    scale = HD ** (-0.5)
    lane = lax.broadcasted_iota(jnp.int32, (BLOCK, padded), 1)
    of_head = [(lane >= h * HD) & (lane < (h + 1) * HD) for h in range(heads)]
    inside = lane < width
    extra = (lane >= width) & (lane < width + 3)

    rows = Rows(here, tokens_ref, x_all, x_sems)
    cots = Rows(here, cot_ref, cot_all, cot_sems)
    proj_w = Gather(here, wq_mine, wq_all, (wq_lines, wq_pairs))
    in_w = Gather(here, wi_ref, wi_all, (wi_lines, wi_pairs))
    down_w = Gather(here, wd_mine, wd_all, (wd_lines, wd_pairs))

    wq_mine[...] = jnp.zeros_like(wq_mine)
    wd_mine[:, hidden:] = jnp.zeros((side, padded), low)
    bias_ref[...] = jnp.zeros_like(bias_ref)
    for k in range(3):
        wq_mine[:, k * padded : k * padded + width] = wq_ref[k]
        bias_ref[0:1, k * padded : k * padded + width] = bq_ref[k : k + 1, :]
    wd_mine[:, :hidden] = wd_ref[...]
    wd_mine[:, hidden : hidden + width] = wo_ref[...].astype(f32).T.astype(low)
    for k, ref in enumerate((g1_ref, b1_ref, g2_ref, b2_ref, bo_ref, bd_ref, bi_ref)):
        norm_ref[k, :] = ref[...]

    here.greet()
    proj_w.start()
    proj_w.own_pair().start()
    rows.start()
    in_w.start()
    down_w.start()
    own = [
        pltpu.make_async_copy(tokens_ref.at[pl.ds(c * BLOCK, BLOCK)], x_all.at[here.t * per + c], own_sems.at[c])
        for c in range(per)
    ]
    own += [
        pltpu.make_async_copy(cot_ref.at[pl.ds(c * BLOCK, BLOCK)], cot_all.at[here.t * per + c], own_sems.at[per + c])
        for c in range(per)
    ]
    own += [
        pltpu.make_async_copy(mine, whole.at[here.dp], own_sems.at[2 * per + k])
        for k, (mine, whole) in enumerate(((wq_mine, wq_all), (wi_ref, wi_all), (wd_mine, wd_all)))
    ]
    for copy in own:
        copy.start()

    def norm(kind, c):
        r = here.shard(kind) * per + c
        normed, _ = norm_rows(x_all[r].astype(f32))
        first_ref[r] = (normed * norm_ref[0:1, :] + norm_ref[1:2, :]).astype(low)
        second_ref[r] = (normed * norm_ref[2:3, :] + norm_ref[3:4, :]).astype(low)

    def project(kind, c):
        r = here.shard(kind) * per + c
        projected = dot(first_ref[r], flat(wq_all), NN) + bias_ref[...]
        tables = rotary_rows(table_ref, r)
        qkv_ref[r, :, :padded] = rotate(projected[:, :padded], tables, 1).astype(low)
        keys = rotate(projected[:, padded : 2 * padded], tables, 1)
        keys = jnp.where(extra, 1.0, keys)
        keyt_ref[r] = keys.T[:width].astype(low)
        qkv_ref[r, :, padded : 2 * padded] = keys.astype(low)
        values = projected[:, 2 * padded :]
        qkv_ref[r, :, 2 * padded :] = jnp.where(extra, 1.0, values).astype(low)
        for h in range(heads):
            vm_ref[r, h * BLOCK : (h + 1) * BLOCK, :] = jnp.where(
                of_head[h], values, jnp.where(lane == width + h, 1.0, 0.0)
            ).astype(low)

    for c in range(per):
        own[c].wait()

    @pl.loop(0, per)
    def _(c):
        norm(0, c)

    for c in range(per):
        rows.arrived(0, c)
    proj_w.forward(1)

    @pl.loop(0, per)
    def _(c):
        norm(1, c)

    for k in range(2, here.majors - 1):
        proj_w.forward(k)
    for c in range(per - 1):
        rows.forward(c)
    proj_w.forward(here.majors - 1)
    in_w.own_pair().start()
    down_w.own_pair().start()
    cots.start()
    for c in range(per - 1):
        norm(2, c)
    for c in range(per - 1):
        rows.arrived(2, c)
        norm(3, c)
    own[2 * per].wait()
    proj_w.arrived()

    @pl.loop(0, per + 2 * (per - 1))
    def _(number):
        @pl.when(number == per + 1)
        def _():
            rows.forward(per - 1)

        later = number // per
        project(1 + later + number % per * later, number % per * (1 - later))

    @pl.loop(0, per)
    def _(c):
        project(0, c)

    norm(2, per - 1)
    project(2, per - 1)
    rows.arrived(2, per - 1)
    norm(3, per - 1)
    project(3, per - 1)

    @pl.loop(0, blocks)
    def _(i):
        for k in range(1, here.majors):

            @pl.when(i == min(blocks // 2 - 2 + k, blocks - 1))
            def _():
                in_w.forward(k)

        for c in range(per):

            @pl.when(i == blocks - per + c)
            def _():
                cots.forward(c)

        q = qkv_ref[i, :, :padded].astype(f32)
        for h in range(heads):
            qx_ref[i, h * BLOCK : (h + 1) * BLOCK, :] = jnp.where(of_head[h], q, 0.0).astype(low)
        query = qx_ref[i]

        def scores(j):
            return dot(query, qkv_ref[j, :, padded : 2 * padded], NT)

        def widest(s):
            return functools.reduce(
                jnp.maximum, [s[:, c : c + LANES] for c in range(0, BLOCK, LANES)]
            )

        diagonal = scores(i)
        row = lax.broadcasted_iota(jnp.int32, diagonal.shape, 0) % BLOCK
        col = lax.broadcasted_iota(jnp.int32, diagonal.shape, 1)
        diagonal = jnp.where(col <= row, diagonal, -1e30)

        def first_pass(j, top):
            s = scores(j)
            pool_ref[pl.ds(j * heads, heads)] = s.reshape(heads, BLOCK, BLOCK)
            return jnp.maximum(top, widest(s))

        top = lax.fori_loop(0, i, first_pass, widest(diagonal))
        top = jnp.max(top, axis=1, keepdims=True)

        def weigh(s, j):
            p = jnp.exp((s - top) * scale).astype(low)
            parts = [slice(h * BLOCK, (h + 1) * BLOCK) for h in range(heads)]
            return functools.reduce(jnp.add, [dot(p[at], vm_ref[j, at, :], NN) for at in parts])

        def second_pass(j, total):
            s = pool_ref[pl.ds(j * heads, heads)].reshape(heads * BLOCK, BLOCK)
            return total + weigh(s, j)

        mixed = lax.fori_loop(0, i, second_pass, weigh(diagonal, i))
        inverse = jnp.zeros((BLOCK, padded), f32)
        for h in range(heads):
            total = mixed[:, width + h : width + h + 1]
            inverse = jnp.where(of_head[h], 1.0 / total, inverse)
            log_total = top[h * BLOCK : (h + 1) * BLOCK] + jnp.log(total) / scale
            extended = jnp.where(of_head[h], q, 0.0)
            for k, term in enumerate(three_terms(-log_total)):
                extended = jnp.where(lane == width + k, term, extended)
            qx_ref[i, h * BLOCK : (h + 1) * BLOCK, :] = extended.astype(low)
        context_ref[i] = (mixed * inverse).astype(low)

    for k in range(1, here.majors):
        down_w.forward(k)
    for c in range(per):
        cots.arrived(0, c)
        cots.arrived(2, c)
    for copy in own[per : 2 * per] + own[2 * per + 1 :]:
        copy.wait()
    in_w.arrived()
    gwi_sum[...] = jnp.zeros_like(gwi_sum)
    gwd_sum[...] = jnp.zeros_like(gwd_sum)
    gb_sum[...] = jnp.zeros_like(gb_sum)
    gs_sum[...] = jnp.zeros_like(gs_sum)
    down_w.arrived()
    cots.released()
    rows.released()

    branch_ref, part_ref, dox_ref = cot_all, second_ref, vm_ref

    def near_branch(chip):
        owner = chip * 2 + 1 - here.core
        return send(
            branch_ref.at[pl.ds(owner * per, per)], br_near.at[chip], br_sem1, chip, here.near
        )

    def far_branch():
        return send(br_near.at[1 - here.chip], br_far, br_sem2, 0, here.across)

    @pl.loop(0, blocks)
    def _(number):
        r = here.shard(3 - number // per) * per + number % per

        @pl.when(number == per + 1)
        def _():
            near_branch(1 - here.chip).start()

        @pl.when(number == 2 * per + 1)
        def _():
            near_branch(1 - here.chip).wait_recv()

            @pl.loop(0, per)
            def _(c):
                mine = branch_ref[here.across[1] * per + c]
                br_near[1 - here.chip, c] = plus(mine, br_near[1 - here.chip, c]).astype(low)

        @pl.when(number == 3 * per + 1)
        def _():
            near_branch(here.chip).start()

        second = second_ref[r]
        context = context_ref[r]
        row = lax.broadcasted_iota(jnp.int32, second.shape, 0) + r * BLOCK
        grad = jnp.where(row < length_ref[0], cot_all[r].astype(f32), 0.0).astype(low)

        u = dot(second, flat(wi_all), NN) + norm_ref[6:7, :]
        cdf = 0.5 * (1.0 + lax.erf(u * (1.0 / math.sqrt(2.0))))
        act = (u * cdf).astype(low)
        slope = cdf + u * (jnp.exp(-0.5 * u * u) * (1.0 / math.sqrt(2.0 * math.pi)))
        both = jnp.concatenate([act, context], axis=1)
        back = dot(grad, flat(wd_all), NN)
        branch_ref[r] = dot(both, flat(wd_all), NT).astype(low)

        grad_hidden = back[:, :hidden] * slope
        gb_sum[1:2, :] += jnp.sum(grad_hidden, axis=0, keepdims=True)
        hidden_low = grad_hidden.astype(low)
        gwi_sum[...] += dot(second, hidden_low, TN)
        gwd_sum[...] += dot(grad, both, TN)

        @pl.when(number == 2 * per + 1)
        def _():
            far_branch().start()

        grad_context = back[:, hidden:].astype(low).astype(f32)
        product = grad_context * context.astype(f32)
        for h in range(heads):
            extended = jnp.where(of_head[h], grad_context, 0.0)
            delta = jnp.sum(jnp.where(of_head[h], product, 0.0), axis=1, keepdims=True)
            for k, term in enumerate(three_terms(-delta)):
                extended = jnp.where(lane == width + k, term, extended)
            dox_ref[r, h * BLOCK : (h + 1) * BLOCK, :] = extended.astype(low)

        part = dot(hidden_low, flat(wi_all), NT)
        gs_sum[2:3, :] += jnp.sum(part * second.astype(f32), axis=0, keepdims=True)
        gs_sum[3:4, :] += jnp.sum(part, axis=0, keepdims=True)
        part_ref[r] = (part * norm_ref[2:3, :]).astype(low)

    weights = Scatter(here, gw_ref, w_got, w_last, (w_sem1, w_sem2))
    final = Scatter(here, gq_low, q_got, q_last, (q_sem1, q_sem2))
    for block in range(here.n):
        rows_of = slice(block * side, (block + 1) * side)
        gw_ref[block, :, :hidden] = gwi_sum[rows_of, :].astype(low)
        gw_ref[block, :, hidden:] = gwd_sum[rows_of, :].astype(low)
    gwq_sum, gn_ref = gwi_sum, x_all
    gwq_sum[...] = jnp.zeros_like(gwq_sum)
    pool_ref[...] = jnp.zeros_like(pool_ref)
    weights.start()

    last = blocks - 1

    def block_of(number):
        return number // 2 + number % 2 * (last - number // 2 * 2)

    def slot_of(r):
        return r // per // 2 * per + r % per

    def near_block(r):
        return send(gn_ref.at[r], gn_near.at[slot_of(r)], gn_sem1, slot_of(r), here.near)

    def far_block(c):
        mine = gn_near.at[(1 - here.chip) * per + c]
        return send(mine, gn_far.at[c], gn_sem2, c, here.across)

    def hand_over(r):
        @pl.when(r // per % 2 != here.core)
        def _():
            near_block(r).start()

    def collect(r):
        owner = r // per

        @pl.when(owner % 2 == here.core)
        def _():
            near_block(r).wait_recv()
            total = plus(gn_ref[r], gn_near[slot_of(r)])

            @pl.when(owner // 2 == here.chip)
            def _():
                gn_own[r % per] = total

            @pl.when(owner // 2 != here.chip)
            def _():
                gn_near[slot_of(r)] = total.astype(low)

    def pass_on(r):
        owner = r // per

        @pl.when((owner % 2 == here.core) & (owner // 2 != here.chip))
        def _():
            far_block(r % per).start()

    def pair(i, j, own):
        keys, values = qkv_ref[j, :, padded : 2 * padded], qkv_ref[j, :, 2 * padded :]
        query, dout = qx_ref[i], dox_ref[i]
        p = jnp.exp(dot(keys, query, NT) * scale)
        if own:
            key_at = lax.broadcasted_iota(jnp.int32, p.shape, 0)
            query_at = lax.broadcasted_iota(jnp.int32, p.shape, 1) % BLOCK
            p = jnp.where(key_at <= query_at, p, 0.0)
        ds = (p * dot(values, dout, NT)).astype(low)
        pool_ref[blocks + j] += dot(p.astype(low), dout, NN)
        pool_ref[j] += dot(ds, query, NN)
        for h in range(heads):
            pool_ref[2 * blocks + i, h * HD : (h + 1) * HD, :] += dot(
                keyt_ref[j, h * HD : (h + 1) * HD, :], ds[:, h * BLOCK : (h + 1) * BLOCK], NN
            )

    def kept(c, values):
        row = lax.broadcasted_iota(jnp.int32, (BLOCK, d), 0) + (here.t * per + c) * BLOCK
        return jnp.where(row < length_ref[0], values, 0.0)

    def output_copy():
        return pltpu.make_async_copy(gwd_sum.at[:local, :d], out_out, out_sems.at[0])

    @pl.loop(0, blocks)
    def _(step):
        for k in range(1, here.majors):

            @pl.when(step == min(k, last - 2))
            def _():
                weights.add(k)

        @pl.when(step > 0)
        def _():
            hand_over(block_of(step - 1))

        turn = step // 2
        odd = step % 2
        now = block_of(step)
        pair(now, now, True)

        for k in range(1, here.majors):

            @pl.when(step == min(k, last - 2))
            def _():
                weights.forward(k)

        @pl.when(step > 0)
        def _():
            collect(block_of(step - 1))

        @pl.loop(0, last - step)
        def _(number):
            other = turn + 1 + number
            pair(other + odd * (last - turn - other), turn + odd * (other - turn), False)

        @pl.when(step == last // 2)
        def _():
            far_branch().wait()
            for chip in range(2):
                near_branch(chip).wait_send()
            near_branch(here.chip).wait_recv()

            @pl.loop(0, per)
            def _(c):
                total = plus(branch_ref[here.t * per + c], br_near[here.chip, c], br_far[c])
                total += norm_ref[4:5, :] + norm_ref[5:6, :]
                at = pl.ds(pl.multiple_of(c * BLOCK, BLOCK), BLOCK)
                gwd_sum[at, :d] = tokens_ref[at, :].astype(f32) + kept(c, total)

        tables = rotary_rows(table_ref, now)
        grad_query = jnp.concatenate(
            [
                pool_ref[2 * blocks + now, :width, :].T,
                jnp.zeros((BLOCK, padded - width), f32),
            ],
            axis=1,
        )
        projected = jnp.concatenate(
            [
                rotate(grad_query * scale, tables, -1),
                rotate(jnp.where(inside, pool_ref[now] * scale, 0.0), tables, -1),
                jnp.where(inside, pool_ref[blocks + now], 0.0),
            ],
            axis=1,
        )
        gb_sum[0:1, :] += jnp.sum(projected, axis=0, keepdims=True)
        proj_low = projected.astype(low)
        first = first_ref[now]
        gwq_sum[...] += dot(first, proj_low, TN)
        part = dot(proj_low, flat(wq_all), NT)
        gs_sum[0:1, :] += jnp.sum(part * first.astype(f32), axis=0, keepdims=True)
        gs_sum[1:2, :] += jnp.sum(part, axis=0, keepdims=True)
        gn_ref[now] = (part * norm_ref[0:1, :] + part_ref[now].astype(f32)).astype(low)

        @pl.when(step > 0)
        def _():
            pass_on(block_of(step - 1))

        @pl.when(step == last // 2)
        def _():
            output_copy().start()

    now = block_of(last)
    for block in range(here.n):
        rows_of = slice(block * side, (block + 1) * side)
        gq_low[block] = jnp.concatenate(
            [gwq_sum[rows_of, k * padded : k * padded + width] for k in range(3)], axis=1
        ).astype(low)
    hand_over(now)
    for c in range(per):
        cot = kept(c, cot_ref[c * BLOCK : (c + 1) * BLOCK, :].astype(f32))
        gs_sum[4:5, :] += jnp.sum(cot, axis=0, keepdims=True)
    final.start()
    line_ref[here.dp] = jnp.concatenate(
        [gb_sum[0:2, :], gs_sum[0:5, :], jnp.zeros((1, d), f32)]
    )
    line = Exchange(line_ref, line_sem, here.dp, here.n, lambda to: (to, here.t))
    cross = Exchange(cross_ref, cross_sem, here.t, here.ways, lambda to: (here.dp, to))
    collect(now)
    pass_on(now)
    line.start()
    for k in range(1, here.majors):
        final.add(k)
        if k == 1:
            total = weights.finish()
            gi_ref[...] = total[:, :hidden]
            gd_ref[...] = total[:, hidden : 2 * hidden]
            go_ref[...] = total[:, 2 * hidden : 2 * hidden + width].T
        final.forward(k)
    summed = line.total()
    for k in range(3):
        gbq_ref[k : k + 1, :] = summed[0:1, k * padded : k * padded + width]
    gb_ref[...] = summed[1, :]
    cross_ref[here.t] = summed
    cross.start()

    def grad_copy(c):
        return pltpu.make_async_copy(gn_own.at[c], gx_out.at[pl.ds(c * BLOCK, BLOCK)], out_sems.at[1 + c])

    for c in range(per):
        far_block(c).wait()
    for c in range(per):
        at = slice(c * BLOCK, (c + 1) * BLOCK)
        normed, inv_std = norm_rows(tokens_ref[at, :].astype(f32))
        grad_normed = gn_own[c] + gn_far[c].astype(f32)
        gn_own[c] = cot_ref[at, :].astype(f32) + inv_std * (
            grad_normed
            - jnp.mean(grad_normed, axis=1, keepdims=True)
            - normed * jnp.mean(grad_normed * normed, axis=1, keepdims=True)
        )
        grad_copy(c).start()
    summed = cross.total()
    for k in range(2):
        product, plain = summed[2 + 2 * k : 3 + 2 * k, :], summed[3 + 2 * k : 4 + 2 * k, :]
        gain, bias = norm_ref[2 * k : 2 * k + 1, :], norm_ref[2 * k + 1 : 2 * k + 2, :]
        small_ref[2 * k : 2 * k + 1, :] = (product - bias * plain) / gain
        small_ref[2 * k + 1 : 2 * k + 2, :] = plain
    small_ref[4:5, :] = summed[6:7, :]
    for slot in range(2 * per):
        near_block(slot // per * 2 * per + (1 - here.core) * per + slot % per).wait_send()
    for one in (rows, cots, proj_w, in_w, down_w, line, cross):
        one.finish()
    output_copy().wait()
    for c in range(per):
        grad_copy(c).wait()
    total = final.finish()
    for k in range(3):
        gq_ref[k] = total[:, k * width : (k + 1) * width]


def layer(length, tokens, cot, norms, wq, bq, wo, wi, bi, wd, biases, table):
    local, d = tokens.shape
    _, side, width = wq.shape
    hidden = wi.shape[1]
    heads = width // HD
    padded = round_up(width + 3, LANES)
    n, ways = lax.axis_size("dp"), lax.axis_size("tensor")
    majors = n // 2
    rows = local * ways
    blocks, per = rows // BLOCK, local // BLOCK
    assert rows == LMAX and length.shape[0] == 1
    assert ways == 4 and per == 2 and n % 4 == 0 and padded == BLOCK and heads == 3
    assert 3 * padded == d == hidden == side * n
    vmem = pl.BlockSpec(memory_space=pltpu.VMEM)
    hbm = pl.BlockSpec(memory_space=pl.ANY)
    row_blocks = pltpu.VMEM((blocks, BLOCK, d), low)
    head_blocks = pltpu.VMEM((blocks, heads * BLOCK, padded), low)
    columns = hidden + wd.shape[1] + padded
    outs = [
        jax.ShapeDtypeStruct((local, d), f32),
        jax.ShapeDtypeStruct((local, d), f32),
        jax.ShapeDtypeStruct((3, side, width), f32),
        jax.ShapeDtypeStruct((3, width), f32),
        jax.ShapeDtypeStruct((width, side), f32),
        jax.ShapeDtypeStruct((side, hidden), f32),
        jax.ShapeDtypeStruct((hidden,), f32),
        jax.ShapeDtypeStruct((side, hidden), f32),
        jax.ShapeDtypeStruct((5, d), f32),
    ]
    args = (tokens, cot, *norms, wq, bq, wo, wi, bi, wd, *biases, table)
    return pl.pallas_call(
        layer_kernel,
        name="layer",
        in_specs=[pl.BlockSpec(memory_space=pltpu.SMEM)] + [vmem] * len(args),
        out_specs=[hbm, hbm] + [vmem] * (len(outs) - 2),
        out_shape=outs,
        scratch_shapes=[
            pltpu.VMEM((8, d), f32),
            pltpu.VMEM((1, 3 * padded), f32),
            pltpu.VMEM((side, 3 * padded), low),
            pltpu.VMEM((side, hidden + padded), low),
            pltpu.VMEM((n, side, 3 * padded), low),
            pltpu.VMEM((n, side, hidden), low),
            pltpu.VMEM((n, side, hidden + padded), low),
            row_blocks, row_blocks, row_blocks, row_blocks,
            pltpu.VMEM((blocks, BLOCK, 3 * padded), low),
            head_blocks, head_blocks,
            pltpu.VMEM((blocks, BLOCK, padded), low),
            pltpu.VMEM((blocks * heads, BLOCK, BLOCK), f32),
            pltpu.VMEM((blocks, width, BLOCK), low),
            pltpu.VMEM((d, hidden), f32),
            pltpu.VMEM((d, hidden + padded), f32),
            pltpu.VMEM((8, d), f32),
            pltpu.VMEM((8, d), f32),
            pltpu.VMEM((n, side, columns), low),
            pltpu.SemaphoreType.DMA((2 * per + 3,)),
            pltpu.SemaphoreType.DMA((1 + per,)),
            pltpu.SemaphoreType.DMA((2, 3 * per)),
            pltpu.SemaphoreType.DMA((2, 3 * per)),
            *gather_scratch(majors), *gather_scratch(majors), *gather_scratch(majors),
            pltpu.VMEM((2 * per, BLOCK, d), low),
            pltpu.VMEM((per, BLOCK, d), f32),
            pltpu.VMEM((per, BLOCK, d), low),
            pltpu.SemaphoreType.DMA((2, 2 * per)),
            pltpu.SemaphoreType.DMA((2, per)),
            pltpu.VMEM((2, per, BLOCK, d), low),
            pltpu.VMEM((per, BLOCK, d), low),
            pltpu.SemaphoreType.DMA((2, 2)),
            pltpu.SemaphoreType.DMA((2, 1)),
            *scatter_scratch(majors, side, columns),
            pltpu.VMEM((n, side, 3 * width), low),
            *scatter_scratch(majors, side, 3 * width),
            pltpu.VMEM((n, 8, d), f32),
            pltpu.VMEM((ways, 8, d), f32),
            pltpu.SemaphoreType.DMA((2, n)),
            pltpu.SemaphoreType.DMA((2, ways)),
        ],
        compiler_params=pltpu.CompilerParams(
            vmem_limit_bytes=VMEM, collective_id=0, has_side_effects=True
        ),
    )(length, *args)


def per_device(
    tokens, cotangent, seq_lengths, norm1_gain, norm1_bias, norm2_gain, norm2_bias,
    w_qkv, b_qkv, w_attn_out, w_in, b_in, w_down, b_out, b_down,
):
    output, grad_x, g_qkv, gb_qkv, g_out, g_in, gb_in, g_down, small = layer(
        seq_lengths, tokens, cotangent, (norm1_gain, norm1_bias, norm2_gain, norm2_bias),
        w_qkv.transpose(1, 0, 2), b_qkv, w_attn_out, w_in, b_in, w_down.T, (b_out, b_down),
        jnp.asarray(rotary_base()),
    )
    return output, grad_x, g_qkv.transpose(1, 0, 2), gb_qkv, g_out, g_in, gb_in, g_down.T, small


def solution(mesh):
    rows = P(("dp", "tensor"), None)
    placed = (
        rows, rows, P("dp"), P(), P(), P(), P(), P("dp", None, "tensor"), P(None, "tensor"),
        P("tensor", "dp"), P("dp", "tensor"), P("tensor"), P("tensor", "dp"), P(), P(),
    )
    return jax.shard_map(
        per_device,
        mesh=mesh,
        in_specs=placed,
        out_specs=(
            rows, rows, P("dp", None, "tensor"), P(None, "tensor"), P("tensor", "dp"),
            P("dp", "tensor"), P("tensor"), P("tensor", "dp"), P(),
        ),
        check_vma=False,
    )
```

```python
import functools
import math

import jax
import jax.numpy as jnp
import numpy as np
from jax import lax
from jax.experimental import pallas as pl
from jax.experimental.pallas import tpu as pltpu
from jax.sharding import PartitionSpec as P

HD = 64
ROT = 16
LMAX = 2048
LANES = 128
EPS = 1e-05
BLOCK = 256
FAST = 64
VMEM = 66 * 1024 * 1024

f32 = jnp.float32
low = jnp.bfloat16

NN = (((1,), (0,)), ((), ()))
NT = (((1,), (1,)), ((), ()))
TN = (((0,), (0,)), ((), ()))


def dot(a, b, dims):
    return lax.dot_general(a, b, dims, preferred_element_type=f32)


def round_up(n, m):
    return (n + m - 1) // m * m


def rotary_base():
    d = np.arange(LANES) % HD
    half = ROT // 2
    inverse = np.where(d < ROT, np.exp((d % half) * (-2.0 * math.log(10000.0) / ROT)), 0.0)
    slow = np.arange(0, LMAX, FAST)[:, None] * inverse
    fast = np.arange(FAST)[:, None] * inverse
    return np.concatenate([np.cos(slow), np.sin(slow), np.cos(fast), np.sin(fast)]).astype(
        np.float32
    )


def rotary_rows(table_ref, block):
    slow_rows = LMAX // FAST
    fast_cos = table_ref[2 * slow_rows : 2 * slow_rows + FAST, :]
    fast_sin = table_ref[2 * slow_rows + FAST :, :]
    cosines, sines = [], []
    for part in range(BLOCK // FAST):
        row = block * (BLOCK // FAST) + part
        slow_cos = table_ref[pl.ds(row, 1), :]
        slow_sin = table_ref[pl.ds(row + slow_rows, 1), :]
        cosines.append(slow_cos * fast_cos - slow_sin * fast_sin)
        sines.append(slow_sin * fast_cos + slow_cos * fast_sin)
    cosine, sine = jnp.concatenate(cosines), jnp.concatenate(sines)
    d = lax.broadcasted_iota(jnp.int32, cosine.shape, 1) % HD
    return (
        cosine,
        jnp.where(d < ROT // 2, -sine, 0.0),
        jnp.where((d >= ROT // 2) & (d < ROT), sine, 0.0),
    )


def rotate(values, tables, sign):
    cosine, from_right, from_left = tables
    half = ROT // 2
    turned = []
    for first in range(0, values.shape[1], LANES):
        t = values[:, first : first + LANES]
        side = (
            pltpu.roll(t, LANES - half, axis=1) * from_right
            + pltpu.roll(t, half, axis=1) * from_left
        )
        turned.append(t * cosine + side if sign > 0 else t * cosine - side)
    return jnp.concatenate(turned, axis=1)


def three_terms(value):
    first = value.astype(low).astype(f32)
    second = (value - first).astype(low).astype(f32)
    return first, second, value - first - second


MESH = pl.DeviceIdType.MESH


class Place:
    def __init__(self):
        self.dp, self.t = lax.axis_index("dp"), lax.axis_index("tensor")
        self.n, self.ways = lax.axis_size("dp"), lax.axis_size("tensor")
        self.majors = self.n // 2
        self.a, self.b = self.dp // 2, self.dp % 2
        self.chip, self.core = self.t // 2, self.t % 2
        self.upper = self.a * 2 // self.majors
        self.near = (self.dp, self.t + 1 - 2 * self.core)
        self.across = (self.dp, (self.t + 2) % 4)
        self.beside = (self.dp + 1 - 2 * self.b, self.t)

    def major(self, k):
        return ((self.a + k) % self.majors, (self.a + k) % self.majors * 2 + self.b)

    def shard(self, kind):
        return (self.chip + kind // 2) % 2 * 2 + (self.core + kind % 2) % 2

    def greet(self):
        barrier = pltpu.get_barrier_semaphore()
        others = [self.near, self.across, (self.dp, 3 - self.t)]
        others += [((self.dp + k) % self.n, self.t) for k in range(1, self.n)]
        for other in others:
            pl.semaphore_signal(barrier, inc=1, device_id=other, device_id_type=MESH)
        pl.semaphore_wait(barrier, len(others))


def send(src, dst, sems, k, to):
    return pltpu.make_async_remote_copy(
        src_ref=src,
        dst_ref=dst,
        send_sem=sems.at[0, k],
        recv_sem=sems.at[1, k],
        device_id=to,
        device_id_type=MESH,
    )


def plus(*terms):
    return functools.reduce(jnp.add, [t.astype(f32) for t in terms])


class Scatter:
    def __init__(self, place, mine, got, last, sems):
        self.p, self.mine, self.got, self.last, self.pairs, self.lines = place, mine, got, last, *sems

    def first(self, k):
        p = self.p
        mine = self.mine.at[p.major(k)[0] * 2 + 1 - p.b]
        return send(mine, self.got.at[k], self.pairs, k, p.beside)

    def second(self, k):
        to = (self.p.major(k)[1], self.p.t)
        return send(self.got.at[k], self.last.at[k - 1], self.lines, k - 1, to)

    def order(self, number):
        p = self.p
        half = p.majors // 2
        if number <= half:
            a = (1 - p.upper) * half + number - 1
        else:
            a = p.upper * half + (p.a % half + number - half) % half
        return (a - p.a + p.majors) % p.majors

    def start_half(self, turn):
        half = self.p.majors // 2
        for number in range(turn * half + 1, (turn + 1) * half + 1):
            self.first(self.order(number)).start()

    def add(self, number):
        k = self.order(number)
        self.first(k).wait_recv()
        self.got[k] = plus(self.mine[self.p.major(k)[1]], self.got[k]).astype(self.got.dtype)

    def forward(self, number):
        self.second(self.order(number)).start()

    def finish(self):
        p = self.p
        for k in range(p.majors):
            self.first(k).wait_send()
        self.first(0).wait_recv()
        for k in range(1, p.majors):
            self.second(k).wait()
        return plus(self.mine[p.dp], self.got[0], *[self.last[k] for k in range(p.majors - 1)])


class Gather:
    def __init__(self, place, mine, whole, sems):
        self.p, self.mine, self.whole, self.lines, self.pairs = place, mine, whole, *sems

    def line(self, way, hop):
        p = self.p
        step = 1 - 2 * way
        origin = (p.a - step * hop) * 2 + p.b
        mine = self.mine if hop == 0 else self.whole.at[origin]
        to = ((p.a + step) * 2 + p.b, p.t)
        return send(mine, self.whole.at[origin], self.lines, way * (p.majors - 1) + hop, to)

    def pair(self, way, hop):
        p = self.p
        origin = (p.a - (1 - 2 * way) * hop) * 2 + p.b
        mine = self.mine if hop == 0 else self.whole.at[origin]
        return send(mine, self.whole.at[origin], self.pairs, way * p.majors + hop, p.beside)

    def came(self, way, hop):
        p = self.p
        return p.a >= hop if way == 0 else p.a <= p.majors - 1 - hop

    def goes(self, way, hop):
        p = self.p
        return self.came(way, hop) & (p.a < p.majors - 1 if way == 0 else p.a > 0)

    def start(self):
        for way in range(2):

            @pl.when(self.goes(way, 0))
            def _():
                self.line(way, 0).start()

        self.pair(0, 0).start()

    def forward(self, hop):
        for way in range(2):

            @pl.when(self.came(way, hop))
            def _():
                self.arrival(way, hop).wait_recv()
                if hop < self.p.majors - 1:

                    @pl.when(self.goes(way, hop))
                    def _():
                        self.line(way, hop).start()

                self.pair(way, hop).start()

    def arrival(self, way, hop):
        p = self.p
        step = 1 - 2 * way
        block = self.whole.at[(p.a - step * hop) * 2 + p.b]
        back = ((p.a - step) * 2 + p.b, p.t)
        return send(block, block, self.lines, way * (p.majors - 1) + hop - 1, back)

    def arrived(self):
        p = self.p
        for way in range(2):
            for hop in range(way, p.majors):

                @pl.when(self.came(way, hop))
                def _():
                    other = self.whole.at[(p.a - (1 - 2 * way) * hop) * 2 + 1 - p.b]
                    send(other, other, self.pairs, way * p.majors + hop, p.beside).wait_recv()

    def finish(self):
        for way in range(2):
            for hop in range(self.p.majors):
                if hop < self.p.majors - 1:

                    @pl.when(self.goes(way, hop))
                    def _():
                        self.line(way, hop).wait_send()

                if way == 0 or hop > 0:

                    @pl.when(self.came(way, hop))
                    def _():
                        self.pair(way, hop).wait_send()


def gather_scratch(majors):
    return [
        pltpu.SemaphoreType.DMA((2, 2 * (majors - 1))),
        pltpu.SemaphoreType.DMA((2, 2 * majors)),
    ]


class Rows:
    def __init__(self, place, mine, whole, sems):
        self.p, self.mine, self.whole, self.sems = place, mine, whole, sems
        self.per = mine.shape[0] // BLOCK

    def copy(self, kind, c):
        p = self.p
        if kind == 2:
            block = self.whole.at[p.across[1] * self.per + c]
            return send(block, block, self.sems, 2 * self.per + c, p.near)
        to = p.near if kind == 0 else p.across
        mine = self.mine.at[pl.ds(c * BLOCK, BLOCK)]
        return send(mine, self.whole.at[p.t * self.per + c], self.sems, kind * self.per + c, to)

    def start(self):
        for c in range(self.per):
            for kind in range(2):
                self.copy(kind, c).start()

    def arrived(self, kind, c):
        self.copy(kind, c).wait_recv()

    def forward(self, c):
        self.copy(1, c).wait_recv()
        self.copy(2, c).start()

    def released(self):
        for c in range(self.per):
            self.copy(2, c).wait_send()

    def finish(self):
        for c in range(self.per):
            for kind in range(2):
                self.copy(kind, c).wait_send()


class Exchange:
    def __init__(self, slots, sems, me, count, device):
        self.slots, self.sems, self.me, self.count, self.device = slots, sems, me, count, device

    def copy(self, k, source):
        return pltpu.make_async_remote_copy(
            src_ref=self.slots.at[source],
            dst_ref=self.slots.at[source],
            send_sem=self.sems.at[0, k],
            recv_sem=self.sems.at[1, source],
            device_id=self.device((self.me + k) % self.count),
            device_id_type=MESH,
        )

    def start(self):
        for k in range(1, self.count):
            self.copy(k, self.me).start()

    def total(self):
        for k in range(1, self.count):
            self.copy(k, (self.me + k) % self.count).wait_recv()
        return functools.reduce(jnp.add, [self.slots[k] for k in range(self.count)])

    def finish(self):
        for k in range(1, self.count):
            self.copy(k, self.me).wait_send()


def scatter_scratch(majors, rows, columns):
    return [
        pltpu.VMEM((majors, rows, columns), low),
        pltpu.VMEM((majors - 1, rows, columns), low),
        pltpu.SemaphoreType.DMA((2, majors)),
        pltpu.SemaphoreType.DMA((2, majors - 1)),
    ]


def flat(blocks_ref):
    n, side, columns = blocks_ref.shape
    if side % 16 == 0:
        return blocks_ref[...].reshape(n * side, columns)
    return jnp.concatenate([blocks_ref[k].astype(f32) for k in range(n)]).astype(low)


def norm_rows(x):
    shifted = x - jnp.mean(x, axis=1, keepdims=True)
    inv_std = lax.rsqrt(jnp.mean(shifted * shifted, axis=1, keepdims=True) + EPS)
    return shifted * inv_std, inv_std


def layer_kernel(
    length_ref, tokens_ref, cot_ref, g1_ref, b1_ref, g2_ref, b2_ref, wq_ref, bq_ref, wo_ref, wi_ref,
    bi_ref, wd_ref, bo_ref, bd_ref, table_ref,
    out_out, gx_out, spill_out, gq_ref, gbq_ref, go_ref, gi_ref, gb_ref, gd_ref, small_ref,
    norm_ref, bias_ref, wq_mine, wd_mine, wq_all, wi_all, wd_all,
    x_all, first_ref, second_ref, cot_all, qkv_ref, qx_ref, dox_ref, context_ref, pool_ref,
    keyt_ref, queryt_ref, valuet_ref, mixed_ref, top_ref, gwq_sum, stage_ref, gb_sum, gs_sum, gw_ref, own_sems, out_sems, x_sems, cot_sems,
    wq_lines, wq_pairs, wi_lines, wi_pairs, wd_lines, wd_pairs,
    gn_near, gn_far, gn_sem1, gn_sem2,
    br_near, br_far, br_sem1, br_sem2,
    w_got, w_last, w_sem1, w_sem2,
    gq_low, q_got, q_last, q_sem1, q_sem2,
    line_ref, cross_ref, line_sem, cross_sem,
):
    here = Place()
    blocks, _, d = x_all.shape
    local = tokens_ref.shape[0]
    per = local // BLOCK
    width = wq_ref.shape[2]
    heads = width // HD
    padded = qkv_ref.shape[2] // 3
    hidden = wi_ref.shape[1]
    side = wi_ref.shape[0]
    scale = HD ** (-0.5)
    to_power = scale * math.log2(math.e)
    tall = valuet_ref.shape[1] // heads
    lane = lax.broadcasted_iota(jnp.int32, (BLOCK, padded), 1)
    of_head = [(lane >= h * HD) & (lane < (h + 1) * HD) for h in range(heads)]
    extra = (lane >= width) & (lane < width + 3)

    rows = Rows(here, tokens_ref, x_all, x_sems)
    cots = Rows(here, cot_ref, cot_all, cot_sems)
    proj_w = Gather(here, wq_mine, wq_all, (wq_lines, wq_pairs))
    in_w = Gather(here, wi_ref, wi_all, (wi_lines, wi_pairs))
    down_w = Gather(here, wd_mine, wd_all, (wd_lines, wd_pairs))

    wq_mine[...] = jnp.zeros_like(wq_mine)
    wd_mine[:, hidden:] = jnp.zeros((side, padded), low)
    bias_ref[...] = jnp.zeros_like(bias_ref)
    for k in range(3):
        wq_mine[:, k * padded : k * padded + width] = wq_ref[k]
        bias_ref[0:1, k * padded : k * padded + width] = bq_ref[k : k + 1, :]
    wd_mine[:, :hidden] = wd_ref[...]
    wd_mine[:, hidden : hidden + width] = wo_ref[...].astype(f32).T.astype(low)
    for k, ref in enumerate((g1_ref, b1_ref, g2_ref, b2_ref, bo_ref, bd_ref, bi_ref)):
        norm_ref[k, :] = ref[...]

    here.greet()
    proj_w.start()
    rows.start()
    own = [
        pltpu.make_async_copy(tokens_ref.at[pl.ds(c * BLOCK, BLOCK)], x_all.at[here.t * per + c], own_sems.at[c])
        for c in range(per)
    ]
    own += [
        pltpu.make_async_copy(cot_ref.at[pl.ds(c * BLOCK, BLOCK)], cot_all.at[here.t * per + c], own_sems.at[per + c])
        for c in range(per)
    ]
    own += [
        pltpu.make_async_copy(mine, whole.at[here.dp], own_sems.at[2 * per + k])
        for k, (mine, whole) in enumerate(((wq_mine, wq_all), (wi_ref, wi_all), (wd_mine, wd_all)))
    ]
    for copy in own:
        copy.start()

    def norm(kind, c):
        r = here.shard(kind) * per + c
        normed, _ = norm_rows(x_all[r].astype(f32))
        first_ref[r] = (normed * norm_ref[0:1, :] + norm_ref[1:2, :]).astype(low)
        second_ref[r] = (normed * norm_ref[2:3, :] + norm_ref[3:4, :]).astype(low)

    def project(kind, c):
        r = here.shard(kind) * per + c
        projected = dot(first_ref[r], flat(wq_all), NN) + bias_ref[...]
        tables = rotary_rows(table_ref, r)
        queries = rotate(projected[:, :padded], tables, 1)
        queryt_ref[r] = queries.T[:width].astype(low)
        qkv_ref[r, :, :padded] = queries.astype(low)
        keys = rotate(projected[:, padded : 2 * padded], tables, 1)
        keyt_ref[r] = keys.T[:width].astype(low)
        qkv_ref[r, :, padded : 2 * padded] = jnp.where(extra, 1.0, keys).astype(low)
        values = projected[:, 2 * padded :]
        qkv_ref[r, :, 2 * padded :] = jnp.where(extra, 1.0, values).astype(low)
        turned = values.T.astype(low)
        for h in range(heads):
            valuet_ref[r, h * tall : h * tall + HD, :] = turned[h * HD : (h + 1) * HD]
            valuet_ref[r, h * tall + HD : (h + 1) * tall, :] = jnp.ones((tall - HD, BLOCK), low)

    for c in range(per):
        own[c].wait()

    @pl.loop(0, per)
    def _(c):
        norm(0, c)

    for c in range(per):
        rows.arrived(0, c)
    proj_w.forward(1)

    @pl.loop(0, per)
    def _(c):
        norm(1, c)

    for k in range(2, here.majors - 1):
        proj_w.forward(k)
    for c in range(per - 1):
        rows.forward(c)
    proj_w.forward(here.majors - 1)
    in_w.start()
    cots.start()
    for c in range(per - 1):
        norm(2, c)
    for c in range(per - 1):
        rows.arrived(2, c)
        norm(3, c)
    own[2 * per].wait()
    proj_w.arrived()

    @pl.loop(0, per + 2 * (per - 1))
    def _(number):
        @pl.when(number == per + 1)
        def _():
            rows.forward(per - 1)

        @pl.when(number == per - 1)
        def _():
            in_w.forward(1)

        later = number // per
        project(1 + later + number % per * later, number % per * (1 - later))

    @pl.loop(0, per)
    def _(c):
        project(0, c)

    for k in range(2, here.majors - 1):
        in_w.forward(k)
    norm(2, per - 1)
    project(2, per - 1)
    rows.arrived(2, per - 1)
    norm(3, per - 1)
    project(3, per - 1)

    def spilled():
        return pltpu.make_async_copy(first_ref, spill_out, out_sems.at[1 + per])

    def restored():
        return pltpu.make_async_copy(spill_out, first_ref, out_sems.at[1 + per])

    spilled().start()

    def in_fours(count, body):
        @pl.loop(0, count // 4)
        def _(number):
            for k in range(4):
                body(4 * number + k)

        for size in (2, 1):

            @pl.when(count // size % 2 == 1)
            def _():
                for k in range(size):
                    body(count // (2 * size) * (2 * size) + k)

    in_w.forward(here.majors - 1)
    down_w.start()

    @pl.loop(0, blocks)
    def _(i):
        for k in range(1, here.majors):

            @pl.when(i == min(2 * k, blocks - 1))
            def _():
                down_w.forward(k)

        for c in range(per):

            @pl.when(i == blocks - per + c)
            def _():
                cots.forward(c)

        q = qkv_ref[i, :, :padded].astype(f32)
        for h in range(heads):
            qx_ref[i, h * BLOCK : (h + 1) * BLOCK, :] = jnp.where(of_head[h], q, 0.0).astype(low)
        query = qx_ref[i]
        parts = [slice(h * BLOCK, (h + 1) * BLOCK) for h in range(heads)]

        def scores(j):
            return dot(qkv_ref[j, :, padded : 2 * padded], query, NT)

        def highest(s):
            return jnp.max(s.reshape(-1, 8, heads * BLOCK), axis=0)

        def keep(j, s):
            for h in range(heads):
                pool_ref[j * heads + h] = s[:, parts[h]]

        diagonal = scores(i)
        key_at = lax.broadcasted_iota(jnp.int32, diagonal.shape, 0)
        query_at = lax.broadcasted_iota(jnp.int32, diagonal.shape, 1) % BLOCK
        diagonal = jnp.where(key_at <= query_at, diagonal, -1e30)
        keep(i, diagonal)
        top_ref[...] = highest(diagonal)

        def first_pass(j):
            s = scores(j)
            keep(j, s)
            top_ref[...] = jnp.maximum(top_ref[...], highest(s))

        in_fours(i, first_pass)
        top = jnp.max(top_ref[...], axis=0, keepdims=True)
        mixed_ref[...] = jnp.zeros_like(mixed_ref)

        def second_pass(j):
            for h in range(heads):
                p = jnp.exp2((pool_ref[j * heads + h] - top[:, parts[h]]) * to_power).astype(low)
                at = slice(h * tall, (h + 1) * tall)
                mixed_ref[at, :] += dot(valuet_ref[j, at, :], p, NN)

        in_fours(i + 1, second_pass)
        mixed, terms = [], []
        for h in range(heads):
            total = mixed_ref[h * tall + HD : h * tall + HD + 1, :]
            mixed.append(mixed_ref[h * tall : h * tall + HD, :] * (1.0 / total))
            terms.append(jnp.concatenate(three_terms(-top[:, parts[h]] - jnp.log(total) / scale)))
        terms = jnp.concatenate(terms, axis=1)
        side_rows = width - (padded - LANES)
        columns = jnp.concatenate(
            [
                jnp.zeros((side_rows, heads * BLOCK), f32),
                terms,
                jnp.zeros((LANES - side_rows - 3, heads * BLOCK), f32),
            ]
        ).T
        for h in range(heads):
            right = jnp.where(of_head[h], q, 0.0)[:, padded - LANES :]
            qx_ref[i, parts[h], padded - LANES :] = (right + columns[parts[h]]).astype(low)
        mixed.append(jnp.zeros((padded - width, BLOCK), f32))
        context_ref[i] = jnp.concatenate(mixed).T.astype(low)

    grad_ref, act_ref, hidden_ref, gradt_ref = cot_all, x_all, first_ref, valuet_ref
    own[2 * per + 1].wait()
    in_w.arrived()
    rows.released()

    @pl.loop(0, blocks)
    def _(r):
        u = dot(second_ref[r], flat(wi_all), NN) + norm_ref[6:7, :]
        cdf = 0.5 * (1.0 + lax.erf(u * (1.0 / math.sqrt(2.0))))
        act_ref[r] = (u * cdf).astype(low)
        slope = cdf + u * (jnp.exp(-0.5 * u * u) * (1.0 / math.sqrt(2.0 * math.pi)))
        for k in range(3):
            pool_ref[3 * r + k] = slope[:, k * BLOCK : (k + 1) * BLOCK]

    for c in range(per):
        cots.arrived(0, c)
        cots.arrived(2, c)
    for copy in own[per : 2 * per] + own[2 * per + 2 :]:
        copy.wait()
    gb_sum[...] = jnp.zeros_like(gb_sum)
    gs_sum[...] = jnp.zeros_like(gs_sum)
    cots.released()
    spilled().wait()
    down_w.arrived()

    @pl.loop(0, blocks)
    def _(r):
        row = lax.broadcasted_iota(jnp.int32, (BLOCK, d), 0) + r * BLOCK
        grad = jnp.where(row < length_ref[0], cot_all[r].astype(f32), 0.0).astype(low)
        grad_ref[r] = grad
        back = dot(grad, flat(wd_all), NN)
        slope = jnp.concatenate([pool_ref[3 * r + k] for k in range(3)], axis=1)
        grad_hidden = back[:, :hidden] * slope
        gb_sum[1:2, :] += jnp.sum(grad_hidden, axis=0, keepdims=True)
        hidden_ref[r] = grad_hidden.astype(low)

        grad_context = back[:, hidden:].astype(low).astype(f32)
        gradt_ref[r, :width, :] = grad_context.T[:width].astype(low)
        product = grad_context * context_ref[r].astype(f32)
        for h in range(heads):
            extended = jnp.where(of_head[h], grad_context, 0.0)
            delta = jnp.sum(jnp.where(of_head[h], product, 0.0), axis=1, keepdims=True)
            for k, term in enumerate(three_terms(-delta)):
                extended = jnp.where(lane == width + k, term, extended)
            dox_ref[r, h * BLOCK : (h + 1) * BLOCK, :] = extended.astype(low)

    weights = Scatter(here, gw_ref, w_got, w_last, (w_sem1, w_sem2))
    final = Scatter(here, gq_low, q_got, q_last, (q_sem1, q_sem2))
    half = d // 2
    rows_total = blocks * BLOCK

    @pl.loop(0, 2)
    def _(turn):
        which = (1 - turn) * (1 - here.upper) + turn * here.upper
        at = pl.ds(pl.multiple_of(which * half, LANES), half)
        all_rows = lambda ref: ref[...].reshape(rows_total, ref.shape[2])
        mine = second_ref[:, :, at].reshape(rows_total, half)
        first_block = which * (here.n // 2)
        side_blocks = pl.ds(first_block, here.n // 2)
        gwi = dot(mine, all_rows(hidden_ref), TN).reshape(here.n // 2, side, hidden)
        gw_ref[side_blocks, :, :hidden] = gwi.astype(low)
        @pl.when(turn == 1)
        def _():
            weights.start_half(0)

        mine = grad_ref[:, :, at].reshape(rows_total, half)
        gwd = dot(mine, all_rows(act_ref), TN).reshape(here.n // 2, side, hidden)
        gw_ref[side_blocks, :, hidden : 2 * hidden] = gwd.astype(low)
        gwd = dot(mine, all_rows(context_ref), TN).reshape(here.n // 2, side, padded)
        gw_ref[side_blocks, :, 2 * hidden :] = gwd.astype(low)

    branch_ref, part_ref = cot_all, second_ref

    def near_branch(chip):
        owner = chip * 2 + 1 - here.core
        return send(
            branch_ref.at[pl.ds(owner * per, per)], br_near.at[chip], br_sem1, chip, here.near
        )

    def far_branch():
        return send(br_near.at[1 - here.chip], br_far, br_sem2, 0, here.across)

    @pl.loop(0, blocks)
    def _(number):
        r = here.shard(3 - number // per) * per + number % per

        @pl.when(number == per + 1)
        def _():
            near_branch(1 - here.chip).start()

        @pl.when(number == 2 * per + 1)
        def _():
            near_branch(1 - here.chip).wait_recv()

            @pl.loop(0, per)
            def _(c):
                mine = branch_ref[here.across[1] * per + c]
                br_near[1 - here.chip, c] = plus(mine, br_near[1 - here.chip, c]).astype(low)

        @pl.when(number == 3 * per + 1)
        def _():
            near_branch(here.chip).start()

        second = second_ref[r].astype(f32)
        part = dot(hidden_ref[r], flat(wi_all), NT)
        both = jnp.concatenate([act_ref[r], context_ref[r]], axis=1)
        branch_ref[r] = dot(both, flat(wd_all), NT).astype(low)
        gs_sum[2:3, :] += jnp.sum(part * second, axis=0, keepdims=True)
        gs_sum[3:4, :] += jnp.sum(part, axis=0, keepdims=True)
        part_ref[r] = (part * norm_ref[2:3, :]).astype(low)

        @pl.when(number == 0)
        def _():
            weights.start_half(1)

        @pl.when(number == 2 * per + 1)
        def _():
            far_branch().start()

    restored().start()
    gn_ref = x_all
    gwq_sum[...] = jnp.zeros_like(gwq_sum)
    pool_ref[...] = jnp.zeros_like(pool_ref)

    last = blocks - 1

    def block_of(number):
        return number // 2 + number % 2 * (last - number // 2 * 2)

    def slot_of(r):
        return r // per // 2 * per + r % per

    def near_block(r):
        return send(gn_ref.at[r], gn_near.at[slot_of(r)], gn_sem1, slot_of(r), here.near)

    def far_block(c):
        mine = gn_near.at[(1 - here.chip) * per + c]
        return send(mine, gn_far.at[c], gn_sem2, c, here.across)

    def hand_over(r):
        @pl.when(r // per % 2 != here.core)
        def _():
            near_block(r).start()

    def collect(r):
        owner = r // per

        @pl.when(owner % 2 == here.core)
        def _():
            near_block(r).wait_recv()

        @pl.when((owner % 2 == here.core) & (owner // 2 != here.chip))
        def _():
            gn_near[slot_of(r)] = plus(gn_ref[r], gn_near[slot_of(r)]).astype(low)

    def pass_on(r):
        owner = r // per

        @pl.when((owner % 2 == here.core) & (owner // 2 != here.chip))
        def _():
            far_block(r % per).start()

    def pair(i, j, own):
        keys, values = qkv_ref[j, :, padded : 2 * padded], qkv_ref[j, :, 2 * padded :]
        query, dout = qx_ref[i], dox_ref[i]
        p = jnp.exp2(dot(query, keys, NT) * to_power)
        if own:
            query_at = lax.broadcasted_iota(jnp.int32, p.shape, 0) % BLOCK
            key_at = lax.broadcasted_iota(jnp.int32, p.shape, 1)
            p = jnp.where(key_at <= query_at, p, 0.0)
        ds = (p * dot(dout, values, NT)).astype(low)
        p = p.astype(low)
        for h in range(heads):
            at, part = slice(h * HD, (h + 1) * HD), slice(h * BLOCK, (h + 1) * BLOCK)
            pool_ref[blocks + j, at, :] += dot(gradt_ref[i, at, :], p[part], NN)
            pool_ref[j, at, :] += dot(queryt_ref[i, at, :], ds[part], NN)
            pool_ref[2 * blocks + i, at, :] += dot(keyt_ref[j, at, :], ds[part], NT)

    def kept(c, values):
        row = lax.broadcasted_iota(jnp.int32, (BLOCK, d), 0) + (here.t * per + c) * BLOCK
        return jnp.where(row < length_ref[0], values, 0.0)

    def output_copy():
        return pltpu.make_async_copy(stage_ref.at[:], out_out, out_sems.at[0])

    @pl.loop(0, blocks)
    def _(step):
        for k in range(1, here.majors):

            @pl.when(step == min(k - 1, last - 2))
            def _():
                weights.add(k)

        @pl.when(step > 0)
        def _():
            hand_over(block_of(step - 1))

        turn = step // 2
        odd = step % 2
        now = block_of(step)
        pair(now, now, True)

        for k in range(1, here.majors):

            @pl.when(step == min(k - 1, last - 2))
            def _():
                weights.forward(k)

        @pl.when(step > 0)
        def _():
            collect(block_of(step - 1))

        def next_pair(number):
            other = turn + 1 + number
            pair(other + odd * (last - turn - other), turn + odd * (other - turn), False)

        in_fours(last - step, next_pair)

        @pl.when(step == last // 2)
        def _():
            far_branch().wait()
            for chip in range(2):
                near_branch(chip).wait_send()
            near_branch(here.chip).wait_recv()

            @pl.loop(0, per)
            def _(c):
                total = plus(branch_ref[here.t * per + c], br_near[here.chip, c], br_far[c])
                total += norm_ref[4:5, :] + norm_ref[5:6, :]
                at = pl.ds(pl.multiple_of(c * BLOCK, BLOCK), BLOCK)
                stage_ref[at, :] = tokens_ref[at, :].astype(f32) + kept(c, total)

        tables = rotary_rows(table_ref, now)
        filler = jnp.zeros((BLOCK, padded - width), f32)
        turned = [
            jnp.concatenate([pool_ref[k * blocks + now, :width, :].T, filler], axis=1)
            for k in range(3)
        ]
        projected = jnp.concatenate(
            [
                rotate(turned[2] * scale, tables, -1),
                rotate(turned[0] * scale, tables, -1),
                turned[1],
            ],
            axis=1,
        )
        gb_sum[0:1, :] += jnp.sum(projected, axis=0, keepdims=True)
        proj_low = projected.astype(low)
        @pl.when(step == 0)
        def _():
            restored().wait()

        first = first_ref[now]
        gwq_sum[...] += dot(first, proj_low, TN)
        part = dot(proj_low, flat(wq_all), NT)
        gs_sum[0:1, :] += jnp.sum(part * first.astype(f32), axis=0, keepdims=True)
        gs_sum[1:2, :] += jnp.sum(part, axis=0, keepdims=True)
        gn_ref[now] = (part * norm_ref[0:1, :] + part_ref[now].astype(f32)).astype(low)

        @pl.when(step > 0)
        def _():
            pass_on(block_of(step - 1))

        @pl.when(step == last // 2)
        def _():
            output_copy().start()

    now = block_of(last)
    for block in range(here.n):
        rows_of = slice(block * side, (block + 1) * side)
        gq_low[block] = jnp.concatenate(
            [gwq_sum[rows_of, k * padded : k * padded + width] for k in range(3)], axis=1
        ).astype(low)
    hand_over(now)
    for c in range(per):
        cot = kept(c, cot_ref[c * BLOCK : (c + 1) * BLOCK, :].astype(f32))
        gs_sum[4:5, :] += jnp.sum(cot, axis=0, keepdims=True)
    final.start_half(0)
    final.start_half(1)
    line_ref[here.dp] = jnp.concatenate(
        [gb_sum[0:2, :], gs_sum[0:5, :], jnp.zeros((1, d), f32)]
    )
    line = Exchange(line_ref, line_sem, here.dp, here.n, lambda to: (to, here.t))
    cross = Exchange(cross_ref, cross_sem, here.t, here.ways, lambda to: (here.dp, to))
    collect(now)
    pass_on(now)
    line.start()
    for k in range(1, here.majors):
        final.add(k)
        if k == 1:
            total = weights.finish()
            gi_ref[...] = total[:, :hidden]
            gd_ref[...] = total[:, hidden : 2 * hidden]
            go_ref[...] = total[:, 2 * hidden : 2 * hidden + width].T
        final.forward(k)
    summed = line.total()
    for k in range(3):
        gbq_ref[k : k + 1, :] = summed[0:1, k * padded : k * padded + width]
    gb_ref[...] = summed[1, :]
    cross_ref[here.t] = summed
    cross.start()

    def grad_copy(c):
        at = pl.ds(c * BLOCK, BLOCK)
        return pltpu.make_async_copy(stage_ref.at[at], gx_out.at[at], out_sems.at[1 + c])

    for c in range(per):
        far_block(c).wait()
    output_copy().wait()
    for c in range(per):
        at = slice(c * BLOCK, (c + 1) * BLOCK)
        normed, inv_std = norm_rows(tokens_ref[at, :].astype(f32))
        grad_normed = plus(gn_ref[here.t * per + c], gn_near[here.chip * per + c], gn_far[c])
        stage_ref[at, :] = cot_ref[at, :].astype(f32) + inv_std * (
            grad_normed
            - jnp.mean(grad_normed, axis=1, keepdims=True)
            - normed * jnp.mean(grad_normed * normed, axis=1, keepdims=True)
        )
        grad_copy(c).start()
    summed = cross.total()
    for k in range(2):
        product, plain = summed[2 + 2 * k : 3 + 2 * k, :], summed[3 + 2 * k : 4 + 2 * k, :]
        gain, bias = norm_ref[2 * k : 2 * k + 1, :], norm_ref[2 * k + 1 : 2 * k + 2, :]
        small_ref[2 * k : 2 * k + 1, :] = (product - bias * plain) / gain
        small_ref[2 * k + 1 : 2 * k + 2, :] = plain
    small_ref[4:5, :] = summed[6:7, :]
    for slot in range(2 * per):
        near_block(slot // per * 2 * per + (1 - here.core) * per + slot % per).wait_send()
    for one in (rows, cots, proj_w, in_w, down_w, line, cross):
        one.finish()
    for c in range(per):
        grad_copy(c).wait()
    total = final.finish()
    for k in range(3):
        gq_ref[k] = total[:, k * width : (k + 1) * width]


def layer(length, tokens, cot, norms, wq, bq, wo, wi, bi, wd, biases, table):
    local, d = tokens.shape
    _, side, width = wq.shape
    hidden = wi.shape[1]
    heads = width // HD
    padded = round_up(width + 3, LANES)
    n, ways = lax.axis_size("dp"), lax.axis_size("tensor")
    majors = n // 2
    rows = local * ways
    blocks, per = rows // BLOCK, local // BLOCK
    assert rows == LMAX and length.shape[0] == 1
    assert ways == 4 and per == 2 and n % 4 == 0 and padded == BLOCK and heads == 3
    assert 3 * padded == d == hidden == side * n
    vmem = pl.BlockSpec(memory_space=pltpu.VMEM)
    hbm = pl.BlockSpec(memory_space=pl.ANY)
    row_blocks = pltpu.VMEM((blocks, BLOCK, d), low)
    head_blocks = pltpu.VMEM((blocks, heads * BLOCK, padded), low)
    columns = hidden + wd.shape[1] + padded
    outs = [
        jax.ShapeDtypeStruct((local, d), f32),
        jax.ShapeDtypeStruct((local, d), f32),
        jax.ShapeDtypeStruct((blocks, BLOCK, d), low),
        jax.ShapeDtypeStruct((3, side, width), f32),
        jax.ShapeDtypeStruct((3, width), f32),
        jax.ShapeDtypeStruct((width, side), f32),
        jax.ShapeDtypeStruct((side, hidden), f32),
        jax.ShapeDtypeStruct((hidden,), f32),
        jax.ShapeDtypeStruct((side, hidden), f32),
        jax.ShapeDtypeStruct((5, d), f32),
    ]
    args = (tokens, cot, *norms, wq, bq, wo, wi, bi, wd, *biases, table)
    return pl.pallas_call(
        layer_kernel,
        name="layer",
        in_specs=[pl.BlockSpec(memory_space=pltpu.SMEM)] + [vmem] * len(args),
        out_specs=[hbm] * 3 + [vmem] * (len(outs) - 3),
        out_shape=outs,
        scratch_shapes=[
            pltpu.VMEM((8, d), f32),
            pltpu.VMEM((1, 3 * padded), f32),
            pltpu.VMEM((side, 3 * padded), low),
            pltpu.VMEM((side, hidden + padded), low),
            pltpu.VMEM((n, side, 3 * padded), low),
            pltpu.VMEM((n, side, hidden), low),
            pltpu.VMEM((n, side, hidden + padded), low),
            row_blocks, row_blocks, row_blocks, row_blocks,
            pltpu.VMEM((blocks, BLOCK, 3 * padded), low),
            head_blocks, head_blocks,
            pltpu.VMEM((blocks, BLOCK, padded), low),
            pltpu.VMEM((blocks * heads, BLOCK, BLOCK), f32),
            pltpu.VMEM((blocks, width, BLOCK), low),
            pltpu.VMEM((blocks, width, BLOCK), low),
            pltpu.VMEM((blocks, heads * (HD + 16), BLOCK), low),
            pltpu.VMEM((heads * (HD + 16), BLOCK), f32),
            pltpu.VMEM((8, heads * BLOCK), f32),
            pltpu.VMEM((d, hidden), f32),
            pltpu.VMEM((local, d), f32),
            pltpu.VMEM((8, d), f32),
            pltpu.VMEM((8, d), f32),
            pltpu.VMEM((n, side, columns), low),
            pltpu.SemaphoreType.DMA((2 * per + 3,)),
            pltpu.SemaphoreType.DMA((2 + per,)),
            pltpu.SemaphoreType.DMA((2, 3 * per)),
            pltpu.SemaphoreType.DMA((2, 3 * per)),
            *gather_scratch(majors), *gather_scratch(majors), *gather_scratch(majors),
            pltpu.VMEM((2 * per, BLOCK, d), low),
            pltpu.VMEM((per, BLOCK, d), low),
            pltpu.SemaphoreType.DMA((2, 2 * per)),
            pltpu.SemaphoreType.DMA((2, per)),
            pltpu.VMEM((2, per, BLOCK, d), low),
            pltpu.VMEM((per, BLOCK, d), low),
            pltpu.SemaphoreType.DMA((2, 2)),
            pltpu.SemaphoreType.DMA((2, 1)),
            *scatter_scratch(majors, side, columns),
            pltpu.VMEM((n, side, 3 * width), low),
            *scatter_scratch(majors, side, 3 * width),
            pltpu.VMEM((n, 8, d), f32),
            pltpu.VMEM((ways, 8, d), f32),
            pltpu.SemaphoreType.DMA((2, n)),
            pltpu.SemaphoreType.DMA((2, ways)),
        ],
        compiler_params=pltpu.CompilerParams(
            vmem_limit_bytes=VMEM, collective_id=0, has_side_effects=True
        ),
    )(length, *args)


def per_device(
    tokens, cotangent, seq_lengths, norm1_gain, norm1_bias, norm2_gain, norm2_bias,
    w_qkv, b_qkv, w_attn_out, w_in, b_in, w_down, b_out, b_down,
):
    output, grad_x, _, g_qkv, gb_qkv, g_out, g_in, gb_in, g_down, small = layer(
        seq_lengths, tokens, cotangent, (norm1_gain, norm1_bias, norm2_gain, norm2_bias),
        w_qkv.transpose(1, 0, 2), b_qkv, w_attn_out, w_in, b_in, w_down.T, (b_out, b_down),
        jnp.asarray(rotary_base()),
    )
    return output, grad_x, g_qkv.transpose(1, 0, 2), gb_qkv, g_out, g_in, gb_in, g_down.T, small


def solution(mesh):
    rows = P(("dp", "tensor"), None)
    placed = (
        rows, rows, P("dp"), P(), P(), P(), P(), P("dp", None, "tensor"), P(None, "tensor"),
        P("tensor", "dp"), P("dp", "tensor"), P("tensor"), P("tensor", "dp"), P(), P(),
    )
    return jax.shard_map(
        per_device,
        mesh=mesh,
        in_specs=placed,
        out_specs=(
            rows, rows, P("dp", None, "tensor"), P(None, "tensor"), P("tensor", "dp"),
            P("dp", "tensor"), P("tensor"), P("tensor", "dp"), P(),
        ),
        check_vma=False,
    )
```

```python
import functools
import math

import jax
import jax.numpy as jnp
import numpy as np
from jax import lax
from jax.experimental import pallas as pl
from jax.experimental.pallas import tpu as pltpu
from jax.sharding import PartitionSpec as P

HD = 64
ROT = 16
LMAX = 2048
LANES = 128
EPS = 1e-05
BLOCK = 256
FAST = 64
VMEM = 66 * 1024 * 1024

f32 = jnp.float32
low = jnp.bfloat16

NN = (((1,), (0,)), ((), ()))
NT = (((1,), (1,)), ((), ()))
TN = (((0,), (0,)), ((), ()))


def dot(a, b, dims):
    return lax.dot_general(a, b, dims, preferred_element_type=f32)


def round_up(n, m):
    return (n + m - 1) // m * m


def rotary_base():
    d = np.arange(LANES) % HD
    half = ROT // 2
    inverse = np.where(d < ROT, np.exp((d % half) * (-2.0 * math.log(10000.0) / ROT)), 0.0)
    slow = np.arange(0, LMAX, FAST)[:, None] * inverse
    fast = np.arange(FAST)[:, None] * inverse
    return np.concatenate([np.cos(slow), np.sin(slow), np.cos(fast), np.sin(fast)]).astype(
        np.float32
    )


def rotary_turned():
    half = ROT // 2
    inverse = np.exp(np.arange(half) * (-2.0 * math.log(10000.0) / ROT))
    angles = inverse[:, None] * np.arange(LMAX)
    return np.concatenate([np.cos(angles), np.sin(angles)]).astype(np.float32)


def rotary_rows(table_ref, block):
    slow_rows = LMAX // FAST
    fast_cos = table_ref[2 * slow_rows : 2 * slow_rows + FAST, :]
    fast_sin = table_ref[2 * slow_rows + FAST :, :]
    cosines, sines = [], []
    for part in range(BLOCK // FAST):
        row = block * (BLOCK // FAST) + part
        slow_cos = table_ref[pl.ds(row, 1), :]
        slow_sin = table_ref[pl.ds(row + slow_rows, 1), :]
        cosines.append(slow_cos * fast_cos - slow_sin * fast_sin)
        sines.append(slow_sin * fast_cos + slow_cos * fast_sin)
    cosine, sine = jnp.concatenate(cosines), jnp.concatenate(sines)
    d = lax.broadcasted_iota(jnp.int32, cosine.shape, 1) % HD
    return (
        cosine,
        jnp.where(d < ROT // 2, -sine, 0.0),
        jnp.where((d >= ROT // 2) & (d < ROT), sine, 0.0),
    )


def rotate(values, tables, sign):
    cosine, from_right, from_left = tables
    half = ROT // 2
    turned = []
    for first in range(0, values.shape[1], LANES):
        t = values[:, first : first + LANES]
        side = (
            pltpu.roll(t, LANES - half, axis=1) * from_right
            + pltpu.roll(t, half, axis=1) * from_left
        )
        turned.append(t * cosine + side if sign > 0 else t * cosine - side)
    return jnp.concatenate(turned, axis=1)


def three_terms(value):
    first = value.astype(low).astype(f32)
    second = (value - first).astype(low).astype(f32)
    return first, second, value - first - second


MESH = pl.DeviceIdType.MESH


class Place:
    def __init__(self):
        self.dp, self.t = lax.axis_index("dp"), lax.axis_index("tensor")
        self.n, self.ways = lax.axis_size("dp"), lax.axis_size("tensor")
        self.majors = self.n // 2
        self.a, self.b = self.dp // 2, self.dp % 2
        self.chip, self.core = self.t // 2, self.t % 2
        self.upper = self.a * 2 // self.majors
        self.near = (self.dp, self.t + 1 - 2 * self.core)
        self.across = (self.dp, (self.t + 2) % 4)
        self.beside = (self.dp + 1 - 2 * self.b, self.t)

    def major(self, k):
        return ((self.a + k) % self.majors, (self.a + k) % self.majors * 2 + self.b)

    def shard(self, kind):
        return (self.chip + kind // 2) % 2 * 2 + (self.core + kind % 2) % 2

    def greet(self):
        barrier = pltpu.get_barrier_semaphore()
        others = [self.near, self.across, (self.dp, 3 - self.t)]
        others += [((self.dp + k) % self.n, self.t) for k in range(1, self.n)]
        for other in others:
            pl.semaphore_signal(barrier, inc=1, device_id=other, device_id_type=MESH)
        pl.semaphore_wait(barrier, len(others))


def send(src, dst, sems, k, to):
    return pltpu.make_async_remote_copy(
        src_ref=src,
        dst_ref=dst,
        send_sem=sems.at[0, k],
        recv_sem=sems.at[1, k],
        device_id=to,
        device_id_type=MESH,
    )


def plus(*terms):
    return functools.reduce(jnp.add, [t.astype(f32) for t in terms])


class Scatter:
    def __init__(self, place, mine, got, last, sems):
        self.p, self.mine, self.got, self.last, self.pairs, self.lines = place, mine, got, last, *sems

    def first(self, k):
        p = self.p
        mine = self.mine.at[p.major(k)[0] * 2 + 1 - p.b]
        return send(mine, self.got.at[k], self.pairs, k, p.beside)

    def second(self, k):
        to = (self.p.major(k)[1], self.p.t)
        return send(self.got.at[k], self.last.at[k - 1], self.lines, k - 1, to)

    def order(self, number):
        p = self.p
        half = p.majors // 2
        if number <= half:
            a = (1 - p.upper) * half + number - 1
        else:
            a = p.upper * half + (p.a % half + number - half) % half
        return (a - p.a + p.majors) % p.majors

    def start_half(self, turn):
        half = self.p.majors // 2
        for number in range(turn * half + 1, (turn + 1) * half + 1):
            self.first(self.order(number)).start()

    def add(self, number):
        k = self.order(number)
        self.first(k).wait_recv()
        self.got[k] = plus(self.mine[self.p.major(k)[1]], self.got[k]).astype(self.got.dtype)

    def forward(self, number):
        self.second(self.order(number)).start()

    def finish(self):
        p = self.p
        for k in range(p.majors):
            self.first(k).wait_send()
        self.first(0).wait_recv()
        for k in range(1, p.majors):
            self.second(k).wait()
        return plus(self.mine[p.dp], self.got[0], *[self.last[k] for k in range(p.majors - 1)])


class Gather:
    def __init__(self, place, mine, whole, sems):
        self.p, self.mine, self.whole, self.lines, self.pairs = place, mine, whole, *sems

    def line(self, way, hop):
        p = self.p
        step = 1 - 2 * way
        origin = (p.a - step * hop) * 2 + p.b
        mine = self.mine if hop == 0 else self.whole.at[origin]
        to = ((p.a + step) * 2 + p.b, p.t)
        return send(mine, self.whole.at[origin], self.lines, way * (p.majors - 1) + hop, to)

    def pair(self, way, hop):
        p = self.p
        origin = (p.a - (1 - 2 * way) * hop) * 2 + p.b
        mine = self.mine if hop == 0 else self.whole.at[origin]
        return send(mine, self.whole.at[origin], self.pairs, way * p.majors + hop, p.beside)

    def came(self, way, hop):
        p = self.p
        return p.a >= hop if way == 0 else p.a <= p.majors - 1 - hop

    def goes(self, way, hop):
        p = self.p
        return self.came(way, hop) & (p.a < p.majors - 1 if way == 0 else p.a > 0)

    def start(self):
        for way in range(2):

            @pl.when(self.goes(way, 0))
            def _():
                self.line(way, 0).start()

        self.pair(0, 0).start()

    def forward(self, hop):
        for way in range(2):

            @pl.when(self.came(way, hop))
            def _():
                self.arrival(way, hop).wait_recv()
                if hop < self.p.majors - 1:

                    @pl.when(self.goes(way, hop))
                    def _():
                        self.line(way, hop).start()

                self.pair(way, hop).start()

    def arrival(self, way, hop):
        p = self.p
        step = 1 - 2 * way
        block = self.whole.at[(p.a - step * hop) * 2 + p.b]
        back = ((p.a - step) * 2 + p.b, p.t)
        return send(block, block, self.lines, way * (p.majors - 1) + hop - 1, back)

    def arrived(self):
        p = self.p
        for way in range(2):
            for hop in range(way, p.majors):

                @pl.when(self.came(way, hop))
                def _():
                    other = self.whole.at[(p.a - (1 - 2 * way) * hop) * 2 + 1 - p.b]
                    send(other, other, self.pairs, way * p.majors + hop, p.beside).wait_recv()

    def finish(self):
        for way in range(2):
            for hop in range(self.p.majors):
                if hop < self.p.majors - 1:

                    @pl.when(self.goes(way, hop))
                    def _():
                        self.line(way, hop).wait_send()

                if way == 0 or hop > 0:

                    @pl.when(self.came(way, hop))
                    def _():
                        self.pair(way, hop).wait_send()


def gather_scratch(majors):
    return [
        pltpu.SemaphoreType.DMA((2, 2 * (majors - 1))),
        pltpu.SemaphoreType.DMA((2, 2 * majors)),
    ]


class Rows:
    def __init__(self, place, mine, whole, sems):
        self.p, self.mine, self.whole, self.sems = place, mine, whole, sems
        self.per = mine.shape[0] // BLOCK

    def copy(self, kind, c):
        p = self.p
        if kind == 2:
            block = self.whole.at[p.across[1] * self.per + c]
            return send(block, block, self.sems, 2 * self.per + c, p.near)
        to = p.near if kind == 0 else p.across
        mine = self.mine.at[pl.ds(c * BLOCK, BLOCK)]
        return send(mine, self.whole.at[p.t * self.per + c], self.sems, kind * self.per + c, to)

    def start(self):
        for c in range(self.per):
            for kind in range(2):
                self.copy(kind, c).start()

    def arrived(self, kind, c):
        self.copy(kind, c).wait_recv()

    def forward(self, c):
        self.copy(1, c).wait_recv()
        self.copy(2, c).start()

    def released(self):
        for c in range(self.per):
            self.copy(2, c).wait_send()

    def finish(self):
        for c in range(self.per):
            for kind in range(2):
                self.copy(kind, c).wait_send()


class Exchange:
    def __init__(self, slots, sems, me, count, device):
        self.slots, self.sems, self.me, self.count, self.device = slots, sems, me, count, device

    def copy(self, k, source):
        return pltpu.make_async_remote_copy(
            src_ref=self.slots.at[source],
            dst_ref=self.slots.at[source],
            send_sem=self.sems.at[0, k],
            recv_sem=self.sems.at[1, source],
            device_id=self.device((self.me + k) % self.count),
            device_id_type=MESH,
        )

    def start(self):
        for k in range(1, self.count):
            self.copy(k, self.me).start()

    def total(self):
        for k in range(1, self.count):
            self.copy(k, (self.me + k) % self.count).wait_recv()
        return functools.reduce(jnp.add, [self.slots[k] for k in range(self.count)])

    def finish(self):
        for k in range(1, self.count):
            self.copy(k, self.me).wait_send()


def scatter_scratch(majors, rows, columns):
    return [
        pltpu.VMEM((majors, rows, columns), low),
        pltpu.VMEM((majors - 1, rows, columns), low),
        pltpu.SemaphoreType.DMA((2, majors)),
        pltpu.SemaphoreType.DMA((2, majors - 1)),
    ]


def flat(blocks_ref):
    n, side, columns = blocks_ref.shape
    if side % 16 == 0:
        return blocks_ref[...].reshape(n * side, columns)
    return jnp.concatenate([blocks_ref[k].astype(f32) for k in range(n)]).astype(low)


def norm_rows(x):
    shifted = x - jnp.mean(x, axis=1, keepdims=True)
    inv_std = lax.rsqrt(jnp.mean(shifted * shifted, axis=1, keepdims=True) + EPS)
    return shifted * inv_std, inv_std


def layer_kernel(
    length_ref, tokens_ref, cot_ref, g1_ref, b1_ref, g2_ref, b2_ref, wq_ref, bq_ref, wo_ref, wi_ref,
    bi_ref, wd_ref, bo_ref, bd_ref, table_ref, turned_ref,
    out_out, gx_out, spill_out, gq_ref, gbq_ref, go_ref, gi_ref, gb_ref, gd_ref, small_ref,
    norm_ref, bias_ref, wq_mine, wd_mine, wq_all, wi_all, wd_all,
    x_all, first_ref, second_ref, cot_all, qkv_ref, qx_ref, dox_ref, context_ref, pool_ref,
    keyt_ref, queryt_ref, valuet_ref, mixed_ref, top_ref, gwq_sum, stage_ref, gb_sum, gs_sum, gw_ref, own_sems, out_sems, x_sems, cot_sems,
    wq_lines, wq_pairs, wi_lines, wi_pairs, wd_lines, wd_pairs,
    gn_near, gn_far, gn_sem1, gn_sem2,
    br_near, br_far, br_sem1, br_sem2,
    w_got, w_last, w_sem1, w_sem2,
    gq_low, q_got, q_last, q_sem1, q_sem2,
    line_ref, cross_ref, line_sem, cross_sem,
):
    here = Place()
    blocks, _, d = x_all.shape
    local = tokens_ref.shape[0]
    per = local // BLOCK
    width = wq_ref.shape[2]
    heads = width // HD
    padded = qkv_ref.shape[2] // 3
    hidden = wi_ref.shape[1]
    side = wi_ref.shape[0]
    scale = HD ** (-0.5)
    to_power = scale * math.log2(math.e)
    tall = valuet_ref.shape[1] // heads
    lane = lax.broadcasted_iota(jnp.int32, (BLOCK, padded), 1)
    of_head = [(lane >= h * HD) & (lane < (h + 1) * HD) for h in range(heads)]
    extra = (lane >= width) & (lane < width + 3)

    rows = Rows(here, tokens_ref, x_all, x_sems)
    cots = Rows(here, cot_ref, cot_all, cot_sems)
    proj_w = Gather(here, wq_mine, wq_all, (wq_lines, wq_pairs))
    in_w = Gather(here, wi_ref, wi_all, (wi_lines, wi_pairs))
    down_w = Gather(here, wd_mine, wd_all, (wd_lines, wd_pairs))

    wq_mine[...] = jnp.zeros_like(wq_mine)
    wd_mine[:, hidden:] = jnp.zeros((side, padded), low)
    bias_ref[...] = jnp.zeros_like(bias_ref)
    for k in range(3):
        wq_mine[:, k * padded : k * padded + width] = wq_ref[k]
        bias_ref[0:1, k * padded : k * padded + width] = bq_ref[k : k + 1, :]
    wd_mine[:, :hidden] = wd_ref[...]
    wd_mine[:, hidden : hidden + width] = wo_ref[...].astype(f32).T.astype(low)
    for k, ref in enumerate((g1_ref, b1_ref, g2_ref, b2_ref, bo_ref, bd_ref, bi_ref)):
        norm_ref[k, :] = ref[...]

    here.greet()
    proj_w.start()
    rows.start()
    own = [
        pltpu.make_async_copy(tokens_ref.at[pl.ds(c * BLOCK, BLOCK)], x_all.at[here.t * per + c], own_sems.at[c])
        for c in range(per)
    ]
    own += [
        pltpu.make_async_copy(cot_ref.at[pl.ds(c * BLOCK, BLOCK)], cot_all.at[here.t * per + c], own_sems.at[per + c])
        for c in range(per)
    ]
    own += [
        pltpu.make_async_copy(mine, whole.at[here.dp], own_sems.at[2 * per + k])
        for k, (mine, whole) in enumerate(((wq_mine, wq_all), (wi_ref, wi_all), (wd_mine, wd_all)))
    ]
    for copy in own:
        copy.start()

    def norm(kind, c):
        r = here.shard(kind) * per + c
        normed, _ = norm_rows(x_all[r].astype(f32))
        first_ref[r] = (normed * norm_ref[0:1, :] + norm_ref[1:2, :]).astype(low)
        second_ref[r] = (normed * norm_ref[2:3, :] + norm_ref[3:4, :]).astype(low)

    def project(kind, c):
        r = here.shard(kind) * per + c
        projected = dot(first_ref[r], flat(wq_all), NN) + bias_ref[...]
        tables = rotary_rows(table_ref, r)
        queries = rotate(projected[:, :padded], tables, 1)
        queryt_ref[r] = queries.T[:width].astype(low)
        qkv_ref[r, :, :padded] = queries.astype(low)
        keys = rotate(projected[:, padded : 2 * padded], tables, 1)
        keyt_ref[r] = keys.T[:width].astype(low)
        qkv_ref[r, :, padded : 2 * padded] = jnp.where(extra, 1.0, keys).astype(low)
        values = projected[:, 2 * padded :]
        qkv_ref[r, :, 2 * padded :] = jnp.where(extra, 1.0, values).astype(low)
        turned = values.T.astype(low)
        for h in range(heads):
            valuet_ref[r, h * tall : h * tall + HD, :] = turned[h * HD : (h + 1) * HD]
            valuet_ref[r, h * tall + HD : (h + 1) * tall, :] = jnp.ones((tall - HD, BLOCK), low)

    for c in range(per):
        own[c].wait()

    @pl.loop(0, per)
    def _(c):
        norm(0, c)

    for c in range(per):
        rows.arrived(0, c)
    proj_w.forward(1)

    @pl.loop(0, per)
    def _(c):
        norm(1, c)

    for k in range(2, here.majors - 1):
        proj_w.forward(k)
    for c in range(per - 1):
        rows.forward(c)
    proj_w.forward(here.majors - 1)
    in_w.start()
    cots.start()
    for c in range(per - 1):
        norm(2, c)
    for c in range(per - 1):
        rows.arrived(2, c)
        norm(3, c)
    own[2 * per].wait()
    proj_w.arrived()

    @pl.loop(0, per + 2 * (per - 1))
    def _(number):
        @pl.when(number == per + 1)
        def _():
            rows.forward(per - 1)

        @pl.when(number == per - 1)
        def _():
            in_w.forward(1)

        later = number // per
        project(1 + later + number % per * later, number % per * (1 - later))

    @pl.loop(0, per)
    def _(c):
        project(0, c)

    for k in range(2, here.majors - 1):
        in_w.forward(k)
    norm(2, per - 1)
    project(2, per - 1)
    rows.arrived(2, per - 1)
    norm(3, per - 1)
    project(3, per - 1)

    def spilled():
        return pltpu.make_async_copy(first_ref, spill_out, out_sems.at[1 + per])

    def restored():
        return pltpu.make_async_copy(spill_out, first_ref, out_sems.at[1 + per])

    spilled().start()

    def in_fours(count, body):
        @pl.loop(0, count // 4)
        def _(number):
            for k in range(4):
                body(4 * number + k)

        for size in (2, 1):

            @pl.when(count // size % 2 == 1)
            def _():
                for k in range(size):
                    body(count // (2 * size) * (2 * size) + k)

    in_w.forward(here.majors - 1)
    down_w.start()

    @pl.loop(0, blocks)
    def _(i):
        for k in range(1, here.majors):

            @pl.when(i == min(2 * k, blocks - 1))
            def _():
                down_w.forward(k)

        for c in range(per):

            @pl.when(i == blocks - per + c)
            def _():
                cots.forward(c)

        q = qkv_ref[i, :, :padded].astype(f32)
        for h in range(heads):
            qx_ref[i, h * BLOCK : (h + 1) * BLOCK, :] = jnp.where(of_head[h], q, 0.0).astype(low)
        query = qx_ref[i]
        parts = [slice(h * BLOCK, (h + 1) * BLOCK) for h in range(heads)]

        def scores(j):
            return dot(qkv_ref[j, :, padded : 2 * padded], query, NT)

        def highest(s):
            return jnp.max(s.reshape(-1, 8, heads * BLOCK), axis=0)

        def keep(j, s):
            for h in range(heads):
                pool_ref[j * heads + h] = s[:, parts[h]]

        diagonal = scores(i)
        key_at = lax.broadcasted_iota(jnp.int32, diagonal.shape, 0)
        query_at = lax.broadcasted_iota(jnp.int32, diagonal.shape, 1) % BLOCK
        diagonal = jnp.where(key_at <= query_at, diagonal, -1e30)
        keep(i, diagonal)
        top_ref[...] = highest(diagonal)

        def first_pass(j):
            s = scores(j)
            keep(j, s)
            top_ref[...] = jnp.maximum(top_ref[...], highest(s))

        in_fours(i, first_pass)
        top = jnp.max(top_ref[...], axis=0, keepdims=True)
        mixed_ref[...] = jnp.zeros_like(mixed_ref)

        def second_pass(j):
            for h in range(heads):
                p = jnp.exp2((pool_ref[j * heads + h] - top[:, parts[h]]) * to_power).astype(low)
                at = slice(h * tall, (h + 1) * tall)
                mixed_ref[at, :] += dot(valuet_ref[j, at, :], p, NN)

        in_fours(i + 1, second_pass)
        mixed, terms = [], []
        for h in range(heads):
            total = mixed_ref[h * tall + HD : h * tall + HD + 1, :]
            mixed.append(mixed_ref[h * tall : h * tall + HD, :] * (1.0 / total))
            terms.append(jnp.concatenate(three_terms(-top[:, parts[h]] - jnp.log(total) / scale)))
        terms = jnp.concatenate(terms, axis=1)
        side_rows = width - (padded - LANES)
        columns = jnp.concatenate(
            [
                jnp.zeros((side_rows, heads * BLOCK), f32),
                terms,
                jnp.zeros((LANES - side_rows - 3, heads * BLOCK), f32),
            ]
        ).T
        for h in range(heads):
            right = jnp.where(of_head[h], q, 0.0)[:, padded - LANES :]
            qx_ref[i, parts[h], padded - LANES :] = (right + columns[parts[h]]).astype(low)
        mixed.append(jnp.zeros((padded - width, BLOCK), f32))
        context_ref[i] = jnp.concatenate(mixed).T.astype(low)

    grad_ref, act_ref, hidden_ref, gradt_ref = cot_all, x_all, first_ref, valuet_ref
    own[2 * per + 1].wait()
    in_w.arrived()
    rows.released()

    @pl.loop(0, blocks)
    def _(r):
        u = dot(second_ref[r], flat(wi_all), NN) + norm_ref[6:7, :]
        cdf = 0.5 * (1.0 + lax.erf(u * (1.0 / math.sqrt(2.0))))
        act_ref[r] = (u * cdf).astype(low)
        slope = cdf + u * (jnp.exp(-0.5 * u * u) * (1.0 / math.sqrt(2.0 * math.pi)))
        for k in range(3):
            pool_ref[3 * r + k] = slope[:, k * BLOCK : (k + 1) * BLOCK]

    for c in range(per):
        cots.arrived(0, c)
        cots.arrived(2, c)
    for copy in own[per : 2 * per] + own[2 * per + 2 :]:
        copy.wait()
    gb_sum[...] = jnp.zeros_like(gb_sum)
    gs_sum[...] = jnp.zeros_like(gs_sum)
    cots.released()
    spilled().wait()
    down_w.arrived()

    @pl.loop(0, blocks)
    def _(r):
        row = lax.broadcasted_iota(jnp.int32, (BLOCK, d), 0) + r * BLOCK
        grad = jnp.where(row < length_ref[0], cot_all[r].astype(f32), 0.0).astype(low)
        grad_ref[r] = grad
        back = dot(grad, flat(wd_all), NN)
        slope = jnp.concatenate([pool_ref[3 * r + k] for k in range(3)], axis=1)
        grad_hidden = back[:, :hidden] * slope
        gb_sum[1:2, :] += jnp.sum(grad_hidden, axis=0, keepdims=True)
        hidden_ref[r] = grad_hidden.astype(low)

        grad_context = back[:, hidden:].astype(low).astype(f32)
        gradt_ref[r, :width, :] = grad_context.T[:width].astype(low)
        product = grad_context * context_ref[r].astype(f32)
        for h in range(heads):
            extended = jnp.where(of_head[h], grad_context, 0.0)
            delta = jnp.sum(jnp.where(of_head[h], product, 0.0), axis=1, keepdims=True)
            for k, term in enumerate(three_terms(-delta)):
                extended = jnp.where(lane == width + k, term, extended)
            dox_ref[r, h * BLOCK : (h + 1) * BLOCK, :] = extended.astype(low)

    weights = Scatter(here, gw_ref, w_got, w_last, (w_sem1, w_sem2))
    final = Scatter(here, gq_low, q_got, q_last, (q_sem1, q_sem2))
    half = d // 2
    rows_total = blocks * BLOCK

    @pl.loop(0, 2)
    def _(turn):
        which = (1 - turn) * (1 - here.upper) + turn * here.upper
        at = pl.ds(pl.multiple_of(which * half, LANES), half)
        all_rows = lambda ref: ref[...].reshape(rows_total, ref.shape[2])
        mine = second_ref[:, :, at].reshape(rows_total, half)
        first_block = which * (here.n // 2)
        side_blocks = pl.ds(first_block, here.n // 2)
        gwi = dot(mine, all_rows(hidden_ref), TN).reshape(here.n // 2, side, hidden)
        gw_ref[side_blocks, :, :hidden] = gwi.astype(low)
        @pl.when(turn == 1)
        def _():
            weights.start_half(0)

        mine = grad_ref[:, :, at].reshape(rows_total, half)
        gwd = dot(mine, all_rows(act_ref), TN).reshape(here.n // 2, side, hidden)
        gw_ref[side_blocks, :, hidden : 2 * hidden] = gwd.astype(low)
        gwd = dot(mine, all_rows(context_ref), TN).reshape(here.n // 2, side, padded)
        gw_ref[side_blocks, :, 2 * hidden :] = gwd.astype(low)

    branch_ref, part_ref = cot_all, second_ref

    def near_branch(chip):
        owner = chip * 2 + 1 - here.core
        return send(
            branch_ref.at[pl.ds(owner * per, per)], br_near.at[chip], br_sem1, chip, here.near
        )

    def far_branch():
        return send(br_near.at[1 - here.chip], br_far, br_sem2, 0, here.across)

    @pl.loop(0, blocks)
    def _(number):
        r = here.shard(3 - number // per) * per + number % per

        @pl.when(number == per + 1)
        def _():
            near_branch(1 - here.chip).start()

        @pl.when(number == 2 * per + 1)
        def _():
            near_branch(1 - here.chip).wait_recv()

            @pl.loop(0, per)
            def _(c):
                mine = branch_ref[here.across[1] * per + c]
                br_near[1 - here.chip, c] = plus(mine, br_near[1 - here.chip, c]).astype(low)

        @pl.when(number == 3 * per + 1)
        def _():
            near_branch(here.chip).start()

        second = second_ref[r].astype(f32)
        part = dot(hidden_ref[r], flat(wi_all), NT)
        both = jnp.concatenate([act_ref[r], context_ref[r]], axis=1)
        branch_ref[r] = dot(both, flat(wd_all), NT).astype(low)
        gs_sum[2:3, :] += jnp.sum(part * second, axis=0, keepdims=True)
        gs_sum[3:4, :] += jnp.sum(part, axis=0, keepdims=True)
        part_ref[r] = (part * norm_ref[2:3, :]).astype(low)

        @pl.when(number == 0)
        def _():
            weights.start_half(1)

        @pl.when(number == 2 * per + 1)
        def _():
            far_branch().start()

    restored().start()
    gn_ref = x_all
    gwq_sum[...] = jnp.zeros_like(gwq_sum)
    pool_ref[...] = jnp.zeros_like(pool_ref)

    last = blocks - 1
    half_rot = ROT // 2

    def block_of(number):
        return number // 2 + number % 2 * (last - number // 2 * 2)

    def slot_of(r):
        return r // per // 2 * per + r % per

    def near_block(r):
        return send(gn_ref.at[r], gn_near.at[slot_of(r)], gn_sem1, slot_of(r), here.near)

    def far_block(c):
        mine = gn_near.at[(1 - here.chip) * per + c]
        return send(mine, gn_far.at[c], gn_sem2, c, here.across)

    def hand_over(r):
        @pl.when(r // per % 2 != here.core)
        def _():
            near_block(r).start()

    def collect(r):
        owner = r // per

        @pl.when(owner % 2 == here.core)
        def _():
            near_block(r).wait_recv()

        @pl.when((owner % 2 == here.core) & (owner // 2 != here.chip))
        def _():
            gn_near[slot_of(r)] = plus(gn_ref[r], gn_near[slot_of(r)]).astype(low)

    def pass_on(r):
        owner = r // per

        @pl.when((owner % 2 == here.core) & (owner // 2 != here.chip))
        def _():
            far_block(r % per).start()

    def pair(i, j, own):
        keys, values = qkv_ref[j, :, padded : 2 * padded], qkv_ref[j, :, 2 * padded :]
        query, dout = qx_ref[i], dox_ref[i]
        p = jnp.exp2(dot(query, keys, NT) * to_power)
        if own:
            query_at = lax.broadcasted_iota(jnp.int32, p.shape, 0) % BLOCK
            key_at = lax.broadcasted_iota(jnp.int32, p.shape, 1)
            p = jnp.where(key_at <= query_at, p, 0.0)
        ds = (p * dot(dout, values, NT)).astype(low)
        p = p.astype(low)
        for h in range(heads):
            at, part = slice(h * HD, (h + 1) * HD), slice(h * BLOCK, (h + 1) * BLOCK)
            pool_ref[blocks + j, at, :] += dot(gradt_ref[i, at, :], p[part], NN)
            pool_ref[j, at, :] += dot(queryt_ref[i, at, :], ds[part], NN)
            pool_ref[2 * blocks + i, at, :] += dot(keyt_ref[j, at, :], ds[part], NT)

    def kept(c, values):
        row = lax.broadcasted_iota(jnp.int32, (BLOCK, d), 0) + (here.t * per + c) * BLOCK
        return jnp.where(row < length_ref[0], values, 0.0)

    for c in range(per):
        cot = kept(c, cot_ref[c * BLOCK : (c + 1) * BLOCK, :].astype(f32))
        gs_sum[4:5, :] += jnp.sum(cot, axis=0, keepdims=True)

    def output_copy():
        return pltpu.make_async_copy(stage_ref.at[:], out_out, out_sems.at[0])

    @pl.loop(0, blocks)
    def _(step):
        for k in range(1, here.majors):

            @pl.when(step == min(k - 1, last - 2))
            def _():
                weights.add(k)

        @pl.when(step > 0)
        def _():
            hand_over(block_of(step - 1))

        turn = step // 2
        odd = step % 2
        now = block_of(step)
        pair(now, now, True)

        for k in range(1, here.majors):

            @pl.when(step == min(k - 1, last - 2))
            def _():
                weights.forward(k)

        @pl.when(step > 0)
        def _():
            collect(block_of(step - 1))

        def next_pair(number):
            other = turn + 1 + number
            pair(other + odd * (last - turn - other), turn + odd * (other - turn), False)

        in_fours(last - step, next_pair)

        @pl.when(step == last // 2)
        def _():
            far_branch().wait()
            for chip in range(2):
                near_branch(chip).wait_send()
            near_branch(here.chip).wait_recv()

            @pl.loop(0, per)
            def _(c):
                total = plus(branch_ref[here.t * per + c], br_near[here.chip, c], br_far[c])
                total += norm_ref[4:5, :] + norm_ref[5:6, :]
                at = pl.ds(pl.multiple_of(c * BLOCK, BLOCK), BLOCK)
                stage_ref[at, :] = tokens_ref[at, :].astype(f32) + kept(c, total)

        positions = pl.ds(pl.multiple_of(now * BLOCK, BLOCK), BLOCK)
        cosine, sine = turned_ref[:half_rot, positions], turned_ref[half_rot:, positions]
        for slab in (now, 2 * blocks + now):
            for h in range(heads):
                near_rows = slice(h * HD, h * HD + half_rot)
                far_rows = slice(h * HD + half_rot, h * HD + 2 * half_rot)
                near_part, far_part = pool_ref[slab, near_rows, :], pool_ref[slab, far_rows, :]
                pool_ref[slab, near_rows, :] = near_part * cosine + far_part * sine
                pool_ref[slab, far_rows, :] = far_part * cosine - near_part * sine
        filler = jnp.zeros((BLOCK, padded - width), f32)
        turned = [
            jnp.concatenate([pool_ref[k * blocks + now, :width, :].T, filler], axis=1)
            for k in range(3)
        ]
        projected = jnp.concatenate([turned[2] * scale, turned[0] * scale, turned[1]], axis=1)
        gb_sum[0:1, :] += jnp.sum(projected, axis=0, keepdims=True)
        proj_low = projected.astype(low)
        @pl.when(step == 0)
        def _():
            restored().wait()

        first = first_ref[now]
        gwq_sum[...] += dot(first, proj_low, TN)
        part = dot(proj_low, flat(wq_all), NT)
        gs_sum[0:1, :] += jnp.sum(part * first.astype(f32), axis=0, keepdims=True)
        gs_sum[1:2, :] += jnp.sum(part, axis=0, keepdims=True)
        gn_ref[now] = (part * norm_ref[0:1, :] + part_ref[now].astype(f32)).astype(low)

        @pl.when(step > 0)
        def _():
            pass_on(block_of(step - 1))

        @pl.when(step == last // 2)
        def _():
            output_copy().start()

    now = block_of(last)
    for block in range(here.n):
        rows_of = slice(block * side, (block + 1) * side)
        gq_low[block] = jnp.concatenate(
            [gwq_sum[rows_of, k * padded : k * padded + width] for k in range(3)], axis=1
        ).astype(low)
    hand_over(now)
    final.start_half(0)
    final.start_half(1)
    line_ref[here.dp] = jnp.concatenate(
        [gb_sum[0:2, :], gs_sum[0:5, :], jnp.zeros((1, d), f32)]
    )
    line = Exchange(line_ref, line_sem, here.dp, here.n, lambda to: (to, here.t))
    cross = Exchange(cross_ref, cross_sem, here.t, here.ways, lambda to: (here.dp, to))
    collect(now)
    pass_on(now)
    line.start()
    for k in range(1, here.majors):
        final.add(k)
        if k == 1:
            total = weights.finish()
            gi_ref[...] = total[:, :hidden]
            gd_ref[...] = total[:, hidden : 2 * hidden]
            go_ref[...] = total[:, 2 * hidden : 2 * hidden + width].T
        final.forward(k)
    summed = line.total()
    for k in range(3):
        gbq_ref[k : k + 1, :] = summed[0:1, k * padded : k * padded + width]
    gb_ref[...] = summed[1, :]
    cross_ref[here.t] = summed
    cross.start()

    def grad_copy(c):
        at = pl.ds(c * BLOCK, BLOCK)
        return pltpu.make_async_copy(stage_ref.at[at], gx_out.at[at], out_sems.at[1 + c])

    for c in range(per):
        far_block(c).wait()
    output_copy().wait()
    for c in range(per):
        at = slice(c * BLOCK, (c + 1) * BLOCK)
        normed, inv_std = norm_rows(tokens_ref[at, :].astype(f32))
        grad_normed = plus(gn_ref[here.t * per + c], gn_near[here.chip * per + c], gn_far[c])
        stage_ref[at, :] = cot_ref[at, :].astype(f32) + inv_std * (
            grad_normed
            - jnp.mean(grad_normed, axis=1, keepdims=True)
            - normed * jnp.mean(grad_normed * normed, axis=1, keepdims=True)
        )
        grad_copy(c).start()
    summed = cross.total()
    for k in range(2):
        product, plain = summed[2 + 2 * k : 3 + 2 * k, :], summed[3 + 2 * k : 4 + 2 * k, :]
        gain, bias = norm_ref[2 * k : 2 * k + 1, :], norm_ref[2 * k + 1 : 2 * k + 2, :]
        small_ref[2 * k : 2 * k + 1, :] = (product - bias * plain) / gain
        small_ref[2 * k + 1 : 2 * k + 2, :] = plain
    small_ref[4:5, :] = summed[6:7, :]
    for slot in range(2 * per):
        near_block(slot // per * 2 * per + (1 - here.core) * per + slot % per).wait_send()
    for one in (rows, cots, proj_w, in_w, down_w, line, cross):
        one.finish()
    for c in range(per):
        grad_copy(c).wait()
    total = final.finish()
    for k in range(3):
        gq_ref[k] = total[:, k * width : (k + 1) * width]


def layer(length, tokens, cot, norms, wq, bq, wo, wi, bi, wd, biases, table, turned):
    local, d = tokens.shape
    _, side, width = wq.shape
    hidden = wi.shape[1]
    heads = width // HD
    padded = round_up(width + 3, LANES)
    n, ways = lax.axis_size("dp"), lax.axis_size("tensor")
    majors = n // 2
    rows = local * ways
    blocks, per = rows // BLOCK, local // BLOCK
    assert rows == LMAX and length.shape[0] == 1
    assert ways == 4 and per == 2 and n % 4 == 0 and padded == BLOCK and heads == 3
    assert 3 * padded == d == hidden == side * n
    vmem = pl.BlockSpec(memory_space=pltpu.VMEM)
    hbm = pl.BlockSpec(memory_space=pl.ANY)
    row_blocks = pltpu.VMEM((blocks, BLOCK, d), low)
    head_blocks = pltpu.VMEM((blocks, heads * BLOCK, padded), low)
    columns = hidden + wd.shape[1] + padded
    outs = [
        jax.ShapeDtypeStruct((local, d), f32),
        jax.ShapeDtypeStruct((local, d), f32),
        jax.ShapeDtypeStruct((blocks, BLOCK, d), low),
        jax.ShapeDtypeStruct((3, side, width), f32),
        jax.ShapeDtypeStruct((3, width), f32),
        jax.ShapeDtypeStruct((width, side), f32),
        jax.ShapeDtypeStruct((side, hidden), f32),
        jax.ShapeDtypeStruct((hidden,), f32),
        jax.ShapeDtypeStruct((side, hidden), f32),
        jax.ShapeDtypeStruct((5, d), f32),
    ]
    args = (tokens, cot, *norms, wq, bq, wo, wi, bi, wd, *biases, table, turned)
    return pl.pallas_call(
        layer_kernel,
        name="layer",
        in_specs=[pl.BlockSpec(memory_space=pltpu.SMEM)] + [vmem] * len(args),
        out_specs=[hbm] * 3 + [vmem] * (len(outs) - 3),
        out_shape=outs,
        scratch_shapes=[
            pltpu.VMEM((8, d), f32),
            pltpu.VMEM((1, 3 * padded), f32),
            pltpu.VMEM((side, 3 * padded), low),
            pltpu.VMEM((side, hidden + padded), low),
            pltpu.VMEM((n, side, 3 * padded), low),
            pltpu.VMEM((n, side, hidden), low),
            pltpu.VMEM((n, side, hidden + padded), low),
            row_blocks, row_blocks, row_blocks, row_blocks,
            pltpu.VMEM((blocks, BLOCK, 3 * padded), low),
            head_blocks, head_blocks,
            pltpu.VMEM((blocks, BLOCK, padded), low),
            pltpu.VMEM((blocks * heads, BLOCK, BLOCK), f32),
            pltpu.VMEM((blocks, width, BLOCK), low),
            pltpu.VMEM((blocks, width, BLOCK), low),
            pltpu.VMEM((blocks, heads * (HD + 16), BLOCK), low),
            pltpu.VMEM((heads * (HD + 16), BLOCK), f32),
            pltpu.VMEM((8, heads * BLOCK), f32),
            pltpu.VMEM((d, hidden), f32),
            pltpu.VMEM((local, d), f32),
            pltpu.VMEM((8, d), f32),
            pltpu.VMEM((8, d), f32),
            pltpu.VMEM((n, side, columns), low),
            pltpu.SemaphoreType.DMA((2 * per + 3,)),
            pltpu.SemaphoreType.DMA((2 + per,)),
            pltpu.SemaphoreType.DMA((2, 3 * per)),
            pltpu.SemaphoreType.DMA((2, 3 * per)),
            *gather_scratch(majors), *gather_scratch(majors), *gather_scratch(majors),
            pltpu.VMEM((2 * per, BLOCK, d), low),
            pltpu.VMEM((per, BLOCK, d), low),
            pltpu.SemaphoreType.DMA((2, 2 * per)),
            pltpu.SemaphoreType.DMA((2, per)),
            pltpu.VMEM((2, per, BLOCK, d), low),
            pltpu.VMEM((per, BLOCK, d), low),
            pltpu.SemaphoreType.DMA((2, 2)),
            pltpu.SemaphoreType.DMA((2, 1)),
            *scatter_scratch(majors, side, columns),
            pltpu.VMEM((n, side, 3 * width), low),
            *scatter_scratch(majors, side, 3 * width),
            pltpu.VMEM((n, 8, d), f32),
            pltpu.VMEM((ways, 8, d), f32),
            pltpu.SemaphoreType.DMA((2, n)),
            pltpu.SemaphoreType.DMA((2, ways)),
        ],
        compiler_params=pltpu.CompilerParams(
            vmem_limit_bytes=VMEM, collective_id=0, has_side_effects=True
        ),
    )(length, *args)


def settle_kernel(*refs):
    count = len(refs) // 3
    sources, targets, held, sems = refs[:count], refs[count : 2 * count], refs[2 * count : -1], refs[-1]
    taken = [
        pltpu.make_async_copy(source, buffer, sems.at[0, k])
        for k, (source, buffer) in enumerate(zip(sources, held))
    ]
    put = [
        pltpu.make_async_copy(buffer, target, sems.at[1, k])
        for k, (buffer, target) in enumerate(zip(held, targets))
    ]
    for copy in taken:
        copy.start()
    for before, after in zip(taken, put):
        before.wait()
        after.start()
    for copy in put:
        copy.wait()


def settle(arrays):
    hbm = pl.BlockSpec(memory_space=pl.ANY)
    return pl.pallas_call(
        settle_kernel,
        name="settle",
        in_specs=[hbm] * len(arrays),
        out_specs=[hbm] * len(arrays),
        out_shape=[jax.ShapeDtypeStruct(a.shape, a.dtype) for a in arrays],
        scratch_shapes=[pltpu.VMEM(a.shape, a.dtype) for a in arrays]
        + [pltpu.SemaphoreType.DMA((2, len(arrays)))],
        compiler_params=pltpu.CompilerParams(vmem_limit_bytes=VMEM),
    )(*arrays)


def per_device(
    tokens, cotangent, seq_lengths, norm1_gain, norm1_bias, norm2_gain, norm2_bias,
    w_qkv, b_qkv, w_attn_out, w_in, b_in, w_down, b_out, b_down,
):
    output, grad_x, _, *rest = layer(
        seq_lengths, tokens, cotangent, (norm1_gain, norm1_bias, norm2_gain, norm2_bias),
        w_qkv.transpose(1, 0, 2), b_qkv, w_attn_out, w_in, b_in, w_down.T, (b_out, b_down),
        jnp.asarray(rotary_base()), jnp.asarray(rotary_turned()),
    )
    output, grad_x, g_qkv, gb_qkv, g_out, g_in, gb_in, g_down, small = settle(
        [output, grad_x, *rest]
    )
    return output, grad_x, g_qkv.transpose(1, 0, 2), gb_qkv, g_out, g_in, gb_in, g_down.T, small


def solution(mesh):
    rows = P(("dp", "tensor"), None)
    placed = (
        rows, rows, P("dp"), P(), P(), P(), P(), P("dp", None, "tensor"), P(None, "tensor"),
        P("tensor", "dp"), P("dp", "tensor"), P("tensor"), P("tensor", "dp"), P(), P(),
    )
    return jax.shard_map(
        per_device,
        mesh=mesh,
        in_specs=placed,
        out_specs=(
            rows, rows, P("dp", None, "tensor"), P(None, "tensor"), P("tensor", "dp"),
            P("dp", "tensor"), P("tensor"), P("tensor", "dp"), P(),
        ),
        check_vma=False,
    )
```

```python
import functools
import math

import jax
import jax.numpy as jnp
import numpy as np
from jax import lax
from jax.experimental import pallas as pl
from jax.experimental.pallas import tpu as pltpu
from jax.sharding import PartitionSpec as P

HD = 64
ROT = 16
LMAX = 2048
LANES = 128
EPS = 1e-05
BLOCK = 256
FAST = 64
VMEM = 66 * 1024 * 1024

f32 = jnp.float32
low = jnp.bfloat16

NN = (((1,), (0,)), ((), ()))
NT = (((1,), (1,)), ((), ()))
TN = (((0,), (0,)), ((), ()))


def dot(a, b, dims):
    return lax.dot_general(a, b, dims, preferred_element_type=f32)


def round_up(n, m):
    return (n + m - 1) // m * m


def rotary_base():
    d = np.arange(LANES) % HD
    half = ROT // 2
    inverse = np.where(d < ROT, np.exp((d % half) * (-2.0 * math.log(10000.0) / ROT)), 0.0)
    slow = np.arange(0, LMAX, FAST)[:, None] * inverse
    fast = np.arange(FAST)[:, None] * inverse
    return np.concatenate([np.cos(slow), np.sin(slow), np.cos(fast), np.sin(fast)]).astype(
        np.float32
    )


def rotary_turned():
    half = ROT // 2
    inverse = np.exp(np.arange(half) * (-2.0 * math.log(10000.0) / ROT))
    angles = inverse[:, None] * np.arange(LMAX)
    return np.concatenate([np.cos(angles), np.sin(angles)]).astype(np.float32)


def rotary_rows(table_ref, block):
    slow_rows = LMAX // FAST
    fast_cos = table_ref[2 * slow_rows : 2 * slow_rows + FAST, :]
    fast_sin = table_ref[2 * slow_rows + FAST :, :]
    cosines, sines = [], []
    for part in range(BLOCK // FAST):
        row = block * (BLOCK // FAST) + part
        slow_cos = table_ref[pl.ds(row, 1), :]
        slow_sin = table_ref[pl.ds(row + slow_rows, 1), :]
        cosines.append(slow_cos * fast_cos - slow_sin * fast_sin)
        sines.append(slow_sin * fast_cos + slow_cos * fast_sin)
    cosine, sine = jnp.concatenate(cosines), jnp.concatenate(sines)
    d = lax.broadcasted_iota(jnp.int32, cosine.shape, 1) % HD
    return (
        cosine,
        jnp.where(d < ROT // 2, -sine, 0.0),
        jnp.where((d >= ROT // 2) & (d < ROT), sine, 0.0),
    )


def rotate(values, tables, sign):
    cosine, from_right, from_left = tables
    half = ROT // 2
    turned = []
    for first in range(0, values.shape[1], LANES):
        t = values[:, first : first + LANES]
        side = (
            pltpu.roll(t, LANES - half, axis=1) * from_right
            + pltpu.roll(t, half, axis=1) * from_left
        )
        turned.append(t * cosine + side if sign > 0 else t * cosine - side)
    return jnp.concatenate(turned, axis=1)


def three_terms(value):
    first = value.astype(low).astype(f32)
    second = (value - first).astype(low).astype(f32)
    return first, second, value - first - second


MESH = pl.DeviceIdType.MESH


class Place:
    def __init__(self):
        self.dp, self.t = lax.axis_index("dp"), lax.axis_index("tensor")
        self.n, self.ways = lax.axis_size("dp"), lax.axis_size("tensor")
        self.majors = self.n // 2
        self.a, self.b = self.dp // 2, self.dp % 2
        self.chip, self.core = self.t // 2, self.t % 2
        self.upper = self.a * 2 // self.majors
        self.near = (self.dp, self.t + 1 - 2 * self.core)
        self.across = (self.dp, (self.t + 2) % 4)
        self.beside = (self.dp + 1 - 2 * self.b, self.t)

    def major(self, k):
        return ((self.a + k) % self.majors, (self.a + k) % self.majors * 2 + self.b)

    def shard(self, kind):
        return (self.chip + kind // 2) % 2 * 2 + (self.core + kind % 2) % 2

    def greet(self):
        barrier = pltpu.get_barrier_semaphore()
        others = [self.near, self.across, (self.dp, 3 - self.t)]
        others += [((self.dp + k) % self.n, self.t) for k in range(1, self.n)]
        for other in others:
            pl.semaphore_signal(barrier, inc=1, device_id=other, device_id_type=MESH)
        pl.semaphore_wait(barrier, len(others))


def send(src, dst, sems, k, to):
    return pltpu.make_async_remote_copy(
        src_ref=src,
        dst_ref=dst,
        send_sem=sems.at[0, k],
        recv_sem=sems.at[1, k],
        device_id=to,
        device_id_type=MESH,
    )


def plus(*terms):
    return functools.reduce(jnp.add, [t.astype(f32) for t in terms])


class Scatter:
    def __init__(self, place, mine, got, last, sems):
        self.p, self.mine, self.got, self.last, self.pairs, self.lines = place, mine, got, last, *sems

    def first(self, k):
        p = self.p
        mine = self.mine.at[p.major(k)[0] * 2 + 1 - p.b]
        return send(mine, self.got.at[k], self.pairs, k, p.beside)

    def second(self, k):
        to = (self.p.major(k)[1], self.p.t)
        return send(self.got.at[k], self.last.at[k - 1], self.lines, k - 1, to)

    def order(self, number):
        p = self.p
        half = p.majors // 2
        if number <= half:
            a = (1 - p.upper) * half + number - 1
        else:
            a = p.upper * half + (p.a % half + number - half) % half
        return (a - p.a + p.majors) % p.majors

    def start_half(self, turn):
        half = self.p.majors // 2
        for number in range(turn * half + 1, (turn + 1) * half + 1):
            self.first(self.order(number)).start()

    def add(self, number):
        k = self.order(number)
        self.first(k).wait_recv()
        self.got[k] = plus(self.mine[self.p.major(k)[1]], self.got[k]).astype(self.got.dtype)

    def forward(self, number):
        self.second(self.order(number)).start()

    def finish(self):
        p = self.p
        for k in range(p.majors):
            self.first(k).wait_send()
        self.first(0).wait_recv()
        for k in range(1, p.majors):
            self.second(k).wait()
        return plus(self.mine[p.dp], self.got[0], *[self.last[k] for k in range(p.majors - 1)])


class Gather:
    def __init__(self, place, mine, whole, sems):
        self.p, self.mine, self.whole, self.lines, self.pairs = place, mine, whole, *sems

    def line(self, way, hop):
        p = self.p
        step = 1 - 2 * way
        origin = (p.a - step * hop) * 2 + p.b
        mine = self.mine if hop == 0 else self.whole.at[origin]
        to = ((p.a + step) * 2 + p.b, p.t)
        return send(mine, self.whole.at[origin], self.lines, way * (p.majors - 1) + hop, to)

    def pair(self, way, hop):
        p = self.p
        origin = (p.a - (1 - 2 * way) * hop) * 2 + p.b
        mine = self.mine if hop == 0 else self.whole.at[origin]
        return send(mine, self.whole.at[origin], self.pairs, way * p.majors + hop, p.beside)

    def came(self, way, hop):
        p = self.p
        return p.a >= hop if way == 0 else p.a <= p.majors - 1 - hop

    def goes(self, way, hop):
        p = self.p
        return self.came(way, hop) & (p.a < p.majors - 1 if way == 0 else p.a > 0)

    def start(self):
        for way in range(2):

            @pl.when(self.goes(way, 0))
            def _():
                self.line(way, 0).start()

        self.pair(0, 0).start()

    def forward(self, hop):
        for way in range(2):

            @pl.when(self.came(way, hop))
            def _():
                self.arrival(way, hop).wait_recv()
                if hop < self.p.majors - 1:

                    @pl.when(self.goes(way, hop))
                    def _():
                        self.line(way, hop).start()

                self.pair(way, hop).start()

    def arrival(self, way, hop):
        p = self.p
        step = 1 - 2 * way
        block = self.whole.at[(p.a - step * hop) * 2 + p.b]
        back = ((p.a - step) * 2 + p.b, p.t)
        return send(block, block, self.lines, way * (p.majors - 1) + hop - 1, back)

    def arrived(self):
        p = self.p
        for way in range(2):
            for hop in range(way, p.majors):

                @pl.when(self.came(way, hop))
                def _():
                    other = self.whole.at[(p.a - (1 - 2 * way) * hop) * 2 + 1 - p.b]
                    send(other, other, self.pairs, way * p.majors + hop, p.beside).wait_recv()

    def finish(self):
        for way in range(2):
            for hop in range(self.p.majors):
                if hop < self.p.majors - 1:

                    @pl.when(self.goes(way, hop))
                    def _():
                        self.line(way, hop).wait_send()

                if way == 0 or hop > 0:

                    @pl.when(self.came(way, hop))
                    def _():
                        self.pair(way, hop).wait_send()


def gather_scratch(majors):
    return [
        pltpu.SemaphoreType.DMA((2, 2 * (majors - 1))),
        pltpu.SemaphoreType.DMA((2, 2 * majors)),
    ]


class Rows:
    def __init__(self, place, mine, whole, sems):
        self.p, self.mine, self.whole, self.sems = place, mine, whole, sems
        self.per = mine.shape[0] // BLOCK

    def copy(self, kind, c):
        p = self.p
        if kind == 2:
            block = self.whole.at[p.across[1] * self.per + c]
            return send(block, block, self.sems, 2 * self.per + c, p.near)
        to = p.near if kind == 0 else p.across
        mine = self.mine.at[pl.ds(c * BLOCK, BLOCK)]
        return send(mine, self.whole.at[p.t * self.per + c], self.sems, kind * self.per + c, to)

    def start(self):
        for c in range(self.per):
            for kind in range(2):
                self.copy(kind, c).start()

    def arrived(self, kind, c):
        self.copy(kind, c).wait_recv()

    def forward(self, c):
        self.copy(1, c).wait_recv()
        self.copy(2, c).start()

    def released(self):
        for c in range(self.per):
            self.copy(2, c).wait_send()

    def finish(self):
        for c in range(self.per):
            for kind in range(2):
                self.copy(kind, c).wait_send()


class Exchange:
    def __init__(self, slots, sems, me, count, device):
        self.slots, self.sems, self.me, self.count, self.device = slots, sems, me, count, device

    def copy(self, k, source):
        return pltpu.make_async_remote_copy(
            src_ref=self.slots.at[source],
            dst_ref=self.slots.at[source],
            send_sem=self.sems.at[0, k],
            recv_sem=self.sems.at[1, source],
            device_id=self.device((self.me + k) % self.count),
            device_id_type=MESH,
        )

    def start(self):
        for k in range(1, self.count):
            self.copy(k, self.me).start()

    def total(self):
        for k in range(1, self.count):
            self.copy(k, (self.me + k) % self.count).wait_recv()
        return functools.reduce(jnp.add, [self.slots[k] for k in range(self.count)])

    def finish(self):
        for k in range(1, self.count):
            self.copy(k, self.me).wait_send()


def scatter_scratch(majors, rows, columns):
    return [
        pltpu.VMEM((majors, rows, columns), low),
        pltpu.VMEM((majors - 1, rows, columns), low),
        pltpu.SemaphoreType.DMA((2, majors)),
        pltpu.SemaphoreType.DMA((2, majors - 1)),
    ]


def flat(blocks_ref):
    n, side, columns = blocks_ref.shape
    if side % 16 == 0:
        return blocks_ref[...].reshape(n * side, columns)
    return jnp.concatenate([blocks_ref[k].astype(f32) for k in range(n)]).astype(low)


def norm_rows(x):
    shifted = x - jnp.mean(x, axis=1, keepdims=True)
    inv_std = lax.rsqrt(jnp.mean(shifted * shifted, axis=1, keepdims=True) + EPS)
    return shifted * inv_std, inv_std


def layer_kernel(
    length_ref, tokens_ref, cot_ref, g1_ref, b1_ref, g2_ref, b2_ref, wq_ref, bq_ref, wo_ref, wi_ref,
    bi_ref, wd_ref, bo_ref, bd_ref, table_ref, turned_ref,
    out_out, gx_out, spill_out, gq_ref, gbq_ref, go_ref, gi_ref, gb_ref, gd_ref, small_ref,
    norm_ref, bias_ref, wq_mine, wd_mine, wq_all, wi_all, wd_all,
    x_all, first_ref, second_ref, cot_all, qkv_ref, qx_ref, dox_ref, context_ref, pool_ref,
    keyt_ref, queryt_ref, valuet_ref, mixed_ref, top_ref, gwq_sum, stage_ref, gb_sum, gs_sum, gw_ref, own_sems, out_sems, x_sems, cot_sems,
    wq_lines, wq_pairs, wi_lines, wi_pairs, wd_lines, wd_pairs,
    gn_near, gn_far, gn_sem1, gn_sem2,
    br_near, br_far, br_sem1, br_sem2,
    w_got, w_last, w_sem1, w_sem2,
    gq_low, q_got, q_last, q_sem1, q_sem2,
    line_ref, cross_ref, line_sem, cross_sem,
):
    here = Place()
    blocks, _, d = x_all.shape
    local = tokens_ref.shape[0]
    per = local // BLOCK
    width = wq_ref.shape[2]
    heads = width // HD
    padded = qkv_ref.shape[2] // 3
    hidden = wi_ref.shape[1]
    side = wi_ref.shape[0]
    scale = HD ** (-0.5)
    to_power = scale * math.log2(math.e)
    tall = valuet_ref.shape[1] // heads
    lane = lax.broadcasted_iota(jnp.int32, (BLOCK, padded), 1)
    of_head = [(lane >= h * HD) & (lane < (h + 1) * HD) for h in range(heads)]
    extra = (lane >= width) & (lane < width + 3)

    rows = Rows(here, tokens_ref, x_all, x_sems)
    cots = Rows(here, cot_ref, cot_all, cot_sems)
    proj_w = Gather(here, wq_mine, wq_all, (wq_lines, wq_pairs))
    in_w = Gather(here, wi_ref, wi_all, (wi_lines, wi_pairs))
    down_w = Gather(here, wd_mine, wd_all, (wd_lines, wd_pairs))

    wq_mine[...] = jnp.zeros_like(wq_mine)
    wd_mine[:, hidden:] = jnp.zeros((side, padded), low)
    bias_ref[...] = jnp.zeros_like(bias_ref)
    for k in range(3):
        wq_mine[:, k * padded : k * padded + width] = wq_ref[k]
        bias_ref[0:1, k * padded : k * padded + width] = bq_ref[k : k + 1, :]
    wd_mine[:, :hidden] = wd_ref[...]
    wd_mine[:, hidden : hidden + width] = wo_ref[...].astype(f32).T.astype(low)
    for k, ref in enumerate((g1_ref, b1_ref, g2_ref, b2_ref, bo_ref, bd_ref, bi_ref)):
        norm_ref[k, :] = ref[...]

    here.greet()
    proj_w.start()
    rows.start()
    own = [
        pltpu.make_async_copy(tokens_ref.at[pl.ds(c * BLOCK, BLOCK)], x_all.at[here.t * per + c], own_sems.at[c])
        for c in range(per)
    ]
    own += [
        pltpu.make_async_copy(cot_ref.at[pl.ds(c * BLOCK, BLOCK)], cot_all.at[here.t * per + c], own_sems.at[per + c])
        for c in range(per)
    ]
    own += [
        pltpu.make_async_copy(mine, whole.at[here.dp], own_sems.at[2 * per + k])
        for k, (mine, whole) in enumerate(((wq_mine, wq_all), (wi_ref, wi_all), (wd_mine, wd_all)))
    ]
    for copy in own:
        copy.start()

    def norm(kind, c):
        r = here.shard(kind) * per + c
        normed, _ = norm_rows(x_all[r].astype(f32))
        first_ref[r] = (normed * norm_ref[0:1, :] + norm_ref[1:2, :]).astype(low)
        second_ref[r] = (normed * norm_ref[2:3, :] + norm_ref[3:4, :]).astype(low)

    def project(kind, c):
        r = here.shard(kind) * per + c
        projected = dot(first_ref[r], flat(wq_all), NN) + bias_ref[...]
        tables = rotary_rows(table_ref, r)
        queries = rotate(projected[:, :padded], tables, 1)
        queryt_ref[r] = queries.T[:width].astype(low)
        qkv_ref[r, :, :padded] = queries.astype(low)
        keys = rotate(projected[:, padded : 2 * padded], tables, 1)
        keyt_ref[r] = keys.T[:width].astype(low)
        qkv_ref[r, :, padded : 2 * padded] = jnp.where(extra, 1.0, keys).astype(low)
        values = projected[:, 2 * padded :]
        qkv_ref[r, :, 2 * padded :] = jnp.where(extra, 1.0, values).astype(low)
        turned = values.T.astype(low)
        for h in range(heads):
            valuet_ref[r, h * tall : h * tall + HD, :] = turned[h * HD : (h + 1) * HD]
            valuet_ref[r, h * tall + HD : (h + 1) * tall, :] = jnp.ones((tall - HD, BLOCK), low)

    for c in range(per):
        own[c].wait()

    @pl.loop(0, per)
    def _(c):
        norm(0, c)

    for c in range(per):
        rows.arrived(0, c)
    proj_w.forward(1)

    @pl.loop(0, per)
    def _(c):
        norm(1, c)

    for k in range(2, here.majors - 1):
        proj_w.forward(k)
    for c in range(per - 1):
        rows.forward(c)
    proj_w.forward(here.majors - 1)
    in_w.start()
    down_w.start()
    cots.start()
    for c in range(per - 1):
        norm(2, c)
    for c in range(per - 1):
        rows.arrived(2, c)
        norm(3, c)
    own[2 * per].wait()
    proj_w.arrived()

    @pl.loop(0, per + 2 * (per - 1))
    def _(number):
        @pl.when(number == per + 1)
        def _():
            rows.forward(per - 1)

        @pl.when(number == per - 1)
        def _():
            in_w.forward(1)

        later = number // per
        project(1 + later + number % per * later, number % per * (1 - later))

    @pl.loop(0, per)
    def _(c):
        project(0, c)

    norm(2, per - 1)
    project(2, per - 1)
    for k in range(2, here.majors - 1):
        in_w.forward(k)
    rows.arrived(2, per - 1)
    norm(3, per - 1)
    project(3, per - 1)

    def spilled():
        return pltpu.make_async_copy(first_ref, spill_out, out_sems.at[1 + per])

    def restored():
        return pltpu.make_async_copy(spill_out, first_ref, out_sems.at[1 + per])

    spilled().start()

    def in_fours(count, body):
        @pl.loop(0, count // 4)
        def _(number):
            for k in range(4):
                body(4 * number + k)

        for size in (2, 1):

            @pl.when(count // size % 2 == 1)
            def _():
                for k in range(size):
                    body(count // (2 * size) * (2 * size) + k)

    in_w.forward(here.majors - 1)

    @pl.loop(0, blocks)
    def _(i):
        for k in range(1, here.majors):

            @pl.when(i == min(2 * k + 1, blocks - 1))
            def _():
                down_w.forward(k)

        for c in range(per):

            @pl.when(i == blocks - per + c)
            def _():
                cots.forward(c)

        q = qkv_ref[i, :, :padded].astype(f32)
        for h in range(heads):
            qx_ref[i, h * BLOCK : (h + 1) * BLOCK, :] = jnp.where(of_head[h], q, 0.0).astype(low)
        query = qx_ref[i]
        parts = [slice(h * BLOCK, (h + 1) * BLOCK) for h in range(heads)]

        def scores(j):
            return dot(qkv_ref[j, :, padded : 2 * padded], query, NT)

        def highest(s):
            return jnp.max(s.reshape(-1, 8, heads * BLOCK), axis=0)

        def keep(j, s):
            for h in range(heads):
                pool_ref[j * heads + h] = s[:, parts[h]]

        diagonal = scores(i)
        key_at = lax.broadcasted_iota(jnp.int32, diagonal.shape, 0)
        query_at = lax.broadcasted_iota(jnp.int32, diagonal.shape, 1) % BLOCK
        diagonal = jnp.where(key_at <= query_at, diagonal, -1e30)
        keep(i, diagonal)
        top_ref[...] = highest(diagonal)

        def first_pass(j):
            s = scores(j)
            keep(j, s)
            top_ref[...] = jnp.maximum(top_ref[...], highest(s))

        in_fours(i, first_pass)
        top = jnp.max(top_ref[...], axis=0, keepdims=True)
        mixed_ref[...] = jnp.zeros_like(mixed_ref)

        def second_pass(j):
            for h in range(heads):
                p = jnp.exp2((pool_ref[j * heads + h] - top[:, parts[h]]) * to_power).astype(low)
                at = slice(h * tall, (h + 1) * tall)
                mixed_ref[at, :] += dot(valuet_ref[j, at, :], p, NN)

        in_fours(i + 1, second_pass)
        mixed, terms = [], []
        for h in range(heads):
            total = mixed_ref[h * tall + HD : h * tall + HD + 1, :]
            mixed.append(mixed_ref[h * tall : h * tall + HD, :] * (1.0 / total))
            terms.append(jnp.concatenate(three_terms(-top[:, parts[h]] - jnp.log(total) / scale)))
        terms = jnp.concatenate(terms, axis=1)
        side_rows = width - (padded - LANES)
        columns = jnp.concatenate(
            [
                jnp.zeros((side_rows, heads * BLOCK), f32),
                terms,
                jnp.zeros((LANES - side_rows - 3, heads * BLOCK), f32),
            ]
        ).T
        for h in range(heads):
            right = jnp.where(of_head[h], q, 0.0)[:, padded - LANES :]
            qx_ref[i, parts[h], padded - LANES :] = (right + columns[parts[h]]).astype(low)
        mixed.append(jnp.zeros((padded - width, BLOCK), f32))
        context_ref[i] = jnp.concatenate(mixed).T.astype(low)

    grad_ref, act_ref, hidden_ref, gradt_ref = cot_all, x_all, first_ref, valuet_ref
    own[2 * per + 1].wait()
    in_w.arrived()
    rows.released()

    @pl.loop(0, blocks)
    def _(r):
        u = dot(second_ref[r], flat(wi_all), NN) + norm_ref[6:7, :]
        cdf = 0.5 * (1.0 + lax.erf(u * (1.0 / math.sqrt(2.0))))
        act_ref[r] = (u * cdf).astype(low)
        slope = cdf + u * (jnp.exp(-0.5 * u * u) * (1.0 / math.sqrt(2.0 * math.pi)))
        for k in range(3):
            pool_ref[3 * r + k] = slope[:, k * BLOCK : (k + 1) * BLOCK]

    for c in range(per):
        cots.arrived(0, c)
        cots.arrived(2, c)
    for copy in own[per : 2 * per] + own[2 * per + 2 :]:
        copy.wait()
    gb_sum[...] = jnp.zeros_like(gb_sum)
    gs_sum[...] = jnp.zeros_like(gs_sum)
    cots.released()
    spilled().wait()
    down_w.arrived()

    @pl.loop(0, blocks)
    def _(r):
        row = lax.broadcasted_iota(jnp.int32, (BLOCK, d), 0) + r * BLOCK
        grad = jnp.where(row < length_ref[0], cot_all[r].astype(f32), 0.0).astype(low)
        grad_ref[r] = grad
        back = dot(grad, flat(wd_all), NN)
        slope = jnp.concatenate([pool_ref[3 * r + k] for k in range(3)], axis=1)
        grad_hidden = back[:, :hidden] * slope
        gb_sum[1:2, :] += jnp.sum(grad_hidden, axis=0, keepdims=True)
        hidden_ref[r] = grad_hidden.astype(low)

        grad_context = back[:, hidden:].astype(low).astype(f32)
        gradt_ref[r, :width, :] = grad_context.T[:width].astype(low)
        product = grad_context * context_ref[r].astype(f32)
        for h in range(heads):
            extended = jnp.where(of_head[h], grad_context, 0.0)
            delta = jnp.sum(jnp.where(of_head[h], product, 0.0), axis=1, keepdims=True)
            for k, term in enumerate(three_terms(-delta)):
                extended = jnp.where(lane == width + k, term, extended)
            dox_ref[r, h * BLOCK : (h + 1) * BLOCK, :] = extended.astype(low)

    weights = Scatter(here, gw_ref, w_got, w_last, (w_sem1, w_sem2))
    final = Scatter(here, gq_low, q_got, q_last, (q_sem1, q_sem2))
    half = d // 2
    rows_total = blocks * BLOCK

    @pl.loop(0, 2)
    def _(turn):
        which = (1 - turn) * (1 - here.upper) + turn * here.upper
        at = pl.ds(pl.multiple_of(which * half, LANES), half)
        all_rows = lambda ref: ref[...].reshape(rows_total, ref.shape[2])
        mine = second_ref[:, :, at].reshape(rows_total, half)
        first_block = which * (here.n // 2)
        side_blocks = pl.ds(first_block, here.n // 2)
        gwi = dot(mine, all_rows(hidden_ref), TN).reshape(here.n // 2, side, hidden)
        gw_ref[side_blocks, :, :hidden] = gwi.astype(low)
        @pl.when(turn == 1)
        def _():
            weights.start_half(0)

        mine = grad_ref[:, :, at].reshape(rows_total, half)
        gwd = dot(mine, all_rows(act_ref), TN).reshape(here.n // 2, side, hidden)
        gw_ref[side_blocks, :, hidden : 2 * hidden] = gwd.astype(low)
        gwd = dot(mine, all_rows(context_ref), TN).reshape(here.n // 2, side, padded)
        gw_ref[side_blocks, :, 2 * hidden :] = gwd.astype(low)

    branch_ref, part_ref = cot_all, second_ref

    def near_branch(chip):
        owner = chip * 2 + 1 - here.core
        return send(
            branch_ref.at[pl.ds(owner * per, per)], br_near.at[chip], br_sem1, chip, here.near
        )

    def far_branch():
        return send(br_near.at[1 - here.chip], br_far, br_sem2, 0, here.across)

    @pl.loop(0, blocks)
    def _(number):
        r = here.shard(3 - number // per) * per + number % per

        @pl.when(number == per + 1)
        def _():
            near_branch(1 - here.chip).start()

        @pl.when(number == 2 * per + 1)
        def _():
            near_branch(1 - here.chip).wait_recv()

            @pl.loop(0, per)
            def _(c):
                mine = branch_ref[here.across[1] * per + c]
                br_near[1 - here.chip, c] = plus(mine, br_near[1 - here.chip, c]).astype(low)

        @pl.when(number == 3 * per + 1)
        def _():
            near_branch(here.chip).start()

        second = second_ref[r].astype(f32)
        part = dot(hidden_ref[r], flat(wi_all), NT)
        both = jnp.concatenate([act_ref[r], context_ref[r]], axis=1)
        branch_ref[r] = dot(both, flat(wd_all), NT).astype(low)
        gs_sum[2:3, :] += jnp.sum(part * second, axis=0, keepdims=True)
        gs_sum[3:4, :] += jnp.sum(part, axis=0, keepdims=True)
        part_ref[r] = (part * norm_ref[2:3, :]).astype(low)

        @pl.when(number == 0)
        def _():
            weights.start_half(1)

        @pl.when(number == 2 * per + 1)
        def _():
            far_branch().start()

    restored().start()
    gn_ref = x_all
    gwq_sum[...] = jnp.zeros_like(gwq_sum)
    pool_ref[...] = jnp.zeros_like(pool_ref)

    last = blocks - 1
    half_rot = ROT // 2

    def block_of(number):
        return number // 2 + number % 2 * (last - number // 2 * 2)

    def slot_of(r):
        return r // per // 2 * per + r % per

    def near_block(r):
        return send(gn_ref.at[r], gn_near.at[slot_of(r)], gn_sem1, slot_of(r), here.near)

    def far_block(c):
        mine = gn_near.at[(1 - here.chip) * per + c]
        return send(mine, gn_far.at[c], gn_sem2, c, here.across)

    def hand_over(r):
        @pl.when(r // per % 2 != here.core)
        def _():
            near_block(r).start()

    def collect(r):
        owner = r // per

        @pl.when(owner % 2 == here.core)
        def _():
            near_block(r).wait_recv()

        @pl.when((owner % 2 == here.core) & (owner // 2 != here.chip))
        def _():
            gn_near[slot_of(r)] = plus(gn_ref[r], gn_near[slot_of(r)]).astype(low)

    def pass_on(r):
        owner = r // per

        @pl.when((owner % 2 == here.core) & (owner // 2 != here.chip))
        def _():
            far_block(r % per).start()

    def pair(i, j, own):
        keys, values = qkv_ref[j, :, padded : 2 * padded], qkv_ref[j, :, 2 * padded :]
        query, dout = qx_ref[i], dox_ref[i]
        p = jnp.exp2(dot(query, keys, NT) * to_power)
        if own:
            query_at = lax.broadcasted_iota(jnp.int32, p.shape, 0) % BLOCK
            key_at = lax.broadcasted_iota(jnp.int32, p.shape, 1)
            p = jnp.where(key_at <= query_at, p, 0.0)
        ds = (p * dot(dout, values, NT)).astype(low)
        p = p.astype(low)
        for h in range(heads):
            at, part = slice(h * HD, (h + 1) * HD), slice(h * BLOCK, (h + 1) * BLOCK)
            pool_ref[blocks + j, at, :] += dot(gradt_ref[i, at, :], p[part], NN)
            pool_ref[j, at, :] += dot(queryt_ref[i, at, :], ds[part], NN)
            pool_ref[2 * blocks + i, at, :] += dot(keyt_ref[j, at, :], ds[part], NT)

    def kept(c, values):
        row = lax.broadcasted_iota(jnp.int32, (BLOCK, d), 0) + (here.t * per + c) * BLOCK
        return jnp.where(row < length_ref[0], values, 0.0)

    for c in range(per):
        cot = kept(c, cot_ref[c * BLOCK : (c + 1) * BLOCK, :].astype(f32))
        gs_sum[4:5, :] += jnp.sum(cot, axis=0, keepdims=True)

    def output_copy():
        return pltpu.make_async_copy(stage_ref.at[:], out_out, out_sems.at[0])

    @pl.loop(0, blocks)
    def _(step):
        for k in range(1, here.majors):

            @pl.when(step == min(k, last - 2))
            def _():
                weights.add(k)

        @pl.when(step > 0)
        def _():
            hand_over(block_of(step - 1))

        turn = step // 2
        odd = step % 2
        now = block_of(step)
        pair(now, now, True)

        for k in range(1, here.majors):

            @pl.when(step == min(k, last - 2))
            def _():
                weights.forward(k)

        @pl.when(step > 0)
        def _():
            collect(block_of(step - 1))

        def next_pair(number):
            other = turn + 1 + number
            pair(other + odd * (last - turn - other), turn + odd * (other - turn), False)

        in_fours(last - step, next_pair)

        @pl.when(step == last // 2)
        def _():
            far_branch().wait()
            for chip in range(2):
                near_branch(chip).wait_send()
            near_branch(here.chip).wait_recv()

            @pl.loop(0, per)
            def _(c):
                total = plus(branch_ref[here.t * per + c], br_near[here.chip, c], br_far[c])
                total += norm_ref[4:5, :] + norm_ref[5:6, :]
                at = pl.ds(pl.multiple_of(c * BLOCK, BLOCK), BLOCK)
                stage_ref[at, :] = tokens_ref[at, :].astype(f32) + kept(c, total)

        positions = pl.ds(pl.multiple_of(now * BLOCK, BLOCK), BLOCK)
        cosine, sine = turned_ref[:half_rot, positions], turned_ref[half_rot:, positions]
        for slab in (now, 2 * blocks + now):
            for h in range(heads):
                near_rows = slice(h * HD, h * HD + half_rot)
                far_rows = slice(h * HD + half_rot, h * HD + 2 * half_rot)
                near_part, far_part = pool_ref[slab, near_rows, :], pool_ref[slab, far_rows, :]
                pool_ref[slab, near_rows, :] = near_part * cosine + far_part * sine
                pool_ref[slab, far_rows, :] = far_part * cosine - near_part * sine
        filler = jnp.zeros((BLOCK, padded - width), f32)
        turned = [
            jnp.concatenate([pool_ref[k * blocks + now, :width, :].T, filler], axis=1)
            for k in range(3)
        ]
        projected = jnp.concatenate([turned[2] * scale, turned[0] * scale, turned[1]], axis=1)
        gb_sum[0:1, :] += jnp.sum(projected, axis=0, keepdims=True)
        proj_low = projected.astype(low)
        @pl.when(step == 0)
        def _():
            restored().wait()

        first = first_ref[now]
        gwq_sum[...] += dot(first, proj_low, TN)
        part = dot(proj_low, flat(wq_all), NT)
        gs_sum[0:1, :] += jnp.sum(part * first.astype(f32), axis=0, keepdims=True)
        gs_sum[1:2, :] += jnp.sum(part, axis=0, keepdims=True)
        gn_ref[now] = (part * norm_ref[0:1, :] + part_ref[now].astype(f32)).astype(low)

        @pl.when(step > 0)
        def _():
            pass_on(block_of(step - 1))

        @pl.when(step == last // 2)
        def _():
            output_copy().start()

    now = block_of(last)
    for block in range(here.n):
        rows_of = slice(block * side, (block + 1) * side)
        gq_low[block] = jnp.concatenate(
            [gwq_sum[rows_of, k * padded : k * padded + width] for k in range(3)], axis=1
        ).astype(low)
    hand_over(now)
    final.start_half(0)
    final.start_half(1)
    line_ref[here.dp] = jnp.concatenate(
        [gb_sum[0:2, :], gs_sum[0:5, :], jnp.zeros((1, d), f32)]
    )
    line = Exchange(line_ref, line_sem, here.dp, here.n, lambda to: (to, here.t))
    cross = Exchange(cross_ref, cross_sem, here.t, here.ways, lambda to: (here.dp, to))
    collect(now)
    pass_on(now)
    line.start()
    for k in range(1, here.majors):
        final.add(k)
        if k == 1:
            total = weights.finish()
            gi_ref[...] = total[:, :hidden]
            gd_ref[...] = total[:, hidden : 2 * hidden]
            go_ref[...] = total[:, 2 * hidden : 2 * hidden + width].T
        final.forward(k)
    summed = line.total()
    for k in range(3):
        gbq_ref[k : k + 1, :] = summed[0:1, k * padded : k * padded + width]
    gb_ref[...] = summed[1, :]
    cross_ref[here.t] = summed
    cross.start()

    def grad_copy(c):
        at = pl.ds(c * BLOCK, BLOCK)
        return pltpu.make_async_copy(stage_ref.at[at], gx_out.at[at], out_sems.at[1 + c])

    for c in range(per):
        far_block(c).wait()
    output_copy().wait()
    for c in range(per):
        at = slice(c * BLOCK, (c + 1) * BLOCK)
        normed, inv_std = norm_rows(tokens_ref[at, :].astype(f32))
        grad_normed = plus(gn_ref[here.t * per + c], gn_near[here.chip * per + c], gn_far[c])
        stage_ref[at, :] = cot_ref[at, :].astype(f32) + inv_std * (
            grad_normed
            - jnp.mean(grad_normed, axis=1, keepdims=True)
            - normed * jnp.mean(grad_normed * normed, axis=1, keepdims=True)
        )
        grad_copy(c).start()
    summed = cross.total()
    for k in range(2):
        product, plain = summed[2 + 2 * k : 3 + 2 * k, :], summed[3 + 2 * k : 4 + 2 * k, :]
        gain, bias = norm_ref[2 * k : 2 * k + 1, :], norm_ref[2 * k + 1 : 2 * k + 2, :]
        small_ref[2 * k : 2 * k + 1, :] = (product - bias * plain) / gain
        small_ref[2 * k + 1 : 2 * k + 2, :] = plain
    small_ref[4:5, :] = summed[6:7, :]
    for slot in range(2 * per):
        near_block(slot // per * 2 * per + (1 - here.core) * per + slot % per).wait_send()
    for one in (rows, cots, proj_w, in_w, down_w, line, cross):
        one.finish()
    for c in range(per):
        grad_copy(c).wait()
    total = final.finish()
    for k in range(3):
        gq_ref[k] = total[:, k * width : (k + 1) * width]


def layer(length, tokens, cot, norms, wq, bq, wo, wi, bi, wd, biases, table, turned):
    local, d = tokens.shape
    _, side, width = wq.shape
    hidden = wi.shape[1]
    heads = width // HD
    padded = round_up(width + 3, LANES)
    n, ways = lax.axis_size("dp"), lax.axis_size("tensor")
    majors = n // 2
    rows = local * ways
    blocks, per = rows // BLOCK, local // BLOCK
    assert rows == LMAX and length.shape[0] == 1
    assert ways == 4 and per == 2 and n % 4 == 0 and padded == BLOCK and heads == 3
    assert 3 * padded == d == hidden == side * n
    vmem = pl.BlockSpec(memory_space=pltpu.VMEM)
    hbm = pl.BlockSpec(memory_space=pl.ANY)
    row_blocks = pltpu.VMEM((blocks, BLOCK, d), low)
    head_blocks = pltpu.VMEM((blocks, heads * BLOCK, padded), low)
    columns = hidden + wd.shape[1] + padded
    outs = [
        jax.ShapeDtypeStruct((local, d), f32),
        jax.ShapeDtypeStruct((local, d), f32),
        jax.ShapeDtypeStruct((blocks, BLOCK, d), low),
        jax.ShapeDtypeStruct((3, side, width), f32),
        jax.ShapeDtypeStruct((3, width), f32),
        jax.ShapeDtypeStruct((width, side), f32),
        jax.ShapeDtypeStruct((side, hidden), f32),
        jax.ShapeDtypeStruct((hidden,), f32),
        jax.ShapeDtypeStruct((side, hidden), f32),
        jax.ShapeDtypeStruct((5, d), f32),
    ]
    args = (tokens, cot, *norms, wq, bq, wo, wi, bi, wd, *biases, table, turned)
    return pl.pallas_call(
        layer_kernel,
        name="layer",
        in_specs=[pl.BlockSpec(memory_space=pltpu.SMEM)] + [vmem] * len(args),
        out_specs=[hbm] * 3 + [vmem] * (len(outs) - 3),
        out_shape=outs,
        scratch_shapes=[
            pltpu.VMEM((8, d), f32),
            pltpu.VMEM((1, 3 * padded), f32),
            pltpu.VMEM((side, 3 * padded), low),
            pltpu.VMEM((side, hidden + padded), low),
            pltpu.VMEM((n, side, 3 * padded), low),
            pltpu.VMEM((n, side, hidden), low),
            pltpu.VMEM((n, side, hidden + padded), low),
            row_blocks, row_blocks, row_blocks, row_blocks,
            pltpu.VMEM((blocks, BLOCK, 3 * padded), low),
            head_blocks, head_blocks,
            pltpu.VMEM((blocks, BLOCK, padded), low),
            pltpu.VMEM((blocks * heads, BLOCK, BLOCK), f32),
            pltpu.VMEM((blocks, width, BLOCK), low),
            pltpu.VMEM((blocks, width, BLOCK), low),
            pltpu.VMEM((blocks, heads * (HD + 16), BLOCK), low),
            pltpu.VMEM((heads * (HD + 16), BLOCK), f32),
            pltpu.VMEM((8, heads * BLOCK), f32),
            pltpu.VMEM((d, hidden), f32),
            pltpu.VMEM((local, d), f32),
            pltpu.VMEM((8, d), f32),
            pltpu.VMEM((8, d), f32),
            pltpu.VMEM((n, side, columns), low),
            pltpu.SemaphoreType.DMA((2 * per + 3,)),
            pltpu.SemaphoreType.DMA((2 + per,)),
            pltpu.SemaphoreType.DMA((2, 3 * per)),
            pltpu.SemaphoreType.DMA((2, 3 * per)),
            *gather_scratch(majors), *gather_scratch(majors), *gather_scratch(majors),
            pltpu.VMEM((2 * per, BLOCK, d), low),
            pltpu.VMEM((per, BLOCK, d), low),
            pltpu.SemaphoreType.DMA((2, 2 * per)),
            pltpu.SemaphoreType.DMA((2, per)),
            pltpu.VMEM((2, per, BLOCK, d), low),
            pltpu.VMEM((per, BLOCK, d), low),
            pltpu.SemaphoreType.DMA((2, 2)),
            pltpu.SemaphoreType.DMA((2, 1)),
            *scatter_scratch(majors, side, columns),
            pltpu.VMEM((n, side, 3 * width), low),
            *scatter_scratch(majors, side, 3 * width),
            pltpu.VMEM((n, 8, d), f32),
            pltpu.VMEM((ways, 8, d), f32),
            pltpu.SemaphoreType.DMA((2, n)),
            pltpu.SemaphoreType.DMA((2, ways)),
        ],
        compiler_params=pltpu.CompilerParams(
            vmem_limit_bytes=VMEM, collective_id=0, has_side_effects=True
        ),
    )(length, *args)


def settle_kernel(*refs):
    count = len(refs) // 3
    sources, targets, held, sems = refs[:count], refs[count : 2 * count], refs[2 * count : -1], refs[-1]
    taken = [
        pltpu.make_async_copy(source, buffer, sems.at[0, k])
        for k, (source, buffer) in enumerate(zip(sources, held))
    ]
    put = [
        pltpu.make_async_copy(buffer, target, sems.at[1, k])
        for k, (buffer, target) in enumerate(zip(held, targets))
    ]
    for copy in taken:
        copy.start()
    for before, after in zip(taken, put):
        before.wait()
        after.start()
    for copy in put:
        copy.wait()


def settle(arrays):
    hbm = pl.BlockSpec(memory_space=pl.ANY)
    return pl.pallas_call(
        settle_kernel,
        name="settle",
        in_specs=[hbm] * len(arrays),
        out_specs=[hbm] * len(arrays),
        out_shape=[jax.ShapeDtypeStruct(a.shape, a.dtype) for a in arrays],
        scratch_shapes=[pltpu.VMEM(a.shape, a.dtype) for a in arrays]
        + [pltpu.SemaphoreType.DMA((2, len(arrays)))],
        compiler_params=pltpu.CompilerParams(vmem_limit_bytes=VMEM),
    )(*arrays)


def per_device(
    tokens, cotangent, seq_lengths, norm1_gain, norm1_bias, norm2_gain, norm2_bias,
    w_qkv, b_qkv, w_attn_out, w_in, b_in, w_down, b_out, b_down,
):
    output, grad_x, _, *rest = layer(
        seq_lengths, tokens, cotangent, (norm1_gain, norm1_bias, norm2_gain, norm2_bias),
        w_qkv.transpose(1, 0, 2), b_qkv, w_attn_out, w_in, b_in, w_down.T, (b_out, b_down),
        jnp.asarray(rotary_base()), jnp.asarray(rotary_turned()),
    )
    output, grad_x, g_qkv, gb_qkv, g_out, g_in, gb_in, g_down, small = settle(
        [output, grad_x, *rest]
    )
    return output, grad_x, g_qkv.transpose(1, 0, 2), gb_qkv, g_out, g_in, gb_in, g_down.T, small


def solution(mesh):
    rows = P(("dp", "tensor"), None)
    placed = (
        rows, rows, P("dp"), P(), P(), P(), P(), P("dp", None, "tensor"), P(None, "tensor"),
        P("tensor", "dp"), P("dp", "tensor"), P("tensor"), P("tensor", "dp"), P(), P(),
    )
    return jax.shard_map(
        per_device,
        mesh=mesh,
        in_specs=placed,
        out_specs=(
            rows, rows, P("dp", None, "tensor"), P(None, "tensor"), P("tensor", "dp"),
            P("dp", "tensor"), P("tensor"), P("tensor", "dp"), P(),
        ),
        check_vma=False,
    )
```
